64 devices in a mesh: dp: 4 (over x, y), ep: 16 (over z, core).
Axes of the slice: x: 2, y: 2, z: 8, core: 2. Of those that a mesh axis runs over, the one named last changes fastest.
The devices are a block of a 4x4x8 slice.
Arguments:
- x_in: bfloat16 [16384, 512], P(('dp', 'ep')), parts along dimension 0
- d_out: bfloat16 [16384, 512], P(('dp', 'ep')), parts along dimension 0
- idx_a: int32 [16384, 6], P(('dp', 'ep')), parts along dimension 0
- gate_a: float32 [16384, 6], P(('dp', 'ep')), parts along dimension 0
- idx_b: int32 [16384, 6], P(('dp', 'ep')), parts along dimension 0
- gate_b: float32 [16384, 6], P(('dp', 'ep')), parts along dimension 0
- w1_a: bfloat16 [64, 512, 352], P('ep')
- w3_a: bfloat16 [64, 512, 352], P('ep')
- w2_a: bfloat16 [64, 352, 512], P('ep')
- ws1_a: bfloat16 [512, 704], replicated
- ws3_a: bfloat16 [512, 704], replicated
- ws2_a: bfloat16 [704, 512], replicated
- w1_b: bfloat16 [64, 512, 352], P('ep')
- w3_b: bfloat16 [64, 512, 352], P('ep')
- w2_b: bfloat16 [64, 352, 512], P('ep')
- ws1_b: bfloat16 [512, 704], replicated
- ws3_b: bfloat16 [512, 704], replicated
- ws2_b: bfloat16 [704, 512], replicated
Outputs:
- output 1: bfloat16 [16384, 512], P(('dp', 'ep')), parts along dimension 0
- output 2: bfloat16 [16384, 512], P(('dp', 'ep')), parts along dimension 0
- output 3: float32 [256, 512, 352], P(('dp', 'ep')), parts along dimension 0
- output 4: float32 [256, 512, 352], P(('dp', 'ep')), parts along dimension 0
- output 5: float32 [256, 352, 512], P(('dp', 'ep')), parts along dimension 0
- output 6: float32 [256, 512, 352], P(('dp', 'ep')), parts along dimension 0
- output 7: float32 [256, 512, 352], P(('dp', 'ep')), parts along dimension 0
- output 8: float32 [256, 352, 512], P(('dp', 'ep')), parts along dimension 0
- output 9: float32 [16384, 6], P(('dp', 'ep')), parts along dimension 0
- output 10: float32 [16384, 6], P(('dp', 'ep')), parts along dimension 0
There are 4 independent parts. The reference program is written for one: setup_inputs(seed, part) draws one part's arguments, and reference() takes and returns one part's arrays. A program takes and returns all parts, laid end to end along the dimension named above; an argument that names none is the same for every part.
All inputs are finite; a program needn't handle non-finite values.
Results may differ from the reference program's by a relative error of at most 0.0115909.
Values are sent between devices in bfloat16 or wider.
A program may use at most 768 MiB of HBM per device.

```python
import jax
import jax.numpy as jnp
from jax import lax

D_MODEL = 512
FF_EXPERT = 352
FF_SHARED = 704
EXPERTS = 64
TOP_K = 6
TOKENS = 256
GROUP_SIZE = 16
REP_COUNT = 8
CAPACITY = 48

PART_TOKENS = GROUP_SIZE * TOKENS
GROUP_ROWS = GROUP_SIZE * CAPACITY


def draw_routing(rng_key):
    fixed_ids = jnp.repeat(jnp.arange(TOP_K, dtype=jnp.int32), REP_COUNT)
    spare_ids = jnp.repeat(jnp.arange(TOP_K, EXPERTS, dtype=jnp.int32), REP_COUNT)

    def one_device(dev_key):
        sub_keys = jax.random.split(dev_key, 4)
        picked = jax.random.permutation(sub_keys[0], spare_ids)[: TOKENS - TOP_K * REP_COUNT]
        base_ids = jax.random.permutation(sub_keys[1], jnp.concatenate([fixed_ids, picked]))
        shift_by = jax.random.randint(sub_keys[2], (), 0, EXPERTS, dtype=jnp.int32)
        turn_by = jax.random.randint(sub_keys[3], (TOKENS, 1), 0, TOP_K, dtype=jnp.int32)
        offsets = (jnp.arange(TOP_K, dtype=jnp.int32)[None, :] + turn_by) % TOP_K
        return (base_ids[:, None] + offsets + shift_by) % EXPERTS

    dev_keys = jax.random.split(rng_key, GROUP_SIZE)
    return jax.vmap(one_device)(dev_keys).reshape(PART_TOKENS, TOP_K)


def normal_bf16(rng_key, out_shape, scale):
    return (jax.random.normal(rng_key, out_shape, jnp.float32) * scale).astype(jnp.bfloat16)


def layer_weights(weight_keys, key_start):
    return (
        normal_bf16(weight_keys[key_start], (EXPERTS, D_MODEL, FF_EXPERT), D_MODEL ** -0.5),
        normal_bf16(weight_keys[key_start + 1], (EXPERTS, D_MODEL, FF_EXPERT), D_MODEL ** -0.5),
        normal_bf16(weight_keys[key_start + 2], (EXPERTS, FF_EXPERT, D_MODEL), FF_EXPERT ** -0.5),
        normal_bf16(weight_keys[key_start + 3], (D_MODEL, FF_SHARED), D_MODEL ** -0.5),
        normal_bf16(weight_keys[key_start + 4], (D_MODEL, FF_SHARED), D_MODEL ** -0.5),
        normal_bf16(weight_keys[key_start + 5], (FF_SHARED, D_MODEL), FF_SHARED ** -0.5),
    )


def setup_inputs(seed: int = 0, part: int = 0) -> dict:
    part_keys = jax.random.split(jax.random.fold_in(jax.random.key(seed), part), 6)
    weight_keys = jax.random.split(jax.random.key(seed + 1), 12)
    gate_scale = TOP_K ** -0.5
    w1_a, w3_a, w2_a, ws1_a, ws3_a, ws2_a = layer_weights(weight_keys, 0)
    w1_b, w3_b, w2_b, ws1_b, ws3_b, ws2_b = layer_weights(weight_keys, 6)
    return {
        'x_in': normal_bf16(part_keys[0], (PART_TOKENS, D_MODEL), 1.0),
        'd_out': normal_bf16(part_keys[1], (PART_TOKENS, D_MODEL), 1.0),
        'idx_a': draw_routing(part_keys[2]),
        'gate_a': jax.random.uniform(part_keys[3], (PART_TOKENS, TOP_K), jnp.float32, 0.5, 1.5) * gate_scale,
        'idx_b': draw_routing(part_keys[4]),
        'gate_b': jax.random.uniform(part_keys[5], (PART_TOKENS, TOP_K), jnp.float32, 0.5, 1.5) * gate_scale,
        'w1_a': w1_a, 'w3_a': w3_a, 'w2_a': w2_a,
        'ws1_a': ws1_a, 'ws3_a': ws3_a, 'ws2_a': ws2_a,
        'w1_b': w1_b, 'w3_b': w3_b, 'w2_b': w2_b,
        'ws1_b': ws1_b, 'ws3_b': ws3_b, 'ws2_b': ws2_b,
    }


def route_tables(expert_ids):
    flat_ids = expert_ids.reshape(-1)
    pair_count = flat_ids.shape[0]
    pair_order = jnp.argsort(flat_ids, stable=True)
    expert_count = jax.ops.segment_sum(jnp.ones_like(flat_ids), flat_ids, num_segments=EXPERTS)
    expert_start = jnp.cumsum(expert_count) - expert_count
    position = flat_ids * GROUP_ROWS + jnp.argsort(pair_order) - expert_start[flat_ids]
    slot_index = jnp.arange(GROUP_ROWS)
    src_pair = pair_order[jnp.minimum(expert_start[:, None] + slot_index[None, :], pair_count - 1)]
    slot_used = slot_index[None, :] < expert_count[:, None]
    return src_pair, slot_used, position


def swiglu_hidden(rows, w_gate, w_up):
    pre_gate = jnp.dot(rows, w_gate, preferred_element_type=jnp.float32)
    pre_up = jnp.dot(rows, w_up, preferred_element_type=jnp.float32)
    return pre_gate, pre_up, (jax.nn.silu(pre_gate) * pre_up).astype(jnp.bfloat16)


def swiglu_grads(pre_gate, pre_up, d_hidden):
    sigma = jax.nn.sigmoid(pre_gate)
    d_gate = d_hidden * pre_up * sigma * (1.0 + pre_gate * (1.0 - sigma))
    d_up = d_hidden * pre_gate * sigma
    return d_gate.astype(jnp.bfloat16), d_up.astype(jnp.bfloat16)


def layer_forward(x_rows, expert_ids, gates, w_gate, w_up, w_down, s_gate, s_up, s_down):
    src_pair, slot_used, position = route_tables(expert_ids)
    sent = jnp.where(slot_used[:, :, None], x_rows[src_pair // TOP_K], 0)

    def one_expert(operands):
        rows, gate_w, up_w, down_w = operands
        hidden = swiglu_hidden(rows, gate_w, up_w)[2]
        return jnp.dot(hidden, down_w, preferred_element_type=jnp.float32).astype(jnp.bfloat16)

    expert_out = lax.map(one_expert, (sent, w_gate, w_up, w_down))
    per_pair = expert_out.reshape(-1, D_MODEL)[position].reshape(PART_TOKENS, TOP_K, D_MODEL)
    shared = jnp.dot(swiglu_hidden(x_rows, s_gate, s_up)[2], s_down, preferred_element_type=jnp.float32)
    mixed = x_rows.astype(jnp.float32) + shared + jnp.sum(gates[:, :, None] * per_pair.astype(jnp.float32), axis=1)
    return mixed.astype(jnp.bfloat16)


def layer_backward(x_rows, d_next, expert_ids, gates, w_gate, w_up, w_down, s_gate, s_up, s_down):
    src_pair, slot_used, position = route_tables(expert_ids)
    src_token = src_pair // TOP_K
    sent = jnp.where(slot_used[:, :, None], x_rows[src_token], 0)
    sent_dy = jnp.where(slot_used[:, :, None], d_next[src_token], 0)
    sent_gate = jnp.where(slot_used, gates.reshape(-1)[src_pair], 0.0)

    def one_expert(operands):
        rows, dy_part, gate_part, gate_w, up_w, down_w = operands
        pre_gate, pre_up, hidden = swiglu_hidden(rows, gate_w, up_w)
        projected = jnp.dot(dy_part, down_w.T, preferred_element_type=jnp.float32)
        gate_grad = jnp.sum(hidden.astype(jnp.float32) * projected, axis=1)
        scaled = (gate_part[:, None] * dy_part.astype(jnp.float32)).astype(jnp.bfloat16)
        dw_down = jnp.dot(hidden.T, scaled, preferred_element_type=jnp.float32)
        da_gate, da_up = swiglu_grads(pre_gate, pre_up, gate_part[:, None] * projected)
        dw_gate = jnp.dot(rows.T, da_gate, preferred_element_type=jnp.float32)
        dw_up = jnp.dot(rows.T, da_up, preferred_element_type=jnp.float32)
        d_rows = (jnp.dot(da_gate, gate_w.T, preferred_element_type=jnp.float32)
                  + jnp.dot(da_up, up_w.T, preferred_element_type=jnp.float32)).astype(jnp.bfloat16)
        return dw_gate, dw_up, dw_down, d_rows, gate_grad

    dw_gate, dw_up, dw_down, d_sent, gate_grad = lax.map(
        one_expert, (sent, sent_dy, sent_gate, w_gate, w_up, w_down))
    du_pair = d_sent.reshape(-1, D_MODEL)[position].reshape(PART_TOKENS, TOP_K, D_MODEL)
    d_gates = gate_grad.reshape(-1)[position].reshape(PART_TOKENS, TOP_K)
    s_pre = swiglu_hidden(x_rows, s_gate, s_up)
    s_projected = jnp.dot(d_next, s_down.T, preferred_element_type=jnp.float32)
    ds_gate, ds_up = swiglu_grads(s_pre[0], s_pre[1], s_projected)
    shared_dx = (jnp.dot(ds_gate, s_gate.T, preferred_element_type=jnp.float32)
                 + jnp.dot(ds_up, s_up.T, preferred_element_type=jnp.float32))
    d_x = d_next.astype(jnp.float32) + shared_dx + jnp.sum(du_pair.astype(jnp.float32), axis=1)
    return d_x.astype(jnp.bfloat16), dw_gate, dw_up, dw_down, d_gates


def reference(x_in, d_out, idx_a, gate_a, idx_b, gate_b,
              w1_a, w3_a, w2_a, ws1_a, ws3_a, ws2_a,
              w1_b, w3_b, w2_b, ws1_b, ws3_b, ws2_b):
    x_mid = layer_forward(x_in, idx_a, gate_a, w1_a, w3_a, w2_a, ws1_a, ws3_a, ws2_a)
    x_last = layer_forward(x_mid, idx_b, gate_b, w1_b, w3_b, w2_b, ws1_b, ws3_b, ws2_b)
    d_mid, dw1_b, dw3_b, dw2_b, dgate_b = layer_backward(
        x_mid, d_out, idx_b, gate_b, w1_b, w3_b, w2_b, ws1_b, ws3_b, ws2_b)
    d_first, dw1_a, dw3_a, dw2_a, dgate_a = layer_backward(
        x_in, d_mid, idx_a, gate_a, w1_a, w3_a, w2_a, ws1_a, ws3_a, ws2_a)
    return (x_last, d_first, dw1_a, dw3_a, dw2_a, dw1_b, dw3_b, dw2_b, dgate_a, dgate_b)
```

```python
import jax
import jax.numpy as jnp
from jax import lax
from jax.sharding import PartitionSpec as P

F32 = jnp.float32
BF16 = jnp.bfloat16


def slot_capacity(tokens, n_experts, top_k):
    return top_k * ((2 * tokens + n_experts - 1) // n_experts)


def swiglu_grads(pre_gate, pre_up, d_hidden):
    sigma = jax.nn.sigmoid(pre_gate)
    d_gate = d_hidden * pre_up * sigma * (1.0 + pre_gate * (1.0 - sigma))
    d_up = d_hidden * pre_gate * sigma
    return d_gate.astype(BF16), d_up.astype(BF16)


def hidden_of(rows, w_gate, w_up):
    pre_gate = jnp.matmul(rows, w_gate, preferred_element_type=F32)
    pre_up = jnp.matmul(rows, w_up, preferred_element_type=F32)
    return pre_gate, pre_up, (jax.nn.silu(pre_gate) * pre_up).astype(BF16)


def split3(values):
    hi = values.astype(BF16)
    rest = values - hi.astype(F32)
    mid = rest.astype(BF16)
    return hi, mid, (rest - mid.astype(F32)).astype(BF16)


def routing(ids, gates, n_local, capacity):
    n_src, _, tokens = ids.shape
    first = (lax.axis_index('ep') * n_local).astype(F32)
    experts = first + jnp.arange(n_local, dtype=F32)
    hit = ids[:, None] == experts[None, :, None, None]
    used = jnp.any(hit, axis=2)
    gate = jnp.sum(jnp.where(hit, gates[:, None], 0.0), axis=2)
    before = jnp.triu(jnp.ones((tokens, tokens), BF16), 1)
    rank = jnp.einsum('set,tu->seu', used.astype(BF16), before, preferred_element_type=F32)
    slot = jnp.where(used, rank, -1.0)
    match = slot[:, :, None, :] == jnp.arange(capacity, dtype=F32)[None, None, :, None]
    return match, gate


def solution(mesh):
    group_size = mesh.shape['ep']
    token_spec = P(('dp', 'ep'), None)
    expert_spec = P('ep', None, None)
    shared_spec = P(None, None)
    grad_spec = P(('dp', 'ep'), None, None)
    layer_specs = (expert_spec,) * 3 + (shared_spec,) * 3

    def dispatch(match, gathered):
        rows = jnp.einsum('sect,std->escd', match.astype(BF16), gathered, preferred_element_type=F32)
        n_local = rows.shape[0]
        return rows.astype(BF16).reshape(n_local, -1, rows.shape[-1])

    def gather(rows):
        return lax.all_gather(rows, 'ep')

    def forward(rows, match, gate, weights):
        hidden = hidden_of(rows, weights[0], weights[1])[2]
        out = jnp.matmul(hidden, weights[2], preferred_element_type=F32).astype(BF16)
        n_src, n_local, capacity, tokens = match.shape
        out = out.reshape(n_local, n_src, capacity, -1)
        part = sum(jnp.einsum('sect,escd->std', jnp.where(match, g[:, :, None, :], 0).astype(BF16), out,
                              preferred_element_type=F32) for g in split3(gate))
        return lax.psum_scatter(part, 'ep', scatter_dimension=0, tiled=True)[0]

    def backward(rows, dy, match, gate, weights):
        w_gate, w_up, w_down = weights[:3]
        n_src, n_local, capacity, tokens = match.shape
        gate_slot = jnp.sum(jnp.where(match, gate[:, :, None, :], 0.0), axis=3)
        gate_col = gate_slot.transpose(1, 0, 2).reshape(n_local, -1, 1)
        pre_gate, pre_up, hidden = hidden_of(rows, w_gate, w_up)
        projected = jnp.einsum('erd,efd->erf', dy, w_down, preferred_element_type=F32)
        gate_grad = jnp.sum(hidden.astype(F32) * projected, axis=2)
        scaled = (gate_col * dy).astype(BF16)
        dw_down = jnp.einsum('erf,erd->efd', hidden, scaled, preferred_element_type=F32)
        da_gate, da_up = swiglu_grads(pre_gate, pre_up, gate_col * projected)
        dw_gate = jnp.einsum('erd,erf->edf', rows, da_gate, preferred_element_type=F32)
        dw_up = jnp.einsum('erd,erf->edf', rows, da_up, preferred_element_type=F32)
        du = (jnp.einsum('erf,edf->erd', da_gate, w_gate, preferred_element_type=F32)
              + jnp.einsum('erf,edf->erd', da_up, w_up, preferred_element_type=F32)).astype(BF16)
        du = du.reshape(n_local, n_src, capacity, -1)
        part = jnp.einsum('sect,escd->std', match.astype(BF16), du, preferred_element_type=F32)
        du_sum = lax.psum_scatter(part, 'ep', scatter_dimension=0, tiled=True)[0]
        grad_slot = gate_grad.reshape(n_local, n_src, capacity).transpose(1, 0, 2)
        grad_tok = jnp.sum(jnp.where(match, grad_slot[:, :, :, None], 0.0), axis=2)
        grad_back = lax.all_to_all(grad_tok, 'ep', 0, 0, tiled=True)
        return du_sum, dw_gate, dw_up, dw_down, grad_back.reshape(-1, tokens)

    def gate_grads(grad_back, ids):
        experts = jnp.arange(grad_back.shape[0], dtype=ids.dtype)
        hit = ids[:, :, None] == experts[None, None, :]
        return jnp.sum(jnp.where(hit, grad_back.T[:, None, :], 0.0), axis=2)

    def shared_out(x_rows, weights):
        return jnp.matmul(hidden_of(x_rows, weights[3], weights[4])[2], weights[5], preferred_element_type=F32)

    def shared_grad(x_rows, dy, weights):
        pre_gate, pre_up, _ = hidden_of(x_rows, weights[3], weights[4])
        projected = jnp.einsum('td,fd->tf', dy, weights[5], preferred_element_type=F32)
        da_gate, da_up = swiglu_grads(pre_gate, pre_up, projected)
        return (jnp.einsum('tf,df->td', da_gate, weights[3], preferred_element_type=F32)
                + jnp.einsum('tf,df->td', da_up, weights[4], preferred_element_type=F32))

    def device_step(x_in, d_out, idx_a, gate_a, idx_b, gate_b,
                    w1_a, w3_a, w2_a, ws1_a, ws3_a, ws2_a,
                    w1_b, w3_b, w2_b, ws1_b, ws3_b, ws2_b):
        weights_a = (w1_a, w3_a, w2_a, ws1_a, ws3_a, ws2_a)
        weights_b = (w1_b, w3_b, w2_b, ws1_b, ws3_b, ws2_b)
        tokens, top_k = idx_a.shape
        n_local = w1_a.shape[0]
        capacity = slot_capacity(tokens, n_local * group_size, top_k)
        table = jnp.concatenate([idx_a.astype(F32), idx_b.astype(F32), gate_a, gate_b], axis=1).T
        tables = gather(table)
        match_a, gates_a = routing(tables[:, :top_k], tables[:, 2 * top_k:3 * top_k], n_local, capacity)
        match_b, gates_b = routing(tables[:, top_k:2 * top_k], tables[:, 3 * top_k:], n_local, capacity)
        rows_a = dispatch(match_a, gather(x_in))
        mix = forward(rows_a, match_a, gates_a, weights_a)
        x_mid = (x_in.astype(F32) + shared_out(x_in, weights_a) + mix).astype(BF16)
        rows_b = dispatch(match_b, gather(x_mid))
        mix = forward(rows_b, match_b, gates_b, weights_b)
        x_last = (x_mid.astype(F32) + shared_out(x_mid, weights_b) + mix).astype(BF16)
        dy_b = dispatch(match_b, gather(d_out))
        du_sum, dw1_b, dw3_b, dw2_b, back_b = backward(rows_b, dy_b, match_b, gates_b, weights_b)
        d_mid = (d_out.astype(F32) + shared_grad(x_mid, d_out, weights_b) + du_sum).astype(BF16)
        again = lax.optimization_barrier((x_in, du_sum))[0]
        rows_a = dispatch(match_a, gather(again))
        dy_a = dispatch(match_a, gather(d_mid))
        du_sum, dw1_a, dw3_a, dw2_a, back_a = backward(rows_a, dy_a, match_a, gates_a, weights_a)
        d_first = (d_mid.astype(F32) + shared_grad(x_in, d_mid, weights_a) + du_sum).astype(BF16)
        return (x_last, d_first, dw1_a, dw3_a, dw2_a, dw1_b, dw3_b, dw2_b,
                gate_grads(back_a, idx_a), gate_grads(back_b, idx_b))

    in_specs = (token_spec,) * 6 + layer_specs + layer_specs
    out_specs = (token_spec, token_spec) + (grad_spec,) * 6 + (token_spec, token_spec)
    return jax.shard_map(device_step, mesh=mesh, in_specs=in_specs, out_specs=out_specs, check_vma=False)
```

```python
import functools

import jax
import jax.numpy as jnp
from jax import lax
from jax.experimental import pallas as pl
from jax.experimental.pallas import tpu as pltpu
from jax.sharding import PartitionSpec as P

F32 = jnp.float32
BF16 = jnp.bfloat16
MESH = pl.DeviceIdType.MESH
VMEM_BYTES = 66_900_000
TAB = 8


def slot_capacity(tokens, n_experts, top_k):
    return top_k * ((2 * tokens + n_experts - 1) // n_experts)


def dot(a, b):
    return jnp.dot(a, b, preferred_element_type=F32)


def dot_nt(a, b):
    return lax.dot_general(a, b, (((1,), (1,)), ((), ())), preferred_element_type=F32)


def dot_tn(a, b):
    return lax.dot_general(a, b, (((0,), (0,)), ((), ())), preferred_element_type=F32)


def swiglu_grads(pre_gate, pre_up, d_hidden):
    sigma = jax.nn.sigmoid(pre_gate)
    d_gate = d_hidden * pre_up * sigma * (1.0 + pre_gate * (1.0 - sigma))
    d_up = d_hidden * pre_gate * sigma
    return d_gate.astype(BF16), d_up.astype(BF16)


def hidden_of(rows, w_gate, w_up):
    pre_gate = dot_nt(rows, w_gate)
    pre_up = dot_nt(rows, w_up)
    return pre_gate, pre_up, (pre_gate * jax.nn.sigmoid(pre_gate) * pre_up).astype(BF16)


def when(cond, body):
    if isinstance(cond, bool):
        if cond:
            body()
    else:
        pl.when(cond)(body)


class Place:
    def __init__(self, nz):
        self.nz = nz
        self.me = lax.axis_index('ep')
        self.z = self.me // 2
        self.c = self.me % 2

    def chip(self, offset):
        return lax.rem(self.z + offset + 2 * self.nz, self.nz)

    def source(self, offset, rel):
        return self.chip(offset) * 2 + lax.rem(self.c + rel, 2)

    def device(self, offset, rel=0):
        return {'ep': self.source(offset, rel)}


class Gather:
    def __init__(self, place, buf, pieces, sems):
        self.p, self.buf, self.pieces = place, buf, pieces
        self.ss, self.rs, self.xs, self.xr = sems
        self.rows = buf.shape[1] // pieces

    def far(self, di, h):
        near = self.p.nz // 2 - 1
        return near + 1 if di == h else near

    def at(self, offset, rel, h):
        return self.buf.at[self.p.source(offset, rel), pl.ds(h * self.rows, self.rows)]

    def hop(self, di, h, k, offset):
        d = 1 - 2 * di
        ref = self.at(offset, 0, h)
        return pltpu.make_async_remote_copy(ref, ref, self.ss.at[di, h, k - 1], self.rs.at[di, h, k - 1],
                                            device_id=self.p.device(d), device_id_type=MESH)

    def send(self, di, h, k):
        d = 1 - 2 * di
        return self.hop(di, h, k, -d * (k - 1))

    def recv(self, di, h, k):
        d = 1 - 2 * di
        return self.hop(di, h, k, -d * k)

    def cross(self, h, offset, rel=0):
        ref = self.at(offset, rel, h)
        roff = lax.rem(offset + self.p.nz, self.p.nz) if not isinstance(offset, int) else offset % self.p.nz
        return pltpu.make_async_remote_copy(ref, ref, self.xs.at[roff, h], self.xr.at[roff, h],
                                            device_id=self.p.device(0, 1), device_id_type=MESH)

    def start(self):
        for h in range(self.pieces):
            for di in range(2):
                self.send(di, h, 1).start()
        for h in range(self.pieces):
            self.cross(h, 0).start()

    def step(self, k):
        for h in range(self.pieces):
            for di in range(2):
                d = 1 - 2 * di
                far = self.far(di, h)

                def arrive(di=di, h=h, d=d, far=far):
                    self.recv(di, h, k).wait_recv()
                    when(k + 1 <= far, lambda: self.send(di, h, k + 1).start())
                    self.cross(h, -d * k).start()

                when(k <= far, arrive)

    def wait_cross(self, offset):
        for h in range(self.pieces):
            self.cross(h, offset, 1).wait_recv()

    def drain(self):
        for h in range(self.pieces):
            for di in range(2):
                for k in range(1, self.far(di, h) + 1):
                    self.send(di, h, k).wait_send()
            for roff in range(self.p.nz):
                self.cross(h, roff).wait_send()


class Scatter:
    def __init__(self, place, acc, out, sib, box, sems):
        self.p, self.acc, self.out, self.sib, self.box = place, acc, out, sib, box
        self.xs, self.xr, self.ss, self.rs = sems
        self.half = acc.shape[1] // 2
        self.steps = place.nz - 1

    def cross(self, roff, slot):
        return pltpu.make_async_remote_copy(self.out.at[slot], self.sib.at[roff], self.xs.at[roff], self.xr.at[roff],
                                            device_id=self.p.device(0, 1), device_id_type=MESH)

    def merge(self, roff):
        self.cross(roff, 0).wait_recv()

        def add(i, carry):
            rows = pl.ds(i * 64, 64)
            self.acc[roff, rows, :] += self.sib[roff, rows, :]
            return carry

        lax.fori_loop(0, self.acc.shape[1] // 64, add, 0)

    def reach(self, i):
        return self.p.nz // 2 - (i + 1) // 2

    def roff(self, di, i):
        r = self.reach(i)
        return r if di == 0 else self.p.nz - r

    def side(self, di, i):
        return (i + di) % 2

    def hop(self, di, i):
        rows = pl.ds(self.side(di, i) * self.half, self.half)
        return pltpu.make_async_remote_copy(self.acc.at[self.roff(di, i), rows], self.box.at[di, i],
                                            self.ss.at[di, i], self.rs.at[di, i],
                                            device_id=self.p.device(1 - 2 * di), device_id_type=MESH)

    def take(self, di, i, roff):
        self.hop(di, i).wait_recv()
        first = self.side(di, i) * self.half

        def add(j, carry):
            rows = pl.ds(pl.multiple_of(first + j * 64, 64), 64)
            self.acc[roff, rows, :] += self.box[di, i, pl.ds(j * 64, 64), :]
            return carry

        lax.fori_loop(0, self.half // 64, add, 0)

    def step(self, i):
        for di in range(2):
            if isinstance(i, int) and i < 2:
                self.hop(di, i).start()
            else:
                self.take(di, i - 2, self.roff(di, i))
                self.hop(di, i).start()

    def finish(self):
        for i in (self.steps - 2, self.steps - 1):
            for di in range(2):
                self.take(di, i, 0)

    def drain(self):
        for i in range(self.steps):
            for di in range(2):
                self.hop(di, i).wait_send()


def stage_kernel(names, dims, fwd, bwd, layer, *refs):
    r = dict(zip(names, refs))
    nz, n_local, cap, tokens = dims
    p = Place(nz)
    n_dev = 2 * nz
    far = nz // 2
    slots = n_local * cap

    loads = [(r['x_in'], r['xg'].at[p.me], r['lsem'].at[0])]
    if bwd:
        loads.append((r['dy_in'], r['dg'].at[p.me], r['lsem'].at[1]))
        loads.append((r['tab_in'], r['tab'], r['lsem'].at[2]))
    else:
        loads.append((r['tab_in'], r['tab'].at[p.me], r['lsem'].at[2]))
    own = [pltpu.make_async_copy(*args) for args in loads]
    weights = [pltpu.make_async_copy(r[n + '_in'], r[n], r['wsem'].at[i])
               for i, n in enumerate(('ws1', 'ws3', 'ws2', 'w1', 'w3', 'w2'))]
    for copy in own + weights:
        copy.start()

    barrier = pltpu.get_barrier_semaphore()
    if bwd:
        for o in range(1, n_dev):
            pl.semaphore_signal(barrier, inc=1, device_id={'ep': lax.rem(p.me + o, n_dev)}, device_id_type=MESH)
        pl.semaphore_wait(barrier, n_dev - 1)
    else:
        for peer in (p.device(1), p.device(-1), p.device(0, 1)):
            pl.semaphore_signal(barrier, inc=1, device_id=peer, device_id_type=MESH)
        pl.semaphore_wait(barrier, 3)
    for copy in own:
        copy.wait()

    streams = []
    if not bwd:
        streams.append(Gather(p, r['tab'], 1, (r['ts'], r['tr'], r['txs'], r['txr'])))
    streams.append(Gather(p, r['xg'], 2, (r['gs'], r['gr'], r['gxs'], r['gxr'])))
    if bwd:
        streams.append(Gather(p, r['dg'], 2, (r['ds'], r['dr'], r['dxs'], r['dxr'])))
    for st in streams:
        st.start()

    tri = (lax.broadcasted_iota(jnp.int32, (tokens, tokens), 0)
           < lax.broadcasted_iota(jnp.int32, (tokens, tokens), 1))
    r['tri'][...] = jnp.where(tri, 1.0, 0.0).astype(BF16)

    for copy in weights[:3]:
        copy.wait()
    x_own = r['xg'][p.me]
    s_gate, s_up, s_hidden = hidden_of(x_own, r['ws1'][...], r['ws3'][...])
    if fwd:
        r['sh'][...] = dot(s_hidden, r['ws2'][...]) + x_own.astype(F32)
    if bwd:
        d_own = r['dg'][p.me]
        d_sg, d_su = swiglu_grads(s_gate, s_up, dot_nt(d_own, r['ws2'][...]))
        r['shd'][...] = dot(d_sg, r['ws1'][...]) + dot(d_su, r['ws3'][...]) + d_own.astype(F32)
    for copy in weights[3:]:
        copy.wait()

    sf = sb = None
    if fwd:
        sf = Scatter(p, r['facc'], r['fout'], r['fsib'], r['fbox'], (r['fxs'], r['fxr'], r['fss'], r['frs']))
    if bwd:
        sb = Scatter(p, r['bacc'], r['bout'], r['bsib'], r['bbox'], (r['bxs'], r['bxr'], r['bss'], r['brs']))

    def offset_of(k, q):
        sign = 1 - 2 * (q // 2)
        return k * sign

    def pos_rows(base, n):
        return pl.ds(pl.multiple_of(base * cap, 16), n * cap)

    def dispatch(k, base, n):
        def body(q, carry):
            s = p.source(offset_of(k, q), q % 2)
            ids = r['tab'][s, pl.ds(layer * TAB, TAB), :]
            gates = r['tab'][s, pl.ds((2 + layer) * TAB, TAB), :]
            used, gate = [], []
            for e in range(n_local):
                hit = ids == (p.me * n_local + e).astype(F32)
                used.append(jnp.max(jnp.where(hit, 1.0, 0.0), axis=0, keepdims=True))
                gate.append(jnp.sum(jnp.where(hit, gates, 0.0), axis=0, keepdims=True))
            zeros = jnp.zeros((8 - n_local, tokens), F32)
            used = jnp.concatenate(used + [zeros], axis=0)
            gate = jnp.concatenate(gate + [zeros], axis=0)
            rank = dot(used.astype(BF16), r['tri'][...])
            slot = jnp.where(used > 0, rank, -1.0)
            pos = base + q
            r['grow'][pos] = gate
            rows48 = lax.broadcasted_iota(jnp.int32, (cap, tokens), 0).astype(F32)
            for e in range(n_local):
                match = rows48 == slot[e:e + 1, :]
                r['pall'][pos, e * cap:(e + 1) * cap, :] = jnp.where(match, 1.0, 0.0).astype(BF16)
                if bwd:
                    col = jnp.sum(jnp.where(match, gate[e:e + 1, :], 0.0), axis=1, keepdims=True)
                    r['gcol'][e, pl.ds(pl.multiple_of(q * cap, 16), cap), :] = jnp.broadcast_to(col, (cap, 128))
            pick = r['pall'][pos]
            rows = dot(pick, r['xg'][s]).astype(BF16)
            for e in range(n_local):
                r['xr'][e, pos_rows(pos, 1), :] = rows[e * cap:(e + 1) * cap]
            if bwd:
                rows = dot(pick, r['dg'][s]).astype(BF16)
                for e in range(n_local):
                    r['dyr'][e, pos_rows(pos, 1), :] = rows[e * cap:(e + 1) * cap]
            return carry

        lax.fori_loop(0, n, body, 0)

    def expert_fwd(base, n):
        def body(e, carry):
            hidden = hidden_of(r['xr'][e, pos_rows(base, n), :], r['w1'][e], r['w3'][e])[2]
            r['rowbuf'][e, 0:n * cap, :] = dot(hidden, r['w2'][e]).astype(BF16)
            return carry

        lax.fori_loop(0, n_local, body, 0)

    def combine(k, base, n, sc, gated):
        for ridx in range(n // 2):
            offset = offset_of(k, 2 * ridx)
            roff = offset % nz if isinstance(offset, int) else lax.rem(offset + nz, nz)
            if not (isinstance(k, int) and k == 0):
                prev = k - 1
                if ridx == 0:
                    sc.cross(prev, 0).wait_send()
                else:
                    when(prev > 0, lambda: sc.cross(lax.rem(nz - prev, nz), 1).wait_send())
            for rel in (1, 0):
                q = 2 * ridx + rel
                pos = base + q
                rows = jnp.concatenate([r['rowbuf'][e, q * cap:(q + 1) * cap, :] for e in range(n_local)], axis=0)
                if gated:
                    pick = r['pall'][pos].astype(F32)
                    gate = r['grow'][pos]
                    part = None
                    for _ in range(3):
                        term = gate.astype(BF16).astype(F32)
                        gate = gate - term
                        wide = jnp.concatenate(
                            [pick[e * cap:(e + 1) * cap] * term[e:e + 1, :] for e in range(n_local)], axis=0)
                        one = dot_tn(wide.astype(BF16), rows)
                        part = one if part is None else part + one
                else:
                    part = dot_tn(r['pall'][pos], rows)
                if rel == 1:
                    sc.out[ridx] = part
                else:
                    sc.acc[roff] = part
            sc.cross(roff, ridx).start()

    def expert_bwd(base, n):
        def body(e, carry):
            span = pos_rows(base, n)
            here = slice(0, n * cap)
            pre_gate, pre_up, hidden = hidden_of(r['xr'][e, span, :], r['w1'][e], r['w3'][e])
            dy = r['dyr'][e, span, :]
            projected = dot_nt(dy, r['w2'][e])
            gcol = r['gcol'][e, here, 0:1]
            dgate = jnp.sum(hidden.astype(F32) * projected, axis=1, keepdims=True)
            r['gcol'][e, here, :] = jnp.broadcast_to(dgate, (n * cap, 128))
            r['dyr'][e, span, :] = (gcol * dy.astype(F32)).astype(BF16)
            da_gate, da_up = swiglu_grads(pre_gate, pre_up, gcol * projected)
            r['h'][e, span, :] = hidden
            r['da1'][e, span, :] = da_gate
            r['da3'][e, span, :] = da_up
            du = dot(da_gate, r['w1'][e]) + dot(da_up, r['w3'][e])
            r['rowbuf'][e, here, :] = du.astype(BF16)
            return carry

        lax.fori_loop(0, n_local, body, 0)

    def gate_rows(k, base, n):
        def body(q, carry):
            s = p.source(offset_of(k, q), q % 2)
            pos = base + q
            rows = []
            for e in range(n_local):
                col = r['gcol'][e, pl.ds(pl.multiple_of(q * cap, 16), cap), 0:1]
                pick = r['pall'][pos, e * cap:(e + 1) * cap, :].astype(F32)
                rows.append(jnp.sum(pick * col, axis=0, keepdims=True))
            wide = jnp.concatenate(rows, axis=0)
            half = tokens // 2
            r['dgout'][s] = jnp.concatenate([wide[:, :half], wide[:, half:]], axis=0)
            return carry

        lax.fori_loop(0, n, body, 0)

    def group(k, base, n, between=None):
        offsets = [offset_of(k, 2 * i) for i in range(n // 2)]
        for st in streams:
            for offset in offsets:
                st.wait_cross(offset)
        dispatch(k, base, n)
        if fwd:
            expert_fwd(base, n)
            combine(k, base, n, sf, True)
        if between is not None:
            between()
        if bwd:
            expert_bwd(base, n)
            combine(k, base, n, sb, False)
            gate_rows(k, base, n)

    def steps(k):
        for st in streams:
            st.step(k)

    def chain_start(sc):
        sc.merge(far)
        sc.step(0)
        sc.merge(far - 1)
        sc.merge(nz - far + 1)
        sc.step(1)

    group(0, 0, 2)

    def middle(k, carry):
        steps(k)
        group(k, 2 + (k - 1) * 4, 4)
        return carry

    lax.fori_loop(1, far, middle, 0)
    steps(far)
    group(far, n_dev - 2, 2, (lambda: chain_start(sf)) if fwd and bwd else None)
    if fwd and not bwd:
        chain_start(sf)
    if bwd:
        chain_start(sb)

    def grad_copy(o, wait):
        to = lax.rem(p.me + o, n_dev)
        landed = r['dgin'].at[lax.rem(p.me - o + n_dev, n_dev)] if wait else r['dgin'].at[p.me]
        return pltpu.make_async_remote_copy(r['dgout'].at[to], landed, r['as'].at[o], r['ar'].at[o],
                                            device_id={'ep': to}, device_id_type=MESH)

    if bwd:
        def push(o, carry):
            grad_copy(o, False).start()
            return carry

        lax.fori_loop(1, n_dev, push, 0)

    scatters = [sc for sc in (sf, sb) if sc is not None]

    def put(e):
        return [pltpu.make_async_copy(r['g' + n], r[n + '_out'].at[e], r['osem'].at[i])
                for i, n in enumerate(('dw1', 'dw3', 'dw2'))]

    def weight_grads(e):
        copies = put(e)

        @pl.when(e > 0)
        def _():
            for copy in copies:
                copy.wait()

        rows = r['xr'][e]
        r['gdw1'][...] = dot_tn(r['da1'][e], rows)
        r['gdw3'][...] = dot_tn(r['da3'][e], rows)
        r['gdw2'][...] = dot_tn(r['h'][e], r['dyr'][e])
        for copy in copies:
            copy.start()

    def ring(i, carry):
        for sc in scatters:
            @pl.when(i % 2 == 1)
            def _():
                sc.merge(sc.roff(0, i))
                sc.merge(sc.roff(1, i))
            sc.step(i)
        if bwd:
            @pl.when(i - 2 < n_local)
            def _():
                weight_grads(i - 2)
        return carry

    lax.fori_loop(2, nz - 1, ring, 0)
    for sc in scatters:
        sc.merge(0)
    if bwd:
        r['dgin'][p.me] = r['dgout'][p.me]

        def pull(o, carry):
            grad_copy(o, True).wait_recv()
            return carry

        lax.fori_loop(1, n_dev, pull, 0)
        ids = r['tab'][p.me, pl.ds(layer * TAB, TAB), :]

        def collect(dev, total):
            block = r['dgin'][dev]
            wide = jnp.concatenate([block[:n_local], block[n_local:]], axis=1)
            for e in range(n_local):
                total += jnp.where(ids == (dev * n_local + e).astype(F32), wide[e:e + 1, :], 0.0)
            return total

        r['dgate_out'][...] = lax.fori_loop(0, n_dev, collect, jnp.zeros((TAB, tokens), F32))
    if fwd:
        sf.finish()
        r['y_out'][...] = (r['sh'][...] + sf.acc[0]).astype(BF16)
    if bwd:
        sb.finish()
        r['dx_out'][...] = (r['shd'][...] + sb.acc[0]).astype(BF16)
        for copy in put(n_local - 1):
            copy.wait()

        def done(o, carry):
            grad_copy(o, False).wait_send()
            return carry

        lax.fori_loop(1, n_dev, done, 0)
    else:
        keep = pltpu.make_async_copy(r['tab'], r['tab_out'], r['osem'].at[0])
        keep.start()
        keep.wait()
    for st in streams:
        st.drain()
    for sc in scatters:
        sc.cross(far, 0).wait_send()
        sc.cross(nz - far + 1, 1).wait_send()
        sc.drain()


def stage(mesh_axis, dims, fwd, bwd, layer, x, dy, tab, weights, cid):
    nz, n_local, cap, tokens = dims
    n_dev = 2 * nz
    d = x.shape[1]
    w1, w3, w2, ws1, ws3, ws2 = weights
    f = w1.shape[1]
    slots = n_local * cap
    rows = n_dev * cap
    any_spec = pl.BlockSpec(memory_space=pl.ANY)
    vmem_spec = pl.BlockSpec(memory_space=pltpu.VMEM)
    dma = pltpu.SemaphoreType.DMA
    ins = {'x_in': x}
    if bwd:
        ins['dy_in'] = dy
    ins.update({'tab_in': tab, 'ws1_in': ws1, 'ws3_in': ws3, 'ws2_in': ws2, 'w1_in': w1, 'w3_in': w3, 'w2_in': w2})
    outs = {}
    if fwd:
        outs['y_out'] = ((tokens, d), BF16, vmem_spec)
    if bwd:
        outs['dx_out'] = ((tokens, d), BF16, vmem_spec)
        outs['dw1_out'] = (w1.shape, F32, any_spec)
        outs['dw3_out'] = (w3.shape, F32, any_spec)
        outs['dw2_out'] = (w2.shape, F32, any_spec)
        outs['dgate_out'] = ((TAB, tokens), F32, vmem_spec)
    else:
        outs['tab_out'] = ((n_dev,) + tab.shape, F32, any_spec)
    scratch = {
        'lsem': dma((3,)), 'wsem': dma((6,)), 'osem': dma((3,)),
        'xg': pltpu.VMEM((n_dev, tokens, d), BF16),
        'tab': pltpu.VMEM((n_dev, 4 * TAB, tokens), F32),
        'tri': pltpu.VMEM((tokens, tokens), BF16),
        'pall': pltpu.VMEM((n_dev, slots, tokens), BF16),
        'grow': pltpu.VMEM((n_dev, 8, tokens), F32),
        'xr': pltpu.VMEM((n_local, rows, d), BF16),
        'rowbuf': pltpu.VMEM((n_local, 4 * cap, d), BF16),
        'ws1': pltpu.VMEM(ws1.shape, BF16), 'ws3': pltpu.VMEM(ws3.shape, BF16), 'ws2': pltpu.VMEM(ws2.shape, BF16),
        'w1': pltpu.VMEM(w1.shape, BF16), 'w3': pltpu.VMEM(w3.shape, BF16), 'w2': pltpu.VMEM(w2.shape, BF16),
        'gs': dma((2, 2, nz // 2)), 'gr': dma((2, 2, nz // 2)), 'gxs': dma((nz, 2)), 'gxr': dma((nz, 2)),
    }
    if not bwd:
        scratch.update({'ts': dma((2, 1, nz // 2)), 'tr': dma((2, 1, nz // 2)), 'txs': dma((nz, 1)), 'txr': dma((nz, 1))})
    for on, tag in ((fwd, 'f'), (bwd, 'b')):
        if on:
            scratch.update({
                tag + 'acc': pltpu.VMEM((nz, tokens, d), F32),
                tag + 'out': pltpu.VMEM((2, tokens, d), F32),
                tag + 'sib': pltpu.VMEM((nz, tokens, d), F32),
                tag + 'box': pltpu.VMEM((2, nz - 1, tokens // 2, d), F32),
                tag + 'xs': dma((nz,)), tag + 'xr': dma((nz,)),
                tag + 'ss': dma((2, nz - 1)), tag + 'rs': dma((2, nz - 1)),
            })
    if fwd:
        scratch['sh'] = pltpu.VMEM((tokens, d), F32)
    if bwd:
        scratch.update({
            'dg': pltpu.VMEM((n_dev, tokens, d), BF16),
            'ds': dma((2, 2, nz // 2)), 'dr': dma((2, 2, nz // 2)), 'dxs': dma((nz, 2)), 'dxr': dma((nz, 2)),
            'shd': pltpu.VMEM((tokens, d), F32),
            'dyr': pltpu.VMEM((n_local, rows, d), BF16),
            'gcol': pltpu.VMEM((n_local, 4 * cap, 128), F32),
            'h': pltpu.VMEM((n_local, rows, f), BF16),
            'da1': pltpu.VMEM((n_local, rows, f), BF16),
            'da3': pltpu.VMEM((n_local, rows, f), BF16),
            'gdw1': pltpu.VMEM((f, d), F32), 'gdw3': pltpu.VMEM((f, d), F32), 'gdw2': pltpu.VMEM((f, d), F32),
            'dgout': pltpu.VMEM((n_dev, 2 * n_local, tokens // 2), F32),
            'dgin': pltpu.VMEM((n_dev, 2 * n_local, tokens // 2), F32),
            'as': dma((n_dev,)), 'ar': dma((n_dev,)),
        })
    names = list(ins) + list(outs) + list(scratch)
    result = pl.pallas_call(
        functools.partial(stage_kernel, names, dims, fwd, bwd, layer),
        out_shape=[jax.ShapeDtypeStruct(s, t) for s, t, _ in outs.values()],
        in_specs=[any_spec] * len(ins),
        out_specs=[spec for _, _, spec in outs.values()],
        scratch_shapes=list(scratch.values()),
        compiler_params=pltpu.CompilerParams(collective_id=cid, has_side_effects=True, vmem_limit_bytes=VMEM_BYTES),
        name='stage_' + ('f' if fwd else '') + ('b' if bwd else '') + '_ab'[1 + layer],
    )(*ins.values())
    return dict(zip(outs, result))


def solution(mesh):
    group_size = mesh.shape['ep']
    token_spec = P(('dp', 'ep'), None)
    expert_spec = P('ep', None, None)
    shared_spec = P(None, None)
    grad_spec = P(('dp', 'ep'), None, None)
    layer_specs = (expert_spec,) * 3 + (shared_spec,) * 3

    def device_step(x_in, d_out, idx_a, gate_a, idx_b, gate_b,
                    w1_a, w3_a, w2_a, ws1_a, ws3_a, ws2_a,
                    w1_b, w3_b, w2_b, ws1_b, ws3_b, ws2_b):
        def turned(w):
            return jnp.swapaxes(w, -1, -2)

        weights_a = (turned(w1_a), turned(w3_a), w2_a, turned(ws1_a), turned(ws3_a), ws2_a)
        weights_b = (turned(w1_b), turned(w3_b), w2_b, turned(ws1_b), turned(ws3_b), ws2_b)
        tokens, top_k = idx_a.shape
        n_local = w1_a.shape[0]
        dims = (group_size // 2, n_local, slot_capacity(tokens, n_local * group_size, top_k), tokens)

        def padded(values, fill):
            return jnp.pad(values.astype(F32), ((0, 0), (0, TAB - top_k)), constant_values=fill)

        table = jnp.concatenate([padded(idx_a, -1.0), padded(idx_b, -1.0), padded(gate_a, 0.0), padded(gate_b, 0.0)],
                                axis=1).T
        first = stage('ep', dims, True, False, 0, x_in, None, table, weights_a, 0)
        x_mid, tables = first['y_out'], first['tab_out']
        second = stage('ep', dims, True, True, 1, x_mid, d_out, tables, weights_b, 1)
        third = stage('ep', dims, False, True, 0, x_in, second['dx_out'], tables, weights_a, 2)
        return (second['y_out'], third['dx_out'],
                turned(third['dw1_out']), turned(third['dw3_out']), third['dw2_out'],
                turned(second['dw1_out']), turned(second['dw3_out']), second['dw2_out'],
                third['dgate_out'][:top_k].T, second['dgate_out'][:top_k].T)

    in_specs = (token_spec,) * 6 + layer_specs + layer_specs
    out_specs = (token_spec, token_spec) + (grad_spec,) * 6 + (token_spec, token_spec)
    return jax.shard_map(device_step, mesh=mesh, in_specs=in_specs, out_specs=out_specs, check_vma=False)
```

```python
import functools

import jax
import jax.numpy as jnp
from jax import lax
from jax.experimental import pallas as pl
from jax.experimental.pallas import tpu as pltpu
from jax.sharding import PartitionSpec as P

F32 = jnp.float32
BF16 = jnp.bfloat16
MESH = pl.DeviceIdType.MESH
VMEM_BYTES = 66_900_000
TAB = 8


def slot_capacity(tokens, n_experts, top_k):
    return top_k * ((2 * tokens + n_experts - 1) // n_experts)


def dot(a, b):
    return jnp.dot(a, b, preferred_element_type=F32)


def dot_nt(a, b):
    return lax.dot_general(a, b, (((1,), (1,)), ((), ())), preferred_element_type=F32)


def dot_tn(a, b):
    return lax.dot_general(a, b, (((0,), (0,)), ((), ())), preferred_element_type=F32)


def swiglu_grads(pre_gate, pre_up, d_hidden):
    sigma = jax.nn.sigmoid(pre_gate)
    d_gate = d_hidden * pre_up * sigma * (1.0 + pre_gate * (1.0 - sigma))
    d_up = d_hidden * pre_gate * sigma
    return d_gate.astype(BF16), d_up.astype(BF16)


def hidden_of(rows, w_gate, w_up):
    pre_gate = dot_nt(rows, w_gate)
    pre_up = dot_nt(rows, w_up)
    return pre_gate, pre_up, (pre_gate * jax.nn.sigmoid(pre_gate) * pre_up).astype(BF16)


def when(cond, body):
    if isinstance(cond, bool):
        if cond:
            body()
    else:
        pl.when(cond)(body)


class Place:
    def __init__(self, nz):
        self.nz = nz
        self.me = lax.axis_index('ep')
        self.z = self.me // 2
        self.c = self.me % 2

    def chip(self, offset):
        return lax.rem(self.z + offset + 2 * self.nz, self.nz)

    def source(self, offset, rel):
        return self.chip(offset) * 2 + lax.rem(self.c + rel, 2)

    def device(self, offset, rel=0):
        return {'ep': self.source(offset, rel)}


class Gather:
    def __init__(self, place, buf, pieces, sems):
        self.p, self.buf, self.pieces = place, buf, pieces
        self.ss, self.rs, self.xs, self.xr = sems
        self.rows = buf.shape[1] // pieces

    def far(self, di, h):
        near = self.p.nz // 2 - 1
        return near + 1 if di == h else near

    def at(self, offset, rel, h):
        return self.buf.at[self.p.source(offset, rel), pl.ds(h * self.rows, self.rows)]

    def hop(self, di, h, k, offset):
        d = 1 - 2 * di
        ref = self.at(offset, 0, h)
        return pltpu.make_async_remote_copy(ref, ref, self.ss.at[di, h, k - 1], self.rs.at[di, h, k - 1],
                                            device_id=self.p.device(d), device_id_type=MESH)

    def send(self, di, h, k):
        d = 1 - 2 * di
        return self.hop(di, h, k, -d * (k - 1))

    def recv(self, di, h, k):
        d = 1 - 2 * di
        return self.hop(di, h, k, -d * k)

    def cross(self, h, offset, rel=0):
        ref = self.at(offset, rel, h)
        roff = lax.rem(offset + self.p.nz, self.p.nz) if not isinstance(offset, int) else offset % self.p.nz
        return pltpu.make_async_remote_copy(ref, ref, self.xs.at[roff, h], self.xr.at[roff, h],
                                            device_id=self.p.device(0, 1), device_id_type=MESH)

    def start(self):
        for h in range(self.pieces):
            for di in range(2):
                self.send(di, h, 1).start()
        for h in range(self.pieces):
            self.cross(h, 0).start()

    def step(self, k):
        for h in range(self.pieces):
            for di in range(2):
                d = 1 - 2 * di
                far = self.far(di, h)

                def arrive(di=di, h=h, d=d, far=far):
                    self.recv(di, h, k).wait_recv()
                    when(k + 1 <= far, lambda: self.send(di, h, k + 1).start())
                    self.cross(h, -d * k).start()

                when(k <= far, arrive)

    def wait_cross(self, offset):
        for h in range(self.pieces):
            self.cross(h, offset, 1).wait_recv()

    def drain(self):
        for h in range(self.pieces):
            for di in range(2):
                for k in range(1, self.far(di, h) + 1):
                    self.send(di, h, k).wait_send()
            for roff in range(self.p.nz):
                self.cross(h, roff).wait_send()


class Scatter:
    def __init__(self, place, acc, out, sib, box, sems):
        self.p, self.acc, self.out, self.sib, self.box = place, acc, out, sib, box
        self.xs, self.xr, self.ss, self.rs = sems
        self.half = acc.shape[1] // 2
        self.steps = place.nz - 1

    def cross(self, roff, slot):
        return pltpu.make_async_remote_copy(self.out.at[slot], self.sib.at[roff], self.xs.at[roff], self.xr.at[roff],
                                            device_id=self.p.device(0, 1), device_id_type=MESH)

    def merge(self, roff):
        self.cross(roff, 0).wait_recv()

        def add(i, carry):
            rows = pl.ds(i * 64, 64)
            self.acc[roff, rows, :] += self.sib[roff, rows, :]
            return carry

        lax.fori_loop(0, self.acc.shape[1] // 64, add, 0)

    def reach(self, i):
        return self.p.nz // 2 - (i + 1) // 2

    def roff(self, di, i):
        r = self.reach(i)
        return r if di == 0 else self.p.nz - r

    def side(self, di, i):
        return (i + di) % 2

    def hop(self, di, i):
        rows = pl.ds(self.side(di, i) * self.half, self.half)
        return pltpu.make_async_remote_copy(self.acc.at[self.roff(di, i), rows], self.box.at[di, i],
                                            self.ss.at[di, i], self.rs.at[di, i],
                                            device_id=self.p.device(1 - 2 * di), device_id_type=MESH)

    def take(self, di, i, roff):
        self.hop(di, i).wait_recv()
        first = self.side(di, i) * self.half

        def add(j, carry):
            rows = pl.ds(pl.multiple_of(first + j * 64, 64), 64)
            self.acc[roff, rows, :] += self.box[di, i, pl.ds(j * 64, 64), :]
            return carry

        lax.fori_loop(0, self.half // 64, add, 0)

    def begin(self, i):
        for roff in sorted({self.roff(0, i), self.roff(1, i)}):
            self.merge(roff)
        for di in range(2):
            self.hop(di, i).start()

    def step(self, i):
        for di in range(2):
            self.take(di, i - 2, self.roff(di, i))
            self.hop(di, i).start()

    def merge_for(self, i):
        self.merge(self.roff(0, i))
        self.merge(self.roff(1, i))

    def free(self, frees):
        for slot, roff, cond in frees:
            when(cond, functools.partial(lambda slot, roff: self.cross(roff, slot).wait_send(), slot, roff))

    def finish(self):
        for i in (self.steps - 2, self.steps - 1):
            for di in range(2):
                self.take(di, i, 0)

    def drain(self):
        for i in range(self.steps):
            for di in range(2):
                self.hop(di, i).wait_send()


def stage_kernel(names, dims, fwd, bwd, layer, *refs):
    r = dict(zip(names, refs))
    nz, n_local, cap, tokens = dims
    p = Place(nz)
    n_dev = 2 * nz
    far = nz // 2
    slots = n_local * cap

    loads = [(r['x_in'], r['xg'].at[p.me], r['lsem'].at[0])]
    if bwd:
        loads.append((r['dy_in'], r['dg'].at[p.me], r['lsem'].at[1]))
        loads.append((r['tab_in'], r['tab'], r['lsem'].at[2]))
    else:
        loads.append((r['tab_in'], r['tab'].at[p.me], r['lsem'].at[2]))
    own = [pltpu.make_async_copy(*args) for args in loads]
    weights = [pltpu.make_async_copy(r[n + '_in'], r[n], r['wsem'].at[i])
               for i, n in enumerate(('ws1', 'ws3', 'ws2', 'w1', 'w3', 'w2'))]
    for copy in own + weights:
        copy.start()

    barrier = pltpu.get_barrier_semaphore()
    if bwd:
        for o in range(1, n_dev):
            pl.semaphore_signal(barrier, inc=1, device_id={'ep': lax.rem(p.me + o, n_dev)}, device_id_type=MESH)
        pl.semaphore_wait(barrier, n_dev - 1)
    else:
        for peer in (p.device(1), p.device(-1), p.device(0, 1)):
            pl.semaphore_signal(barrier, inc=1, device_id=peer, device_id_type=MESH)
        pl.semaphore_wait(barrier, 3)
    for copy in own:
        copy.wait()

    streams = []
    if not bwd:
        streams.append(Gather(p, r['tab'], 1, (r['ts'], r['tr'], r['txs'], r['txr'])))
    streams.append(Gather(p, r['xg'], 2, (r['gs'], r['gr'], r['gxs'], r['gxr'])))
    x_streams, dy_stream = list(streams), None
    if bwd:
        dy_stream = Gather(p, r['dg'], 2, (r['ds'], r['dr'], r['dxs'], r['dxr']))
        streams.append(dy_stream)
    for st in streams:
        st.start()

    tri = (lax.broadcasted_iota(jnp.int32, (tokens, tokens), 0)
           < lax.broadcasted_iota(jnp.int32, (tokens, tokens), 1))
    r['tri'][...] = jnp.where(tri, 1.0, 0.0).astype(BF16)

    for copy in weights[:3]:
        copy.wait()
    x_own = r['xg'][p.me]
    s_gate, s_up, s_hidden = hidden_of(x_own, r['ws1'][...], r['ws3'][...])
    if fwd:
        r['sh'][...] = dot(s_hidden, r['ws2'][...]) + x_own.astype(F32)
    if bwd:
        d_own = r['dg'][p.me]
        d_sg, d_su = swiglu_grads(s_gate, s_up, dot_nt(d_own, r['ws2'][...]))
        r['shd'][...] = dot(d_sg, r['ws1'][...]) + dot(d_su, r['ws3'][...]) + d_own.astype(F32)
    for copy in weights[3:]:
        copy.wait()

    sf = sb = None
    if fwd:
        sf = Scatter(p, r['facc'], r['fout'], r['fsib'], r['fbox'], (r['fxs'], r['fxr'], r['fss'], r['frs']))
    if bwd:
        sb = Scatter(p, r['bacc'], r['bout'], r['bsib'], r['bbox'], (r['bxs'], r['bxr'], r['bss'], r['brs']))

    def offset_of(k, q):
        sign = 1 - 2 * (q // 2)
        return k * sign

    def pos_rows(base, n):
        return pl.ds(pl.multiple_of(base * cap, 16), n * cap)

    def dispatch(k, base, n):
        def body(q, carry):
            s = p.source(offset_of(k, q), q % 2)
            ids = r['tab'][s, pl.ds(layer * TAB, TAB), :]
            gates = r['tab'][s, pl.ds((2 + layer) * TAB, TAB), :]
            used, gate = [], []
            for e in range(n_local):
                hit = ids == (p.me * n_local + e).astype(F32)
                used.append(jnp.max(jnp.where(hit, 1.0, 0.0), axis=0, keepdims=True))
                gate.append(jnp.sum(jnp.where(hit, gates, 0.0), axis=0, keepdims=True))
            zeros = jnp.zeros((8 - n_local, tokens), F32)
            used = jnp.concatenate(used + [zeros], axis=0)
            gate = jnp.concatenate(gate + [zeros], axis=0)
            rank = dot(used.astype(BF16), r['tri'][...])
            slot = jnp.where(used > 0, rank, -1.0)
            pos = base + q
            r['grow'][pos] = gate
            rows48 = lax.broadcasted_iota(jnp.int32, (cap, tokens), 0).astype(F32)
            for e in range(n_local):
                match = rows48 == slot[e:e + 1, :]
                r['pall'][pos, e * cap:(e + 1) * cap, :] = jnp.where(match, 1.0, 0.0).astype(BF16)
            rows = dot(r['pall'][pos], r['xg'][s]).astype(BF16)
            for e in range(n_local):
                r['xr'][e, pos_rows(pos, 1), :] = rows[e * cap:(e + 1) * cap]
            return carry

        lax.fori_loop(0, n, body, 0)

    def dispatch_dy(k, base, n):
        def body(q, carry):
            s = p.source(offset_of(k, q), q % 2)
            pos = base + q
            pick = r['pall'][pos]
            gate = r['grow'][pos]
            rows = dot(pick, r['dg'][s]).astype(BF16)
            for e in range(n_local):
                wide = pick[e * cap:(e + 1) * cap].astype(F32) * gate[e:e + 1, :]
                col = jnp.sum(wide, axis=1, keepdims=True)
                r['gcol'][e, pl.ds(pl.multiple_of(q * cap, 16), cap), :] = jnp.broadcast_to(col, (cap, 128))
                r['dyr'][e, pos_rows(pos, 1), :] = rows[e * cap:(e + 1) * cap]
            return carry

        lax.fori_loop(0, n, body, 0)

    def expert_fwd(base, n):
        def body(e, carry):
            hidden = hidden_of(r['xr'][e, pos_rows(base, n), :], r['w1'][e], r['w3'][e])[2]
            r['rowbuf'][e, 0:n * cap, :] = dot(hidden, r['w2'][e]).astype(BF16)
            return carry

        lax.fori_loop(0, n_local, body, 0)

    def combine(k, base, n, sc, gated, frees):
        sc.free(frees)
        for ridx in range(n // 2):
            offset = offset_of(k, 2 * ridx)
            roff = offset % nz if isinstance(offset, int) else lax.rem(offset + nz, nz)
            for rel in (1, 0):
                q = 2 * ridx + rel
                pos = base + q
                rows = jnp.concatenate([r['rowbuf'][e, q * cap:(q + 1) * cap, :] for e in range(n_local)], axis=0)
                if gated:
                    pick = r['pall'][pos].astype(F32)
                    gate = r['grow'][pos]
                    part = None
                    for _ in range(3):
                        term = gate.astype(BF16).astype(F32)
                        gate = gate - term
                        wide = jnp.concatenate(
                            [pick[e * cap:(e + 1) * cap] * term[e:e + 1, :] for e in range(n_local)], axis=0)
                        one = dot_tn(wide.astype(BF16), rows)
                        part = one if part is None else part + one
                else:
                    part = dot_tn(r['pall'][pos], rows)
                if rel == 1:
                    sc.out[ridx] = part
                else:
                    sc.acc[roff] = part
            sc.cross(roff, ridx).start()

    def expert_bwd(base, n):
        def body(e, carry):
            span = pos_rows(base, n)
            here = slice(0, n * cap)
            pre_gate, pre_up, hidden = hidden_of(r['xr'][e, span, :], r['w1'][e], r['w3'][e])
            dy = r['dyr'][e, span, :]
            projected = dot_nt(dy, r['w2'][e])
            gcol = r['gcol'][e, here, 0:1]
            dgate = jnp.sum(hidden.astype(F32) * projected, axis=1, keepdims=True)
            r['gcol'][e, here, :] = jnp.broadcast_to(dgate, (n * cap, 128))
            r['dyr'][e, span, :] = (gcol * dy.astype(F32)).astype(BF16)
            da_gate, da_up = swiglu_grads(pre_gate, pre_up, gcol * projected)
            r['h'][e, span, :] = hidden
            r['da1'][e, span, :] = da_gate
            r['da3'][e, span, :] = da_up
            du = dot(da_gate, r['w1'][e]) + dot(da_up, r['w3'][e])
            r['rowbuf'][e, here, :] = du.astype(BF16)
            return carry

        lax.fori_loop(0, n_local, body, 0)

    def gate_rows(k, base, n):
        def body(q, carry):
            s = p.source(offset_of(k, q), q % 2)
            pos = base + q
            rows = []
            for e in range(n_local):
                col = r['gcol'][e, pl.ds(pl.multiple_of(q * cap, 16), cap), 0:1]
                pick = r['pall'][pos, e * cap:(e + 1) * cap, :].astype(F32)
                rows.append(jnp.sum(pick * col, axis=0, keepdims=True))
            wide = jnp.concatenate(rows, axis=0)
            half = tokens // 2
            r['dgout'][s] = jnp.concatenate([wide[:, :half], wide[:, half:]], axis=0)
            return carry

        lax.fori_loop(0, n, body, 0)

    def spot(k):
        if isinstance(k, int) and k in (0, far):
            return (0 if k == 0 else n_dev - 2), 2
        return 2 + (k - 1) * 4, 4

    def arrived(st, k, n):
        for i in range(n // 2):
            st.wait_cross(offset_of(k, 2 * i))

    def group_x(k, frees):
        base, n = spot(k)
        for st in x_streams:
            arrived(st, k, n)
        dispatch(k, base, n)
        if fwd:
            expert_fwd(base, n)
            combine(k, base, n, sf, True, frees)

    def group_dy(k, frees):
        base, n = spot(k)
        arrived(dy_stream, k, n)
        dispatch_dy(k, base, n)
        expert_bwd(base, n)
        combine(k, base, n, sb, False, frees)
        gate_rows(k, base, n)

    def steps(k):
        for st in streams:
            st.step(k)

    def upward(k, first):
        return [(0, k - 1, k > first), (1, lax.rem(nz - (k - 1), nz), k > max(first, 1))]

    first = 0 if bwd else 1
    if bwd:
        group_x(0, [])
        if not fwd:
            group_dy(0, [])

    def middle(k, carry):
        steps(k)
        group_x(k, upward(k, first))
        if not fwd:
            group_dy(k, upward(k, first))
        return carry

    lax.fori_loop(1, far, middle, 0)
    steps(far)
    lead = sf if fwd else sb
    lead.begin(1)
    last = [(0, far - 1, True)]
    group_x(far, last)
    if not fwd:
        group_dy(far, last)
    lead.begin(0)
    left = [(lead, 0, far), (lead, 1, nz - far + 1)]

    def grad_copy(o, wait):
        to = lax.rem(p.me + o, n_dev)
        landed = r['dgin'].at[lax.rem(p.me - o + n_dev, n_dev)] if wait else r['dgin'].at[p.me]
        return pltpu.make_async_remote_copy(r['dgout'].at[to], landed, r['as'].at[o], r['ar'].at[o],
                                            device_id={'ep': to}, device_id_type=MESH)

    def push(o, carry):
        grad_copy(o, False).start()
        return carry

    scatters = [sc for sc in (sf, sb) if sc is not None]

    def put(e):
        return [pltpu.make_async_copy(r['g' + n], r[n + '_out'].at[e], r['osem'].at[i])
                for i, n in enumerate(('dw1', 'dw3', 'dw2'))]

    def weight_grads(e):
        copies = put(e)

        @pl.when(e > 0)
        def _():
            for copy in copies:
                copy.wait()

        rows = r['xr'][e]
        r['gdw1'][...] = dot_tn(r['da1'][e], rows)
        r['gdw3'][...] = dot_tn(r['da3'][e], rows)
        r['gdw2'][...] = dot_tn(r['h'][e], r['dyr'][e])
        for copy in copies:
            copy.start()

    def order(j):
        return 3 + 2 * (j // 2) - j % 2

    def turn(sc, j):
        i = order(j)
        when(j % 2 == 0, lambda: sc.merge_for(i))
        sc.step(i)

    turns = nz - 4
    if not bwd:
        turn(sf, 0)
        group_x(0, [(0, far, True)])
        left[0] = (sf, 0, 0)
        for j in range(1, turns):
            turn(sf, j)
        sf.step(nz - 2)
    else:
        if fwd:
            group_dy(far, [])
            turn(sf, 0)
            group_dy(far - 1, [(0, far, True)])
            turn(sf, 1)
            sb.begin(1)
            sb.begin(0)

            def outward(j, carry):
                k = far - j
                group_dy(k, [(0, k + 1, True), (1, nz - (k + 1), True)])
                turn(sf, j)
                return carry

            lax.fori_loop(2, far, outward, 0)
            group_dy(0, [(0, 1, True)])
            left += [(sb, 0, 0), (sb, 1, nz - 1)]
            sf.step(nz - 2)
        lax.fori_loop(1, n_dev, push, 0)

        def ring(j, carry):
            turn(sb, j)
            weight_grads(j)
            return carry

        lax.fori_loop(0, turns, ring, 0)
        sb.step(nz - 2)
    for sc in scatters:
        sc.merge(0)
    if bwd:
        r['dgin'][p.me] = r['dgout'][p.me]

        def pull(o, carry):
            grad_copy(o, True).wait_recv()
            return carry

        lax.fori_loop(1, n_dev, pull, 0)
        ids = r['tab'][p.me, pl.ds(layer * TAB, TAB), :]

        def collect(dev, total):
            block = r['dgin'][dev]
            wide = jnp.concatenate([block[:n_local], block[n_local:]], axis=1)
            for e in range(n_local):
                total += jnp.where(ids == (dev * n_local + e).astype(F32), wide[e:e + 1, :], 0.0)
            return total

        r['dgate_out'][...] = lax.fori_loop(0, n_dev, collect, jnp.zeros((TAB, tokens), F32))
    if fwd:
        sf.finish()
        r['y_out'][...] = (r['sh'][...] + sf.acc[0]).astype(BF16)
    if bwd:
        sb.finish()
        r['dx_out'][...] = (r['shd'][...] + sb.acc[0]).astype(BF16)
        for copy in put(n_local - 1):
            copy.wait()

        def done(o, carry):
            grad_copy(o, False).wait_send()
            return carry

        lax.fori_loop(1, n_dev, done, 0)
    else:
        keep = pltpu.make_async_copy(r['tab'], r['tab_out'], r['osem'].at[0])
        keep.start()
        keep.wait()
    for st in streams:
        st.drain()
    for sc, slot, roff in left:
        sc.cross(roff, slot).wait_send()
    for sc in scatters:
        sc.drain()


def stage(mesh_axis, dims, fwd, bwd, layer, x, dy, tab, weights, cid):
    nz, n_local, cap, tokens = dims
    n_dev = 2 * nz
    d = x.shape[1]
    w1, w3, w2, ws1, ws3, ws2 = weights
    f = w1.shape[1]
    slots = n_local * cap
    rows = n_dev * cap
    any_spec = pl.BlockSpec(memory_space=pl.ANY)
    vmem_spec = pl.BlockSpec(memory_space=pltpu.VMEM)
    dma = pltpu.SemaphoreType.DMA
    ins = {'x_in': x}
    if bwd:
        ins['dy_in'] = dy
    ins.update({'tab_in': tab, 'ws1_in': ws1, 'ws3_in': ws3, 'ws2_in': ws2, 'w1_in': w1, 'w3_in': w3, 'w2_in': w2})
    outs = {}
    if fwd:
        outs['y_out'] = ((tokens, d), BF16, vmem_spec)
    if bwd:
        outs['dx_out'] = ((tokens, d), BF16, vmem_spec)
        outs['dw1_out'] = (w1.shape, F32, any_spec)
        outs['dw3_out'] = (w3.shape, F32, any_spec)
        outs['dw2_out'] = (w2.shape, F32, any_spec)
        outs['dgate_out'] = ((TAB, tokens), F32, vmem_spec)
    else:
        outs['tab_out'] = ((n_dev,) + tab.shape, F32, any_spec)
    scratch = {
        'lsem': dma((3,)), 'wsem': dma((6,)), 'osem': dma((3,)),
        'xg': pltpu.VMEM((n_dev, tokens, d), BF16),
        'tab': pltpu.VMEM((n_dev, 4 * TAB, tokens), F32),
        'tri': pltpu.VMEM((tokens, tokens), BF16),
        'pall': pltpu.VMEM((n_dev, slots, tokens), BF16),
        'grow': pltpu.VMEM((n_dev, 8, tokens), F32),
        'xr': pltpu.VMEM((n_local, rows, d), BF16),
        'rowbuf': pltpu.VMEM((n_local, 4 * cap, d), BF16),
        'ws1': pltpu.VMEM(ws1.shape, BF16), 'ws3': pltpu.VMEM(ws3.shape, BF16), 'ws2': pltpu.VMEM(ws2.shape, BF16),
        'w1': pltpu.VMEM(w1.shape, BF16), 'w3': pltpu.VMEM(w3.shape, BF16), 'w2': pltpu.VMEM(w2.shape, BF16),
        'gs': dma((2, 2, nz // 2)), 'gr': dma((2, 2, nz // 2)), 'gxs': dma((nz, 2)), 'gxr': dma((nz, 2)),
    }
    if not bwd:
        scratch.update({'ts': dma((2, 1, nz // 2)), 'tr': dma((2, 1, nz // 2)), 'txs': dma((nz, 1)), 'txr': dma((nz, 1))})
    for on, tag in ((fwd, 'f'), (bwd, 'b')):
        if on:
            scratch.update({
                tag + 'acc': pltpu.VMEM((nz, tokens, d), F32),
                tag + 'out': pltpu.VMEM((2, tokens, d), F32),
                tag + 'sib': pltpu.VMEM((nz, tokens, d), F32),
                tag + 'box': pltpu.VMEM((2, nz - 1, tokens // 2, d), F32),
                tag + 'xs': dma((nz,)), tag + 'xr': dma((nz,)),
                tag + 'ss': dma((2, nz - 1)), tag + 'rs': dma((2, nz - 1)),
            })
    if fwd:
        scratch['sh'] = pltpu.VMEM((tokens, d), F32)
    if bwd:
        scratch.update({
            'dg': pltpu.VMEM((n_dev, tokens, d), BF16),
            'ds': dma((2, 2, nz // 2)), 'dr': dma((2, 2, nz // 2)), 'dxs': dma((nz, 2)), 'dxr': dma((nz, 2)),
            'shd': pltpu.VMEM((tokens, d), F32),
            'dyr': pltpu.VMEM((n_local, rows, d), BF16),
            'gcol': pltpu.VMEM((n_local, 4 * cap, 128), F32),
            'h': pltpu.VMEM((n_local, rows, f), BF16),
            'da1': pltpu.VMEM((n_local, rows, f), BF16),
            'da3': pltpu.VMEM((n_local, rows, f), BF16),
            'gdw1': pltpu.VMEM((f, d), F32), 'gdw3': pltpu.VMEM((f, d), F32), 'gdw2': pltpu.VMEM((f, d), F32),
            'dgout': pltpu.VMEM((n_dev, 2 * n_local, tokens // 2), F32),
            'dgin': pltpu.VMEM((n_dev, 2 * n_local, tokens // 2), F32),
            'as': dma((n_dev,)), 'ar': dma((n_dev,)),
        })
    names = list(ins) + list(outs) + list(scratch)
    result = pl.pallas_call(
        functools.partial(stage_kernel, names, dims, fwd, bwd, layer),
        out_shape=[jax.ShapeDtypeStruct(s, t) for s, t, _ in outs.values()],
        in_specs=[any_spec] * len(ins),
        out_specs=[spec for _, _, spec in outs.values()],
        scratch_shapes=list(scratch.values()),
        compiler_params=pltpu.CompilerParams(collective_id=cid, has_side_effects=True, vmem_limit_bytes=VMEM_BYTES),
        name='stage_' + ('f' if fwd else '') + ('b' if bwd else '') + '_ab'[1 + layer],
    )(*ins.values())
    return dict(zip(outs, result))


def settle_kernel(pieces, *refs):
    n = len(refs[:-2]) // 3
    ins, outs, bufs = refs[:n], refs[n:2 * n], refs[2 * n:3 * n]
    get_sem, put_sem = refs[-2:]
    gets, puts = [], []
    for i in range(n):
        for j in range(pieces[i]):
            rows = pl.ds(j * (ins[i].shape[0] // pieces[i]), ins[i].shape[0] // pieces[i])
            at = len(gets)
            gets.append(pltpu.make_async_copy(ins[i].at[rows], bufs[i].at[rows], get_sem.at[at]))
            puts.append(pltpu.make_async_copy(bufs[i].at[rows], outs[i].at[rows], put_sem.at[at]))
    for get in gets:
        get.start()
    for get, put in zip(gets, puts):
        get.wait()
        put.start()
    for put in puts:
        put.wait()


def settle(arrays):
    pieces = [a.shape[0] if a.ndim == 3 else 1 for a in arrays]
    total = sum(pieces)
    any_spec = pl.BlockSpec(memory_space=pl.ANY)
    return pl.pallas_call(
        functools.partial(settle_kernel, pieces),
        out_shape=[jax.ShapeDtypeStruct(a.shape, a.dtype) for a in arrays],
        in_specs=[any_spec] * len(arrays),
        out_specs=[any_spec] * len(arrays),
        scratch_shapes=[pltpu.VMEM(a.shape, a.dtype) for a in arrays]
        + [pltpu.SemaphoreType.DMA((total,)), pltpu.SemaphoreType.DMA((total,))],
        compiler_params=pltpu.CompilerParams(vmem_limit_bytes=VMEM_BYTES),
        name='settle',
    )(*arrays)


def solution(mesh):
    group_size = mesh.shape['ep']
    token_spec = P(('dp', 'ep'), None)
    expert_spec = P('ep', None, None)
    shared_spec = P(None, None)
    grad_spec = P(('dp', 'ep'), None, None)
    layer_specs = (expert_spec,) * 3 + (shared_spec,) * 3

    def device_step(x_in, d_out, idx_a, gate_a, idx_b, gate_b,
                    w1_a, w3_a, w2_a, ws1_a, ws3_a, ws2_a,
                    w1_b, w3_b, w2_b, ws1_b, ws3_b, ws2_b):
        def turned(w):
            return jnp.swapaxes(w, -1, -2)

        weights_a = (turned(w1_a), turned(w3_a), w2_a, turned(ws1_a), turned(ws3_a), ws2_a)
        weights_b = (turned(w1_b), turned(w3_b), w2_b, turned(ws1_b), turned(ws3_b), ws2_b)
        tokens, top_k = idx_a.shape
        n_local = w1_a.shape[0]
        dims = (group_size // 2, n_local, slot_capacity(tokens, n_local * group_size, top_k), tokens)

        def padded(values, fill):
            return jnp.pad(values.astype(F32), ((0, 0), (0, TAB - top_k)), constant_values=fill)

        table = jnp.concatenate([padded(idx_a, -1.0), padded(idx_b, -1.0), padded(gate_a, 0.0), padded(gate_b, 0.0)],
                                axis=1).T
        first = stage('ep', dims, True, False, 0, x_in, None, table, weights_a, 0)
        x_mid, tables = first['y_out'], first['tab_out']
        second = stage('ep', dims, True, True, 1, x_mid, d_out, tables, weights_b, 1)
        third = stage('ep', dims, False, True, 0, x_in, second['dx_out'], tables, weights_a, 2)
        x_last, d_first, *grads = settle(
            [second['y_out'], third['dx_out']]
            + [layer[n] for layer in (third, second) for n in ('dw1_out', 'dw3_out', 'dw2_out')])
        for at in (0, 1, 3, 4):
            grads[at] = turned(grads[at])
        return (x_last, d_first, *grads, third['dgate_out'][:top_k].T, second['dgate_out'][:top_k].T)

    in_specs = (token_spec,) * 6 + layer_specs + layer_specs
    out_specs = (token_spec, token_spec) + (grad_spec,) * 6 + (token_spec, token_spec)
    return jax.shard_map(device_step, mesh=mesh, in_specs=in_specs, out_specs=out_specs, check_vma=False)
```

```python
import functools

import jax
import jax.numpy as jnp
from jax import lax
from jax.experimental import pallas as pl
from jax.experimental.pallas import tpu as pltpu
from jax.sharding import PartitionSpec as P

F32 = jnp.float32
BF16 = jnp.bfloat16
MESH = pl.DeviceIdType.MESH
VMEM_BYTES = 67_000_000
TAB = 8


def slot_capacity(tokens, n_experts, top_k):
    return top_k * ((2 * tokens + n_experts - 1) // n_experts)


def dot(a, b):
    return jnp.dot(a, b, preferred_element_type=F32)


def dot_nt(a, b):
    return lax.dot_general(a, b, (((1,), (1,)), ((), ())), preferred_element_type=F32)


def dot_tn(a, b):
    return lax.dot_general(a, b, (((0,), (0,)), ((), ())), preferred_element_type=F32)


def swiglu_grads(pre_gate, pre_up, d_hidden):
    sigma = jax.nn.sigmoid(pre_gate)
    d_gate = d_hidden * pre_up * sigma * (1.0 + pre_gate * (1.0 - sigma))
    d_up = d_hidden * pre_gate * sigma
    return d_gate.astype(BF16), d_up.astype(BF16)


def hidden_of(rows, w_gate, w_up):
    pre_gate = dot_nt(rows, w_gate)
    pre_up = dot_nt(rows, w_up)
    return pre_gate, pre_up, (pre_gate * jax.nn.sigmoid(pre_gate) * pre_up).astype(BF16)


def when(cond, body):
    if isinstance(cond, bool):
        if cond:
            body()
    else:
        pl.when(cond)(body)


class Place:
    def __init__(self, nz):
        self.nz = nz
        self.me = lax.axis_index('ep')
        self.z = self.me // 2
        self.c = self.me % 2

    def chip(self, offset):
        return lax.rem(self.z + offset + 2 * self.nz, self.nz)

    def source(self, offset, rel):
        return self.chip(offset) * 2 + lax.rem(self.c + rel, 2)

    def device(self, offset, rel=0):
        return {'ep': self.source(offset, rel)}


class Gather:
    def __init__(self, place, buf, pieces, sems):
        self.p, self.buf, self.pieces = place, buf, pieces
        self.ss, self.rs, self.xs, self.xr = sems
        self.rows = buf.shape[1] // pieces

    def far(self, di, h):
        near = self.p.nz // 2 - 1
        return near + 1 if di == h else near

    def at(self, offset, rel, h):
        return self.buf.at[self.p.source(offset, rel), pl.ds(h * self.rows, self.rows)]

    def hop(self, di, h, k, offset):
        d = 1 - 2 * di
        ref = self.at(offset, 0, h)
        return pltpu.make_async_remote_copy(ref, ref, self.ss.at[di, h, k - 1], self.rs.at[di, h, k - 1],
                                            device_id=self.p.device(d), device_id_type=MESH)

    def send(self, di, h, k):
        d = 1 - 2 * di
        return self.hop(di, h, k, -d * (k - 1))

    def recv(self, di, h, k):
        d = 1 - 2 * di
        return self.hop(di, h, k, -d * k)

    def cross(self, h, offset, rel=0):
        ref = self.at(offset, rel, h)
        roff = lax.rem(offset + self.p.nz, self.p.nz) if not isinstance(offset, int) else offset % self.p.nz
        return pltpu.make_async_remote_copy(ref, ref, self.xs.at[roff, h], self.xr.at[roff, h],
                                            device_id=self.p.device(0, 1), device_id_type=MESH)

    def start(self):
        for h in range(self.pieces):
            for di in range(2):
                self.send(di, h, 1).start()
        for h in range(self.pieces):
            self.cross(h, 0).start()

    def step(self, k):
        for h in range(self.pieces):
            for di in range(2):
                d = 1 - 2 * di
                far = self.far(di, h)

                def arrive(di=di, h=h, d=d, far=far):
                    self.recv(di, h, k).wait_recv()
                    when(k + 1 <= far, lambda: self.send(di, h, k + 1).start())
                    self.cross(h, -d * k).start()

                when(k <= far, arrive)

    def wait_cross(self, offset):
        for h in range(self.pieces):
            self.cross(h, offset, 1).wait_recv()

    def drain(self):
        for h in range(self.pieces):
            for di in range(2):
                for k in range(1, self.far(di, h) + 1):
                    self.send(di, h, k).wait_send()
            for roff in range(self.p.nz):
                self.cross(h, roff).wait_send()


class Scatter:
    def __init__(self, place, acc, out, sib, box, sems):
        self.p, self.acc, self.out, self.sib, self.box = place, acc, out, sib, box
        self.xs, self.xr, self.ss, self.rs = sems
        self.half = acc.shape[1] // 2
        self.steps = place.nz - 1

    def cross(self, roff, slot):
        return pltpu.make_async_remote_copy(self.out.at[slot], self.sib.at[roff], self.xs.at[roff], self.xr.at[roff],
                                            device_id=self.p.device(0, 1), device_id_type=MESH)

    def merge(self, roff):
        self.cross(roff, 0).wait_recv()

        def add(i, carry):
            rows = pl.ds(i * 64, 64)
            self.acc[roff, rows, :] += self.sib[roff, rows, :]
            return carry

        lax.fori_loop(0, self.acc.shape[1] // 64, add, 0)

    def reach(self, i):
        return self.p.nz // 2 - (i + 1) // 2

    def roff(self, di, i):
        r = self.reach(i)
        return r if di == 0 else self.p.nz - r

    def side(self, di, i):
        return (i + di) % 2

    def hop(self, di, i):
        rows = pl.ds(self.side(di, i) * self.half, self.half)
        return pltpu.make_async_remote_copy(self.acc.at[self.roff(di, i), rows], self.box.at[di, i],
                                            self.ss.at[di, i], self.rs.at[di, i],
                                            device_id=self.p.device(1 - 2 * di), device_id_type=MESH)

    def take(self, di, i, roff):
        self.hop(di, i).wait_recv()
        first = self.side(di, i) * self.half

        def add(j, carry):
            rows = pl.ds(pl.multiple_of(first + j * 64, 64), 64)
            self.acc[roff, rows, :] += self.box[di, i, pl.ds(j * 64, 64), :]
            return carry

        lax.fori_loop(0, self.half // 64, add, 0)

    def begin(self, i):
        for roff in sorted({self.roff(0, i), self.roff(1, i)}):
            self.merge(roff)
        for di in range(2):
            self.hop(di, i).start()

    def step(self, i):
        for di in range(2):
            self.take(di, i - 2, self.roff(di, i))
            self.hop(di, i).start()

    def merge_for(self, i):
        self.merge(self.roff(0, i))
        self.merge(self.roff(1, i))

    def free(self, frees):
        for slot, roff, cond in frees:
            when(cond, functools.partial(lambda slot, roff: self.cross(roff, slot).wait_send(), slot, roff))

    def finish(self):
        for i in (self.steps - 2, self.steps - 1):
            for di in range(2):
                self.take(di, i, 0)

    def drain(self):
        for i in range(self.steps):
            for di in range(2):
                self.hop(di, i).wait_send()


def step_kernel(names, dims, *refs):
    r = dict(zip(names, refs))
    nz, n_local, cap, tokens = dims
    p = Place(nz)
    n_dev = 2 * nz
    far = nz // 2

    def load_weights(tag):
        return [pltpu.make_async_copy(r[n + tag], r[n], r['wsem'].at[i])
                for i, n in enumerate(('ws1', 'ws3', 'ws2', 'w1', 'w3', 'w2'))]

    def load_own(name, buf, i):
        return pltpu.make_async_copy(r[name], r[buf].at[p.me], r['lsem'].at[i])

    own = [load_own('tab_in', 'tab', 0), load_own('x_in', 'xg', 1)]
    own_dy = load_own('dy_in', 'dg', 2)
    for copy in own + [own_dy]:
        copy.start()

    barrier = pltpu.get_barrier_semaphore()
    for o in range(1, n_dev):
        pl.semaphore_signal(barrier, inc=1, device_id={'ep': lax.rem(p.me + o, n_dev)}, device_id_type=MESH)
    pl.semaphore_wait(barrier, n_dev - 1)

    tabs = Gather(p, r['tab'], 1, (r['ts'], r['tr'], r['txs'], r['txr']))
    xs = Gather(p, r['xg'], 2, (r['gs'], r['gr'], r['gxs'], r['gxr']))
    ds = Gather(p, r['dg'], 2, (r['ds'], r['dr'], r['dxs'], r['dxr']))
    sf = Scatter(p, r['facc'], r['fout'], r['fsib'], r['fbox'], (r['fxs'], r['fxr'], r['fss'], r['frs']))
    sb = Scatter(p, r['bacc'], r['bout'], r['bsib'], r['bbox'], (r['bxs'], r['bxr'], r['bss'], r['brs']))

    for copy in own:
        copy.wait()
    tabs.start()
    xs.start()

    tri = (lax.broadcasted_iota(jnp.int32, (tokens, tokens), 0)
           < lax.broadcasted_iota(jnp.int32, (tokens, tokens), 1))
    r['tri'][...] = jnp.where(tri, 1.0, 0.0).astype(BF16)

    def offset_of(k, q):
        return k * (1 - 2 * (q // 2))

    def pos_rows(base, n):
        return pl.ds(pl.multiple_of(base * cap, 16), n * cap)

    def spot(k):
        if isinstance(k, int) and k in (0, far):
            return (0 if k == 0 else n_dev - 2), 2
        return 2 + (k - 1) * 4, 4

    def arrived(st, k):
        for i in range(spot(k)[1] // 2):
            st.wait_cross(offset_of(k, 2 * i))

    def route(k, layer):
        base, n = spot(k)

        def body(q, carry):
            s = p.source(offset_of(k, q), q % 2)
            ids = r['tab'][s, pl.ds(layer * TAB, TAB), :]
            gates = r['tab'][s, pl.ds((2 + layer) * TAB, TAB), :]
            used, gate = [], []
            for e in range(n_local):
                hit = ids == (p.me * n_local + e).astype(F32)
                used.append(jnp.max(jnp.where(hit, 1.0, 0.0), axis=0, keepdims=True))
                gate.append(jnp.sum(jnp.where(hit, gates, 0.0), axis=0, keepdims=True))
            zeros = jnp.zeros((8 - n_local, tokens), F32)
            used = jnp.concatenate(used + [zeros], axis=0)
            rank = dot(used.astype(BF16), r['tri'][...])
            slot = jnp.where(used > 0, rank, -1.0)
            pos = base + q
            r['grow'][pos] = jnp.concatenate(gate + [zeros], axis=0)
            place = lax.broadcasted_iota(jnp.int32, (cap, tokens), 0).astype(F32)
            for e in range(n_local):
                r['pall'][pos, e * cap:(e + 1) * cap, :] = jnp.where(place == slot[e:e + 1, :], 1.0, 0.0).astype(BF16)
            return carry

        lax.fori_loop(0, n, body, 0)

    def dispatch(k):
        base, n = spot(k)

        def body(q, carry):
            s = p.source(offset_of(k, q), q % 2)
            pos = base + q
            rows = dot(r['pall'][pos], r['xg'][s]).astype(BF16)
            for e in range(n_local):
                r['xr'][e, pos_rows(pos, 1), :] = rows[e * cap:(e + 1) * cap]
            return carry

        lax.fori_loop(0, n, body, 0)

    def dispatch_dy(k):
        base, n = spot(k)

        def body(q, carry):
            s = p.source(offset_of(k, q), q % 2)
            pos = base + q
            pick = r['pall'][pos]
            gate = r['grow'][pos]
            rows = dot(pick, r['dg'][s]).astype(BF16)
            for e in range(n_local):
                wide = pick[e * cap:(e + 1) * cap].astype(F32) * gate[e:e + 1, :]
                col = jnp.sum(wide, axis=1, keepdims=True)
                r['gcol'][e, pl.ds(pl.multiple_of(q * cap, 16), cap), :] = jnp.broadcast_to(col, (cap, 128))
                r['dyr'][e, pos_rows(pos, 1), :] = rows[e * cap:(e + 1) * cap]
            return carry

        lax.fori_loop(0, n, body, 0)

    def expert_fwd(k):
        base, n = spot(k)

        def body(e, carry):
            hidden = hidden_of(r['xr'][e, pos_rows(base, n), :], r['w1'][e], r['w3'][e])[2]
            r['rowbuf'][e, 0:n * cap, :] = dot(hidden, r['w2'][e]).astype(BF16)
            return carry

        lax.fori_loop(0, n_local, body, 0)

    def expert_bwd(k):
        base, n = spot(k)

        def body(e, carry):
            span = pos_rows(base, n)
            here = slice(0, n * cap)
            pre_gate, pre_up, hidden = hidden_of(r['xr'][e, span, :], r['w1'][e], r['w3'][e])
            dy = r['dyr'][e, span, :]
            projected = dot_nt(dy, r['w2'][e])
            gcol = r['gcol'][e, here, 0:1]
            dgate = jnp.sum(hidden.astype(F32) * projected, axis=1, keepdims=True)
            r['gcol'][e, here, :] = jnp.broadcast_to(dgate, (n * cap, 128))
            r['dyr'][e, span, :] = (gcol * dy.astype(F32)).astype(BF16)
            da_gate, da_up = swiglu_grads(pre_gate, pre_up, gcol * projected)
            r['h'][e, span, :] = hidden
            r['da1'][e, span, :] = da_gate
            r['da3'][e, span, :] = da_up
            du = dot(da_gate, r['w1'][e]) + dot(da_up, r['w3'][e])
            r['rowbuf'][e, here, :] = du.astype(BF16)
            return carry

        lax.fori_loop(0, n_local, body, 0)

    def combine(k, sc, gated, frees):
        base, n = spot(k)
        sc.free(frees)
        for ridx in range(n // 2):
            offset = offset_of(k, 2 * ridx)
            roff = offset % nz if isinstance(offset, int) else lax.rem(offset + nz, nz)
            for rel in (1, 0):
                q = 2 * ridx + rel
                pos = base + q
                rows = jnp.concatenate([r['rowbuf'][e, q * cap:(q + 1) * cap, :] for e in range(n_local)], axis=0)
                if gated:
                    pick = r['pall'][pos].astype(F32)
                    gate = r['grow'][pos]
                    part = None
                    for _ in range(3):
                        term = gate.astype(BF16).astype(F32)
                        gate = gate - term
                        wide = jnp.concatenate(
                            [pick[e * cap:(e + 1) * cap] * term[e:e + 1, :] for e in range(n_local)], axis=0)
                        one = dot_tn(wide.astype(BF16), rows)
                        part = one if part is None else part + one
                else:
                    part = dot_tn(r['pall'][pos], rows)
                if rel == 1:
                    sc.out[ridx] = part
                else:
                    sc.acc[roff] = part
            sc.cross(roff, ridx).start()

    def gate_rows(k, dgout):
        base, n = spot(k)

        def body(q, carry):
            s = p.source(offset_of(k, q), q % 2)
            pos = base + q
            rows = []
            for e in range(n_local):
                col = r['gcol'][e, pl.ds(pl.multiple_of(q * cap, 16), cap), 0:1]
                pick = r['pall'][pos, e * cap:(e + 1) * cap, :].astype(F32)
                rows.append(jnp.sum(pick * col, axis=0, keepdims=True))
            wide = jnp.concatenate(rows, axis=0)
            half = tokens // 2
            dgout[s] = jnp.concatenate([wide[:, :half], wide[:, half:]], axis=0)
            return carry

        lax.fori_loop(0, n, body, 0)

    def upward(k, first):
        return [(0, k - 1, k > first), (1, lax.rem(nz - (k - 1), nz), k > max(first, 1))]

    def order(j):
        return 3 + 2 * (j // 2) - j % 2

    def turn(sc, j):
        i = order(j)
        when(j % 2 == 0, lambda: sc.merge_for(i))
        sc.step(i)

    turns = nz - 4

    def phase(fwd, bwd, layer, tag, early, emit_y, emit_dx):
        weights = load_weights(tag)
        for copy in weights:
            copy.start()
        streams = [xs, ds] if bwd else [tabs, xs]
        x_streams = [xs] if bwd else [tabs, xs]
        dgout, dgin, a_ss, a_rs = (r[n] for n in ('dgout', 'dgin' + tag, 'as' + tag, 'ar' + tag)) if bwd else (None,) * 4

        for copy in weights[:3]:
            copy.wait()
        x_own = r['xg'][p.me]
        s_gate, s_up, s_hidden = hidden_of(x_own, r['ws1'][...], r['ws3'][...])
        if fwd:
            r['sh'][...] = dot(s_hidden, r['ws2'][...]) + x_own.astype(F32)
        if bwd:
            d_own = r['dg'][p.me]
            d_sg, d_su = swiglu_grads(s_gate, s_up, dot_nt(d_own, r['ws2'][...]))
            r['shd'][...] = dot(d_sg, r['ws1'][...]) + dot(d_su, r['ws3'][...]) + d_own.astype(F32)
            route(0, layer)
            lax.fori_loop(1, far, lambda k, c: (route(k, layer), c)[1], 0)
            route(far, layer)
        for copy in weights[3:]:
            copy.wait()

        def group_x(k, frees):
            for st in x_streams:
                arrived(st, k)
            if not bwd:
                route(k, layer)
            dispatch(k)
            if fwd:
                expert_fwd(k)
                combine(k, sf, True, frees)

        def group_dy(k, frees):
            arrived(ds, k)
            dispatch_dy(k)
            expert_bwd(k)
            combine(k, sb, False, frees)
            gate_rows(k, dgout)

        def steps(k):
            for st in streams:
                st.step(k)

        first = 0 if bwd else 1
        if bwd:
            group_x(0, [])
            if not fwd:
                group_dy(0, [])

        def middle(k, carry):
            steps(k)
            group_x(k, upward(k, first))
            if not fwd:
                group_dy(k, upward(k, first))
            return carry

        lax.fori_loop(1, far, middle, 0)
        steps(far)
        lead = sf if fwd else sb
        lead.begin(1)
        last = [(0, far - 1, True)]
        group_x(far, last)
        if not fwd:
            group_dy(far, last)
        lead.begin(0)
        left = [(lead, 0, far), (lead, 1, nz - far + 1)]

        def grad_copy(o, wait):
            to = lax.rem(p.me + o, n_dev)
            landed = dgin.at[lax.rem(p.me - o + n_dev, n_dev)] if wait else dgin.at[p.me]
            return pltpu.make_async_remote_copy(dgout.at[to], landed, a_ss.at[o], a_rs.at[o],
                                                device_id={'ep': to}, device_id_type=MESH)

        def put(e):
            return [pltpu.make_async_copy(r['g' + n], r[n + tag].at[e], r['osem'].at[i])
                    for i, n in enumerate(('dw1', 'dw3', 'dw2'))]

        def weight_grads(e):
            copies = put(e)

            @pl.when(e > 0)
            def _():
                for copy in copies:
                    copy.wait()

            rows = r['xr'][e]
            r['gdw1'][...] = dot_tn(r['da1'][e], rows)
            r['gdw3'][...] = dot_tn(r['da3'][e], rows)
            r['gdw2'][...] = dot_tn(r['h'][e], r['dyr'][e])
            for copy in copies:
                copy.start()

        def drain_streams():
            for st in streams:
                st.drain()

        if not bwd:
            turn(sf, 0)
            drain_streams()
            group_x(0, [(0, far, True)])
            left[0] = (sf, 0, 0)
            for j in range(1, turns):
                turn(sf, j)
            sf.step(nz - 2)
        else:
            if fwd:
                group_dy(far, [])
                turn(sf, 0)
                group_dy(far - 1, [(0, far, True)])
                turn(sf, 1)
                sb.begin(1)
                sb.begin(0)

                def outward(j, carry):
                    k = far - j
                    group_dy(k, [(0, k + 1, True), (1, nz - (k + 1), True)])
                    turn(sf, j)
                    return carry

                lax.fori_loop(2, far, outward, 0)
                drain_streams()
                group_dy(0, [(0, 1, True)])
                left += [(sb, 0, 0), (sb, 1, nz - 1)]
                sf.step(nz - 2)

            def push(o, carry):
                grad_copy(o, False).start()
                return carry

            lax.fori_loop(1, n_dev, push, 0)

            def ring(j, carry):
                turn(sb, j)
                weight_grads(j)
                return carry

            lax.fori_loop(0, turns, ring, 0)
            sb.step(nz - 2)
        if not fwd:
            drain_streams()
        if fwd:
            sf.merge(0)
        if bwd:
            sb.merge(0)
        early()
        if bwd:
            dgin[p.me] = dgout[p.me]

            def pull(o, carry):
                grad_copy(o, True).wait_recv()
                return carry

            lax.fori_loop(1, n_dev, pull, 0)
            ids = r['tab'][p.me, pl.ds(layer * TAB, TAB), :]

            def collect(dev, total):
                block = dgin[dev]
                wide = jnp.concatenate([block[:n_local], block[n_local:]], axis=1)
                for e in range(n_local):
                    total += jnp.where(ids == (dev * n_local + e).astype(F32), wide[e:e + 1, :], 0.0)
                return total

            r['dgate' + tag][...] = lax.fori_loop(0, n_dev, collect, jnp.zeros((TAB, tokens), F32))
        if fwd:
            sf.finish()
            emit_y(r['sh'][...] + sf.acc[0])
        if bwd:
            sb.finish()
            emit_dx(r['shd'][...] + sb.acc[0])
            for copy in put(n_local - 1):
                copy.wait()

            def done(o, carry):
                grad_copy(o, False).wait_send()
                return carry

            lax.fori_loop(1, n_dev, done, 0)
        for sc, slot, roff in left:
            sc.cross(roff, slot).wait_send()
        if fwd:
            sf.drain()
        if bwd:
            sb.drain()

    def store(name, index=None):
        def put(value):
            if index is None:
                r[name][...] = value.astype(BF16)
            else:
                r[name][index] = value.astype(BF16)
        return put

    def early_a():
        own_dy.wait()
        ds.start()

    phase(True, False, 0, '_a', early_a, store('xg', p.me), None)
    xs.start()

    again = load_own('x_in', 'xg', 1)

    def early_b():
        again.start()
        again.wait()
        xs.start()

    phase(True, True, 1, '_b', early_b, store('y_out'), store('dg', p.me))
    ds.start()

    phase(False, True, 0, '_a', lambda: None, None, store('dx_out'))


def run_step(dims, x, dy, tab, weights_a, weights_b):
    nz, n_local, cap, tokens = dims
    n_dev = 2 * nz
    d = x.shape[1]
    f = weights_a[0].shape[1]
    slots = n_local * cap
    rows = n_dev * cap
    any_spec = pl.BlockSpec(memory_space=pl.ANY)
    vmem_spec = pl.BlockSpec(memory_space=pltpu.VMEM)
    dma = pltpu.SemaphoreType.DMA
    kinds = ('w1', 'w3', 'w2', 'ws1', 'ws3', 'ws2')
    ins = {'x_in': x, 'dy_in': dy, 'tab_in': tab}
    ins.update({n + '_a': w for n, w in zip(kinds, weights_a)})
    ins.update({n + '_b': w for n, w in zip(kinds, weights_b)})
    outs = {'y_out': ((tokens, d), BF16, vmem_spec), 'dx_out': ((tokens, d), BF16, vmem_spec)}
    for tag in ('_a', '_b'):
        for n in ('dw1', 'dw3', 'dw2'):
            outs[n + tag] = ((n_local, f, d), F32, any_spec)
        outs['dgate' + tag] = ((TAB, tokens), F32, vmem_spec)
    scratch = {n: pltpu.VMEM(w.shape, BF16) for n, w in zip(kinds, weights_a)}
    scratch.update({
        'lsem': dma((3,)), 'wsem': dma((6,)), 'osem': dma((3,)),
        'xg': pltpu.VMEM((n_dev, tokens, d), BF16),
        'dg': pltpu.VMEM((n_dev, tokens, d), BF16),
        'tab': pltpu.VMEM((n_dev, 4 * TAB, tokens), F32),
        'tri': pltpu.VMEM((tokens, tokens), BF16),
        'pall': pltpu.VMEM((n_dev, slots, tokens), BF16),
        'grow': pltpu.VMEM((n_dev, 8, tokens), F32),
        'xr': pltpu.VMEM((n_local, rows, d), BF16),
        'dyr': pltpu.VMEM((n_local, rows, d), BF16),
        'rowbuf': pltpu.VMEM((n_local, 4 * cap, d), BF16),
        'gcol': pltpu.VMEM((n_local, 4 * cap, 128), F32),
        'h': pltpu.VMEM((n_local, rows, f), BF16),
        'da1': pltpu.VMEM((n_local, rows, f), BF16),
        'da3': pltpu.VMEM((n_local, rows, f), BF16),
        'gdw1': pltpu.VMEM((f, d), F32), 'gdw3': pltpu.VMEM((f, d), F32), 'gdw2': pltpu.VMEM((f, d), F32),
        'dgout': pltpu.VMEM((n_dev, 2 * n_local, tokens // 2), F32),
        'sh': pltpu.VMEM((tokens, d), F32), 'shd': pltpu.VMEM((tokens, d), F32),
        'gs': dma((2, 2, nz // 2)), 'gr': dma((2, 2, nz // 2)), 'gxs': dma((nz, 2)), 'gxr': dma((nz, 2)),
        'ds': dma((2, 2, nz // 2)), 'dr': dma((2, 2, nz // 2)), 'dxs': dma((nz, 2)), 'dxr': dma((nz, 2)),
        'ts': dma((2, 1, nz // 2)), 'tr': dma((2, 1, nz // 2)), 'txs': dma((nz, 1)), 'txr': dma((nz, 1)),
    })
    for tag in ('_a', '_b'):
        scratch.update({
            'dgin' + tag: pltpu.VMEM((n_dev, 2 * n_local, tokens // 2), F32),
            'as' + tag: dma((n_dev,)), 'ar' + tag: dma((n_dev,)),
        })
    for tag in ('f', 'b'):
        scratch.update({
            tag + 'acc': pltpu.VMEM((nz, tokens, d), F32),
            tag + 'out': pltpu.VMEM((2, tokens, d), F32),
            tag + 'sib': pltpu.VMEM((nz, tokens, d), F32),
            tag + 'box': pltpu.VMEM((2, nz - 1, tokens // 2, d), F32),
            tag + 'xs': dma((nz,)), tag + 'xr': dma((nz,)),
            tag + 'ss': dma((2, nz - 1)), tag + 'rs': dma((2, nz - 1)),
        })
    result = pl.pallas_call(
        functools.partial(step_kernel, list(ins) + list(outs) + list(scratch), dims),
        out_shape=[jax.ShapeDtypeStruct(s, t) for s, t, _ in outs.values()],
        in_specs=[any_spec] * len(ins),
        out_specs=[spec for _, _, spec in outs.values()],
        scratch_shapes=list(scratch.values()),
        compiler_params=pltpu.CompilerParams(collective_id=0, has_side_effects=True, vmem_limit_bytes=VMEM_BYTES),
        name='two_layers',
    )(*ins.values())
    return dict(zip(outs, result))


def settle_kernel(pieces, *refs):
    n = len(refs[:-2]) // 3
    ins, outs, bufs = refs[:n], refs[n:2 * n], refs[2 * n:3 * n]
    get_sem, put_sem = refs[-2:]
    gets, puts = [], []
    for i in range(n):
        for j in range(pieces[i]):
            rows = pl.ds(j * (ins[i].shape[0] // pieces[i]), ins[i].shape[0] // pieces[i])
            at = len(gets)
            gets.append(pltpu.make_async_copy(ins[i].at[rows], bufs[i].at[rows], get_sem.at[at]))
            puts.append(pltpu.make_async_copy(bufs[i].at[rows], outs[i].at[rows], put_sem.at[at]))
    for get in gets:
        get.start()
    for get, put in zip(gets, puts):
        get.wait()
        put.start()
    for put in puts:
        put.wait()


def settle(arrays):
    pieces = [a.shape[0] if a.ndim == 3 else 1 for a in arrays]
    total = sum(pieces)
    any_spec = pl.BlockSpec(memory_space=pl.ANY)
    return pl.pallas_call(
        functools.partial(settle_kernel, pieces),
        out_shape=[jax.ShapeDtypeStruct(a.shape, a.dtype) for a in arrays],
        in_specs=[any_spec] * len(arrays),
        out_specs=[any_spec] * len(arrays),
        scratch_shapes=[pltpu.VMEM(a.shape, a.dtype) for a in arrays]
        + [pltpu.SemaphoreType.DMA((total,)), pltpu.SemaphoreType.DMA((total,))],
        compiler_params=pltpu.CompilerParams(vmem_limit_bytes=VMEM_BYTES),
        name='settle',
    )(*arrays)


def solution(mesh):
    group_size = mesh.shape['ep']
    token_spec = P(('dp', 'ep'), None)
    expert_spec = P('ep', None, None)
    shared_spec = P(None, None)
    grad_spec = P(('dp', 'ep'), None, None)
    layer_specs = (expert_spec,) * 3 + (shared_spec,) * 3

    def device_step(x_in, d_out, idx_a, gate_a, idx_b, gate_b,
                    w1_a, w3_a, w2_a, ws1_a, ws3_a, ws2_a,
                    w1_b, w3_b, w2_b, ws1_b, ws3_b, ws2_b):
        def turned(w):
            return jnp.swapaxes(w, -1, -2)

        weights_a = (turned(w1_a), turned(w3_a), w2_a, turned(ws1_a), turned(ws3_a), ws2_a)
        weights_b = (turned(w1_b), turned(w3_b), w2_b, turned(ws1_b), turned(ws3_b), ws2_b)
        tokens, top_k = idx_a.shape
        n_local = w1_a.shape[0]
        dims = (group_size // 2, n_local, slot_capacity(tokens, n_local * group_size, top_k), tokens)

        def padded(values, fill):
            return jnp.pad(values.astype(F32), ((0, 0), (0, TAB - top_k)), constant_values=fill)

        table = jnp.concatenate([padded(idx_a, -1.0), padded(idx_b, -1.0), padded(gate_a, 0.0), padded(gate_b, 0.0)],
                                axis=1).T
        got = run_step(dims, x_in, d_out, table, weights_a, weights_b)
        x_last, d_first, *grads = settle(
            [got['y_out'], got['dx_out']] + [got[n + tag] for tag in ('_a', '_b') for n in ('dw1', 'dw3', 'dw2')])
        for at in (0, 1, 3, 4):
            grads[at] = turned(grads[at])
        return (x_last, d_first, *grads, got['dgate_a'][:top_k].T, got['dgate_b'][:top_k].T)

    in_specs = (token_spec,) * 6 + layer_specs + layer_specs
    out_specs = (token_spec, token_spec) + (grad_spec,) * 6 + (token_spec, token_spec)
    return jax.shard_map(device_step, mesh=mesh, in_specs=in_specs, out_specs=out_specs, check_vma=False)
```

```python
import functools

import jax
import jax.numpy as jnp
from jax import lax
from jax.experimental import pallas as pl
from jax.experimental.pallas import tpu as pltpu
from jax.sharding import PartitionSpec as P

F32 = jnp.float32
BF16 = jnp.bfloat16
MESH = pl.DeviceIdType.MESH
VMEM_BYTES = 67_000_000
TAB = 8
PARTS = 2


def slot_capacity(tokens, n_experts, top_k):
    return top_k * ((2 * tokens + n_experts - 1) // n_experts)


def dot(a, b):
    return jnp.dot(a, b, preferred_element_type=F32)


def dot_nt(a, b):
    return lax.dot_general(a, b, (((1,), (1,)), ((), ())), preferred_element_type=F32)


def dot_tn(a, b):
    return lax.dot_general(a, b, (((0,), (0,)), ((), ())), preferred_element_type=F32)


def swiglu_grads(pre_gate, pre_up, d_hidden):
    sigma = jax.nn.sigmoid(pre_gate)
    d_gate = d_hidden * pre_up * sigma * (1.0 + pre_gate * (1.0 - sigma))
    d_up = d_hidden * pre_gate * sigma
    return d_gate.astype(BF16), d_up.astype(BF16)


def hidden_of(rows, w_gate, w_up):
    pre_gate = dot_nt(rows, w_gate)
    pre_up = dot_nt(rows, w_up)
    return pre_gate, pre_up, (pre_gate * jax.nn.sigmoid(pre_gate) * pre_up).astype(BF16)


def when(cond, body):
    if isinstance(cond, bool):
        if cond:
            body()
    else:
        pl.when(cond)(body)


class Place:
    def __init__(self, nz):
        self.nz = nz
        self.me = lax.axis_index('ep')
        self.z = self.me // 2
        self.c = self.me % 2

    def chip(self, offset):
        return lax.rem(self.z + offset + 2 * self.nz, self.nz)

    def source(self, offset, rel):
        return self.chip(offset) * 2 + lax.rem(self.c + rel, 2)

    def device(self, offset, rel=0):
        return {'ep': self.source(offset, rel)}


class Gather:
    def __init__(self, place, buf, pieces, sems):
        self.p, self.buf, self.pieces = place, buf, pieces
        self.ss, self.rs, self.xs, self.xr = sems
        self.rows = buf.shape[1] // pieces

    def far(self, di, h):
        near = self.p.nz // 2 - 1
        return near + 1 if di == h else near

    def at(self, offset, rel, h):
        return self.buf.at[self.p.source(offset, rel), pl.ds(h * self.rows, self.rows)]

    def hop(self, di, h, k, offset):
        d = 1 - 2 * di
        ref = self.at(offset, 0, h)
        return pltpu.make_async_remote_copy(ref, ref, self.ss.at[di, h, k - 1], self.rs.at[di, h, k - 1],
                                            device_id=self.p.device(d), device_id_type=MESH)

    def send(self, di, h, k):
        d = 1 - 2 * di
        return self.hop(di, h, k, -d * (k - 1))

    def recv(self, di, h, k):
        d = 1 - 2 * di
        return self.hop(di, h, k, -d * k)

    def cross(self, h, offset, rel=0):
        ref = self.at(offset, rel, h)
        roff = lax.rem(offset + self.p.nz, self.p.nz) if not isinstance(offset, int) else offset % self.p.nz
        return pltpu.make_async_remote_copy(ref, ref, self.xs.at[roff, h], self.xr.at[roff, h],
                                            device_id=self.p.device(0, 1), device_id_type=MESH)

    def start(self):
        for h in range(self.pieces):
            for di in range(2):
                self.send(di, h, 1).start()
        for h in range(self.pieces):
            self.cross(h, 0).start()

    def step(self, k):
        for h in range(self.pieces):
            for di in range(2):
                d = 1 - 2 * di
                far = self.far(di, h)

                def arrive(di=di, h=h, d=d, far=far):
                    self.recv(di, h, k).wait_recv()
                    when(k + 1 <= far, lambda: self.send(di, h, k + 1).start())
                    self.cross(h, -d * k).start()

                when(k <= far, arrive)

    def wait_cross(self, offset):
        for h in range(self.pieces):
            self.cross(h, offset, 1).wait_recv()

    def drain(self):
        for h in range(self.pieces):
            for di in range(2):
                for k in range(1, self.far(di, h) + 1):
                    self.send(di, h, k).wait_send()
            for roff in range(self.p.nz):
                self.cross(h, roff).wait_send()


class Scatter:
    def __init__(self, place, acc, out, sib, box, sems):
        self.p, self.acc, self.out, self.sib, self.box = place, acc, out, sib, box
        self.xs, self.xr, self.ss, self.rs = sems
        self.half = acc.shape[1] // 2
        self.steps = place.nz - 1

    def cross(self, roff, slot):
        return pltpu.make_async_remote_copy(self.out.at[slot], self.sib.at[roff], self.xs.at[roff], self.xr.at[roff],
                                            device_id=self.p.device(0, 1), device_id_type=MESH)

    def merge(self, roff):
        self.cross(roff, 0).wait_recv()

        def add(i, carry):
            rows = pl.ds(i * 64, 64)
            self.acc[roff, rows, :] += self.sib[roff, rows, :]
            return carry

        lax.fori_loop(0, self.acc.shape[1] // 64, add, 0)

    def reach(self, i):
        return self.p.nz // 2 - (i + 1) // 2

    def roff(self, di, i):
        r = self.reach(i)
        return r if di == 0 else self.p.nz - r

    def side(self, di, i):
        return (i + di) % 2

    def hop(self, di, i, part):
        size = self.half // PARTS
        rows = pl.ds(self.side(di, i) * self.half + part * size, size)
        return pltpu.make_async_remote_copy(self.acc.at[self.roff(di, i), rows],
                                            self.box.at[di, i, pl.ds(part * size, size)],
                                            self.ss.at[di, i, part], self.rs.at[di, i, part],
                                            device_id=self.p.device(1 - 2 * di), device_id_type=MESH)

    def take(self, di, i, part, roff):
        self.hop(di, i, part).wait_recv()
        size = self.half // PARTS
        into = pl.ds(pl.multiple_of(self.side(di, i) * self.half + part * size, size), size)
        self.acc[roff, into, :] += self.box[di, i, pl.ds(part * size, size), :]

    def begin(self, i):
        for roff in sorted({self.roff(0, i), self.roff(1, i)}):
            self.merge(roff)
        for part in range(PARTS):
            for di in range(2):
                self.hop(di, i, part).start()

    def step(self, i):
        for part in range(PARTS):
            for di in range(2):
                self.take(di, i - 2, part, self.roff(di, i))
                self.hop(di, i, part).start()

    def merge_for(self, i):
        self.merge(self.roff(0, i))
        self.merge(self.roff(1, i))

    def free(self, frees):
        for slot, roff, cond in frees:
            when(cond, functools.partial(lambda slot, roff: self.cross(roff, slot).wait_send(), slot, roff))

    def finish(self):
        for i in (self.steps - 2, self.steps - 1):
            for part in range(PARTS):
                for di in range(2):
                    self.take(di, i, part, 0)

    def drain(self):
        for i in range(self.steps):
            for part in range(PARTS):
                for di in range(2):
                    self.hop(di, i, part).wait_send()


def step_kernel(names, dims, *refs):
    r = dict(zip(names, refs))
    nz, n_local, cap, tokens, top_k = dims
    p = Place(nz)
    n_dev = 2 * nz
    far = nz // 2

    def load_weights(tag):
        return [pltpu.make_async_copy(r[n + tag], r[n], r['wsem'].at[i])
                for i, n in enumerate(('ws1', 'ws3', 'ws2', 'w1', 'w3', 'w2'))]

    def load_own(name, buf, i):
        return pltpu.make_async_copy(r[name], r[buf].at[p.me], r['lsem'].at[i])

    own_x, own_dy = load_own('x_in', 'xg', 1), load_own('dy_in', 'dg', 2)
    parts = [pltpu.make_async_copy(r[n + '_in'], r[n], r['tsem'].at[i])
             for i, n in enumerate(('idx_a', 'idx_b', 'gate_a', 'gate_b'))]
    for copy in parts + [own_x, own_dy]:
        copy.start()
    for i, (copy, name) in enumerate(zip(parts, ('idx_a', 'idx_b', 'gate_a', 'gate_b'))):
        copy.wait()
        rows = r[name][...].astype(F32)
        fill = jnp.full((TAB - rows.shape[0], tokens), -1.0 if i < 2 else 0.0, F32)
        r['tab'][p.me, i * TAB:(i + 1) * TAB, :] = jnp.concatenate([rows, fill], axis=0)

    barrier = pltpu.get_barrier_semaphore()
    for peer in (p.device(1), p.device(-1), p.device(0, 1)):
        pl.semaphore_signal(barrier, inc=1, device_id=peer, device_id_type=MESH)
    pl.semaphore_wait(barrier, 3)

    tabs = Gather(p, r['tab'], 1, (r['ts'], r['tr'], r['txs'], r['txr']))
    xs = Gather(p, r['xg'], 2, (r['gs'], r['gr'], r['gxs'], r['gxr']))
    ds = Gather(p, r['dg'], 2, (r['ds'], r['dr'], r['dxs'], r['dxr']))
    sf = Scatter(p, r['facc'], r['fout'], r['fsib'], r['fbox'], (r['fxs'], r['fxr'], r['fss'], r['frs']))
    sb = Scatter(p, r['bacc'], r['bout'], r['bsib'], r['bbox'], (r['bxs'], r['bxr'], r['bss'], r['brs']))

    own_x.wait()
    tabs.start()
    xs.start()

    tri = (lax.broadcasted_iota(jnp.int32, (tokens, tokens), 0)
           < lax.broadcasted_iota(jnp.int32, (tokens, tokens), 1))
    r['tri'][...] = jnp.where(tri, 1.0, 0.0).astype(BF16)

    def offset_of(k, q):
        return k * (1 - 2 * (q // 2))

    def pos_rows(base, n):
        return pl.ds(pl.multiple_of(base * cap, 16), n * cap)

    def spot(k):
        if isinstance(k, int) and k in (0, far):
            return (0 if k == 0 else n_dev - 2), 2
        return 2 + (k - 1) * 4, 4

    def arrived(st, k):
        for i in range(spot(k)[1] // 2):
            st.wait_cross(offset_of(k, 2 * i))

    def route(k, layer):
        base, n = spot(k)

        def body(q, carry):
            s = p.source(offset_of(k, q), q % 2)
            ids = r['tab'][s, pl.ds(layer * TAB, TAB), :]
            gates = r['tab'][s, pl.ds((2 + layer) * TAB, TAB), :]
            used, gate = [], []
            for e in range(n_local):
                hit = ids == (p.me * n_local + e).astype(F32)
                used.append(jnp.max(jnp.where(hit, 1.0, 0.0), axis=0, keepdims=True))
                gate.append(jnp.sum(jnp.where(hit, gates, 0.0), axis=0, keepdims=True))
            zeros = jnp.zeros((8 - n_local, tokens), F32)
            used = jnp.concatenate(used + [zeros], axis=0)
            rank = dot(used.astype(BF16), r['tri'][...])
            slot = jnp.where(used > 0, rank, -1.0)
            pos = base + q
            r['grow'][pos] = jnp.concatenate(gate + [zeros], axis=0)
            place = lax.broadcasted_iota(jnp.int32, (cap, tokens), 0).astype(F32)
            for e in range(n_local):
                r['pall'][pos, e * cap:(e + 1) * cap, :] = jnp.where(place == slot[e:e + 1, :], 1.0, 0.0).astype(BF16)
            return carry

        lax.fori_loop(0, n, body, 0)

    def dispatch(k):
        base, n = spot(k)

        def body(q, carry):
            s = p.source(offset_of(k, q), q % 2)
            pos = base + q
            rows = dot(r['pall'][pos], r['xg'][s]).astype(BF16)
            for e in range(n_local):
                r['xr'][e, pos_rows(pos, 1), :] = rows[e * cap:(e + 1) * cap]
            return carry

        lax.fori_loop(0, n, body, 0)

    def dispatch_dy(k):
        base, n = spot(k)

        def body(q, carry):
            s = p.source(offset_of(k, q), q % 2)
            pos = base + q
            pick = r['pall'][pos]
            gate = r['grow'][pos]
            rows = dot(pick, r['dg'][s]).astype(BF16)
            for e in range(n_local):
                wide = pick[e * cap:(e + 1) * cap].astype(F32) * gate[e:e + 1, :]
                col = jnp.sum(wide, axis=1, keepdims=True)
                r['gcol'][e, pl.ds(pl.multiple_of(q * cap, 16), cap), :] = jnp.broadcast_to(col, (cap, 128))
                r['dyr'][e, pos_rows(pos, 1), :] = rows[e * cap:(e + 1) * cap]
            return carry

        lax.fori_loop(0, n, body, 0)

    def expert_fwd(k):
        base, n = spot(k)

        def body(e, carry):
            hidden = hidden_of(r['xr'][e, pos_rows(base, n), :], r['w1'][e], r['w3'][e])[2]
            r['rowbuf'][e, 0:n * cap, :] = dot(hidden, r['w2'][e]).astype(BF16)
            return carry

        lax.fori_loop(0, n_local, body, 0)

    def expert_bwd(k):
        base, n = spot(k)

        def body(e, carry):
            span = pos_rows(base, n)
            here = slice(0, n * cap)
            pre_gate, pre_up, hidden = hidden_of(r['xr'][e, span, :], r['w1'][e], r['w3'][e])
            dy = r['dyr'][e, span, :]
            projected = dot_nt(dy, r['w2'][e])
            gcol = r['gcol'][e, here, 0:1]
            dgate = jnp.sum(hidden.astype(F32) * projected, axis=1, keepdims=True)
            r['gcol'][e, here, :] = jnp.broadcast_to(dgate, (n * cap, 128))
            r['dyr'][e, span, :] = (gcol * dy.astype(F32)).astype(BF16)
            da_gate, da_up = swiglu_grads(pre_gate, pre_up, gcol * projected)
            r['h'][e, span, :] = hidden
            r['da1'][e, span, :] = da_gate
            r['da3'][e, span, :] = da_up
            du = dot(da_gate, r['w1'][e]) + dot(da_up, r['w3'][e])
            r['rowbuf'][e, here, :] = du.astype(BF16)
            return carry

        lax.fori_loop(0, n_local, body, 0)

    def combine(k, sc, gated, frees):
        base, n = spot(k)
        sc.free(frees)
        for ridx in range(n // 2):
            offset = offset_of(k, 2 * ridx)
            roff = offset % nz if isinstance(offset, int) else lax.rem(offset + nz, nz)
            for rel in (1, 0):
                q = 2 * ridx + rel
                pos = base + q
                rows = jnp.concatenate([r['rowbuf'][e, q * cap:(q + 1) * cap, :] for e in range(n_local)], axis=0)
                if gated:
                    pick = r['pall'][pos].astype(F32)
                    gate = r['grow'][pos]
                    part = None
                    for _ in range(3):
                        term = gate.astype(BF16).astype(F32)
                        gate = gate - term
                        wide = jnp.concatenate(
                            [pick[e * cap:(e + 1) * cap] * term[e:e + 1, :] for e in range(n_local)], axis=0)
                        one = dot_tn(wide.astype(BF16), rows)
                        part = one if part is None else part + one
                else:
                    part = dot_tn(r['pall'][pos], rows)
                if rel == 1:
                    sc.out[ridx] = part
                else:
                    sc.acc[roff] = part
            sc.cross(roff, ridx).start()

    def gate_rows(k, dgout):
        base, n = spot(k)

        def body(q, carry):
            s = p.source(offset_of(k, q), q % 2)
            pos = base + q
            rows = []
            for e in range(n_local):
                col = r['gcol'][e, pl.ds(pl.multiple_of(q * cap, 16), cap), 0:1]
                pick = r['pall'][pos, e * cap:(e + 1) * cap, :].astype(F32)
                rows.append(jnp.sum(pick * col, axis=0, keepdims=True))
            wide = jnp.concatenate(rows, axis=0)
            half = tokens // 2
            dgout[s] = jnp.concatenate([wide[:, :half], wide[:, half:]], axis=0)
            return carry

        lax.fori_loop(0, n, body, 0)

    def upward(k, first):
        return [(0, k - 1, k > first), (1, lax.rem(nz - (k - 1), nz), k > max(first, 1))]

    def order(j):
        return 3 + 2 * (j // 2) - j % 2

    def turn(sc, j):
        i = order(j)
        when(j % 2 == 0, lambda: sc.merge_for(i))
        sc.step(i)

    turns = nz - 4

    def phase(fwd, bwd, layer, tag, middle_hook, early, emit_y, emit_dx):
        weights = load_weights(tag)
        for copy in weights:
            copy.start()
        streams = [xs, ds] if bwd else [tabs, xs]
        x_streams = [xs] if bwd else [tabs, xs]
        dgout, dgin, a_ss, a_rs = (r[n] for n in ('dgout', 'dgin' + tag, 'as' + tag, 'ar' + tag)) if bwd else (None,) * 4

        for copy in weights[:3]:
            copy.wait()
        x_own = r['xg'][p.me]
        s_gate, s_up, s_hidden = hidden_of(x_own, r['ws1'][...], r['ws3'][...])
        if fwd:
            r['sh'][...] = dot(s_hidden, r['ws2'][...]) + x_own.astype(F32)
        if bwd:
            d_own = r['dg'][p.me]
            d_sg, d_su = swiglu_grads(s_gate, s_up, dot_nt(d_own, r['ws2'][...]))
            r['shd'][...] = dot(d_sg, r['ws1'][...]) + dot(d_su, r['ws3'][...]) + d_own.astype(F32)
            route(0, layer)
            lax.fori_loop(1, far, lambda k, c: (route(k, layer), c)[1], 0)
            route(far, layer)
        for copy in weights[3:]:
            copy.wait()

        def group_x(k, frees):
            for st in x_streams:
                arrived(st, k)
            if not bwd:
                route(k, layer)
            dispatch(k)
            if fwd:
                expert_fwd(k)
                combine(k, sf, True, frees)

        def group_dy(k, frees):
            arrived(ds, k)
            dispatch_dy(k)
            expert_bwd(k)
            combine(k, sb, False, frees)
            gate_rows(k, dgout)

        def steps(k):
            for st in x_streams:
                st.step(k)
            if bwd and not fwd:
                ds.step(k)
            elif bwd:
                if isinstance(k, int):
                    ds.step(k)
                else:
                    when(k + 1 < far, lambda: ds.step(k + 1))

        first = 0 if bwd else 1
        if bwd:
            group_x(0, [])
            if not fwd:
                group_dy(0, [])

        def middle(k, carry):
            steps(k)
            group_x(k, upward(k, first))
            if not fwd:
                group_dy(k, upward(k, first))
            return carry

        lax.fori_loop(1, far, middle, 0)
        steps(far)
        middle_hook()
        lead = sf if fwd else sb
        lead.begin(1)
        last = [(0, far - 1, True)]
        group_x(far, last)
        if not fwd:
            group_dy(far, last)
        lead.begin(0)
        left = [(lead, 0, far), (lead, 1, nz - far + 1)]

        def grad_copy(o, wait):
            to = lax.rem(p.me + o, n_dev)
            landed = dgin.at[lax.rem(p.me - o + n_dev, n_dev)] if wait else dgin.at[p.me]
            return pltpu.make_async_remote_copy(dgout.at[to], landed, a_ss.at[o], a_rs.at[o],
                                                device_id={'ep': to}, device_id_type=MESH)

        def put(e):
            return [pltpu.make_async_copy(r['g' + n], r[n + tag].at[e], r['osem'].at[i])
                    for i, n in enumerate(('dw1', 'dw3', 'dw2'))]

        def weight_grads(e):
            copies = put(e)

            @pl.when(e > 0)
            def _():
                for copy in copies:
                    copy.wait()

            rows = r['xr'][e]
            r['gdw1'][...] = dot_tn(r['da1'][e], rows)
            r['gdw3'][...] = dot_tn(r['da3'][e], rows)
            r['gdw2'][...] = dot_tn(r['h'][e], r['dyr'][e])
            for copy in copies:
                copy.start()

        def drain_streams():
            for st in streams:
                st.drain()

        if not bwd:
            turn(sf, 0)
            drain_streams()
            group_x(0, [(0, far, True)])
            left[0] = (sf, 0, 0)
            for j in range(1, turns):
                turn(sf, j)
            sf.step(nz - 2)
        else:
            if fwd:
                group_dy(far, [])
                turn(sf, 0)
                group_dy(far - 1, [(0, far, True)])
                turn(sf, 1)
                sb.begin(1)
                sb.begin(0)

                def outward(j, carry):
                    k = far - j
                    group_dy(k, [(0, k + 1, True), (1, nz - (k + 1), True)])
                    turn(sf, j)
                    return carry

                lax.fori_loop(2, far, outward, 0)
                drain_streams()
                group_dy(0, [(0, 1, True)])
                left += [(sb, 0, 0), (sb, 1, nz - 1)]
                sf.step(nz - 2)

            def push(o, carry):
                grad_copy(o, False).start()
                return carry

            lax.fori_loop(1, n_dev, push, 0)

            def ring(j, carry):
                turn(sb, j)
                weight_grads(j)
                return carry

            lax.fori_loop(0, turns, ring, 0)
            sb.step(nz - 2)
        if not fwd:
            drain_streams()
        if fwd:
            sf.merge(0)
        if bwd:
            sb.merge(0)
        early()
        if bwd:
            dgin[p.me] = dgout[p.me]

            def pull(o, carry):
                grad_copy(o, True).wait_recv()
                return carry

            lax.fori_loop(1, n_dev, pull, 0)
            ids = r['tab'][p.me, pl.ds(layer * TAB, TAB), :]

            def collect(dev, total):
                block = dgin[dev]
                wide = jnp.concatenate([block[:n_local], block[n_local:]], axis=1)
                for e in range(n_local):
                    total += jnp.where(ids == (dev * n_local + e).astype(F32), wide[e:e + 1, :], 0.0)
                return total

            r['dgate' + tag][...] = lax.fori_loop(0, n_dev, collect, jnp.zeros((TAB, tokens), F32))[:top_k]
        if fwd:
            sf.finish()
            emit_y(r['sh'][...] + sf.acc[0])
        if bwd:
            sb.finish()
            emit_dx(r['shd'][...] + sb.acc[0])
            for copy in put(n_local - 1):
                copy.wait()

            def done(o, carry):
                grad_copy(o, False).wait_send()
                return carry

            lax.fori_loop(1, n_dev, done, 0)
        for sc, slot, roff in left:
            sc.cross(roff, slot).wait_send()
        if fwd:
            sf.drain()
        if bwd:
            sb.drain()

    def store(name, index=None):
        def put(value):
            if index is None:
                r[name][...] = value.astype(BF16)
            else:
                r[name][index] = value.astype(BF16)
        return put

    def nothing():
        pass

    def send_dy():
        own_dy.wait()
        ds.start()

    phase(True, False, 0, '_a', send_dy, lambda: ds.step(1), store('xg', p.me), None)
    xs.start()

    again = load_own('x_in', 'xg', 1)

    def send_x():
        again.start()
        again.wait()
        xs.start()

    phase(True, True, 1, '_b', nothing, send_x, store('y_out'), store('dg', p.me))
    ds.start()

    phase(False, True, 0, '_a', nothing, nothing, None, store('dx_out'))


def run_step(dims, x, dy, routes, weights_a, weights_b):
    nz, n_local, cap, tokens, top_k = dims
    n_dev = 2 * nz
    d = x.shape[1]
    f = weights_a[0].shape[1]
    slots = n_local * cap
    rows = n_dev * cap
    any_spec = pl.BlockSpec(memory_space=pl.ANY)
    vmem_spec = pl.BlockSpec(memory_space=pltpu.VMEM)
    dma = pltpu.SemaphoreType.DMA
    kinds = ('w1', 'w3', 'w2', 'ws1', 'ws3', 'ws2')
    ins = {'x_in': x, 'dy_in': dy}
    ins.update({n + '_in': a for n, a in routes.items()})
    ins.update({n + '_a': w for n, w in zip(kinds, weights_a)})
    ins.update({n + '_b': w for n, w in zip(kinds, weights_b)})
    outs = {'y_out': ((tokens, d), BF16, vmem_spec), 'dx_out': ((tokens, d), BF16, vmem_spec)}
    for tag in ('_a', '_b'):
        for n in ('dw1', 'dw3', 'dw2'):
            outs[n + tag] = ((n_local, f, d), F32, any_spec)
        outs['dgate' + tag] = ((top_k, tokens), F32, vmem_spec)
    scratch = {n: pltpu.VMEM(w.shape, BF16) for n, w in zip(kinds, weights_a)}
    scratch.update({
        **{n: pltpu.VMEM(a.shape, a.dtype) for n, a in routes.items()},
        'tsem': dma((4,)), 'lsem': dma((3,)), 'wsem': dma((6,)), 'osem': dma((3,)),
        'xg': pltpu.VMEM((n_dev, tokens, d), BF16),
        'dg': pltpu.VMEM((n_dev, tokens, d), BF16),
        'tab': pltpu.VMEM((n_dev, 4 * TAB, tokens), F32),
        'tri': pltpu.VMEM((tokens, tokens), BF16),
        'pall': pltpu.VMEM((n_dev, slots, tokens), BF16),
        'grow': pltpu.VMEM((n_dev, 8, tokens), F32),
        'xr': pltpu.VMEM((n_local, rows, d), BF16),
        'dyr': pltpu.VMEM((n_local, rows, d), BF16),
        'rowbuf': pltpu.VMEM((n_local, 4 * cap, d), BF16),
        'gcol': pltpu.VMEM((n_local, 4 * cap, 128), F32),
        'h': pltpu.VMEM((n_local, rows, f), BF16),
        'da1': pltpu.VMEM((n_local, rows, f), BF16),
        'da3': pltpu.VMEM((n_local, rows, f), BF16),
        'gdw1': pltpu.VMEM((f, d), F32), 'gdw3': pltpu.VMEM((f, d), F32), 'gdw2': pltpu.VMEM((f, d), F32),
        'dgout': pltpu.VMEM((n_dev, 2 * n_local, tokens // 2), F32),
        'sh': pltpu.VMEM((tokens, d), F32), 'shd': pltpu.VMEM((tokens, d), F32),
        'gs': dma((2, 2, nz // 2)), 'gr': dma((2, 2, nz // 2)), 'gxs': dma((nz, 2)), 'gxr': dma((nz, 2)),
        'ds': dma((2, 2, nz // 2)), 'dr': dma((2, 2, nz // 2)), 'dxs': dma((nz, 2)), 'dxr': dma((nz, 2)),
        'ts': dma((2, 1, nz // 2)), 'tr': dma((2, 1, nz // 2)), 'txs': dma((nz, 1)), 'txr': dma((nz, 1)),
    })
    for tag in ('_a', '_b'):
        scratch.update({
            'dgin' + tag: pltpu.VMEM((n_dev, 2 * n_local, tokens // 2), F32),
            'as' + tag: dma((n_dev,)), 'ar' + tag: dma((n_dev,)),
        })
    for tag in ('f', 'b'):
        scratch.update({
            tag + 'acc': pltpu.VMEM((nz, tokens, d), F32),
            tag + 'out': pltpu.VMEM((2, tokens, d), F32),
            tag + 'sib': pltpu.VMEM((nz, tokens, d), F32),
            tag + 'box': pltpu.VMEM((2, nz - 1, tokens // 2, d), F32),
            tag + 'xs': dma((nz,)), tag + 'xr': dma((nz,)),
            tag + 'ss': dma((2, nz - 1, PARTS)), tag + 'rs': dma((2, nz - 1, PARTS)),
        })
    result = pl.pallas_call(
        functools.partial(step_kernel, list(ins) + list(outs) + list(scratch), dims),
        out_shape=[jax.ShapeDtypeStruct(s, t) for s, t, _ in outs.values()],
        in_specs=[any_spec] * len(ins),
        out_specs=[spec for _, _, spec in outs.values()],
        scratch_shapes=list(scratch.values()),
        compiler_params=pltpu.CompilerParams(collective_id=0, has_side_effects=True, vmem_limit_bytes=VMEM_BYTES),
        name='two_layers',
    )(*ins.values())
    return dict(zip(outs, result))


def settle_kernel(pieces, *refs):
    n = len(refs[:-2]) // 3
    ins, outs, bufs = refs[:n], refs[n:2 * n], refs[2 * n:3 * n]
    get_sem, put_sem = refs[-2:]
    gets, puts = [], []
    for i in range(n):
        for j in range(pieces[i]):
            rows = pl.ds(j * (ins[i].shape[0] // pieces[i]), ins[i].shape[0] // pieces[i])
            at = len(gets)
            gets.append(pltpu.make_async_copy(ins[i].at[rows], bufs[i].at[rows], get_sem.at[at]))
            puts.append(pltpu.make_async_copy(bufs[i].at[rows], outs[i].at[rows], put_sem.at[at]))
    for get in gets:
        get.start()
    for get, put in zip(gets, puts):
        get.wait()
        put.start()
    for put in puts:
        put.wait()


def settle(arrays):
    pieces = [a.shape[0] if a.ndim == 3 else 1 for a in arrays]
    total = sum(pieces)
    any_spec = pl.BlockSpec(memory_space=pl.ANY)
    return pl.pallas_call(
        functools.partial(settle_kernel, pieces),
        out_shape=[jax.ShapeDtypeStruct(a.shape, a.dtype) for a in arrays],
        in_specs=[any_spec] * len(arrays),
        out_specs=[any_spec] * len(arrays),
        scratch_shapes=[pltpu.VMEM(a.shape, a.dtype) for a in arrays]
        + [pltpu.SemaphoreType.DMA((total,)), pltpu.SemaphoreType.DMA((total,))],
        compiler_params=pltpu.CompilerParams(vmem_limit_bytes=VMEM_BYTES),
        name='settle',
    )(*arrays)


def solution(mesh):
    group_size = mesh.shape['ep']
    token_spec = P(('dp', 'ep'), None)
    expert_spec = P('ep', None, None)
    shared_spec = P(None, None)
    grad_spec = P(('dp', 'ep'), None, None)
    layer_specs = (expert_spec,) * 3 + (shared_spec,) * 3

    def device_step(x_in, d_out, idx_a, gate_a, idx_b, gate_b,
                    w1_a, w3_a, w2_a, ws1_a, ws3_a, ws2_a,
                    w1_b, w3_b, w2_b, ws1_b, ws3_b, ws2_b):
        def turned(w):
            return jnp.swapaxes(w, -1, -2)

        weights_a = (turned(w1_a), turned(w3_a), w2_a, turned(ws1_a), turned(ws3_a), ws2_a)
        weights_b = (turned(w1_b), turned(w3_b), w2_b, turned(ws1_b), turned(ws3_b), ws2_b)
        tokens, top_k = idx_a.shape
        n_local = w1_a.shape[0]
        dims = (group_size // 2, n_local, slot_capacity(tokens, n_local * group_size, top_k), tokens, top_k)
        routes = {'idx_a': idx_a.T, 'idx_b': idx_b.T, 'gate_a': gate_a.T, 'gate_b': gate_b.T}
        got = run_step(dims, x_in, d_out, routes, weights_a, weights_b)
        x_last, d_first, *grads = settle(
            [got['y_out'], got['dx_out']]
            + [got[n + tag] for tag in ('_a', '_b') for n in ('dw1', 'dw3', 'dw2')]
            + [got['dgate_a'], got['dgate_b']])
        for at in (0, 1, 3, 4):
            grads[at] = turned(grads[at])
        return (x_last, d_first, *grads[:6], grads[6].T, grads[7].T)

    in_specs = (token_spec,) * 6 + layer_specs + layer_specs
    out_specs = (token_spec, token_spec) + (grad_spec,) * 6 + (token_spec, token_spec)
    return jax.shard_map(device_step, mesh=mesh, in_specs=in_specs, out_specs=out_specs, check_vma=False)
```

```python
import functools

import jax
import jax.numpy as jnp
from jax import lax
from jax.experimental import pallas as pl
from jax.experimental.pallas import tpu as pltpu
from jax.sharding import PartitionSpec as P

F32 = jnp.float32
BF16 = jnp.bfloat16
MESH = pl.DeviceIdType.MESH
VMEM_BYTES = 67_000_000
TAB = 8
PARTS = 2


def slot_capacity(tokens, n_experts, top_k):
    return top_k * ((2 * tokens + n_experts - 1) // n_experts)


def dot(a, b):
    return jnp.dot(a, b, preferred_element_type=F32)


def dot_nt(a, b):
    return lax.dot_general(a, b, (((1,), (1,)), ((), ())), preferred_element_type=F32)


def dot_tn(a, b):
    return lax.dot_general(a, b, (((0,), (0,)), ((), ())), preferred_element_type=F32)


def swiglu_grads(pre_gate, pre_up, d_hidden):
    sigma = jax.nn.sigmoid(pre_gate)
    d_gate = d_hidden * pre_up * sigma * (1.0 + pre_gate * (1.0 - sigma))
    d_up = d_hidden * pre_gate * sigma
    return d_gate.astype(BF16), d_up.astype(BF16)


def hidden_of(rows, w_gate, w_up):
    pre_gate = dot_nt(rows, w_gate)
    pre_up = dot_nt(rows, w_up)
    return pre_gate, pre_up, (pre_gate * jax.nn.sigmoid(pre_gate) * pre_up).astype(BF16)


def when(cond, body):
    if isinstance(cond, bool):
        if cond:
            body()
    else:
        pl.when(cond)(body)


class Place:
    def __init__(self, nz):
        self.nz = nz
        self.me = lax.axis_index('ep')
        self.z = self.me // 2
        self.c = self.me % 2

    def chip(self, offset):
        return lax.rem(self.z + offset + 2 * self.nz, self.nz)

    def source(self, offset, rel):
        return self.chip(offset) * 2 + lax.rem(self.c + rel, 2)

    def device(self, offset, rel=0):
        return {'ep': self.source(offset, rel)}


class Gather:
    def __init__(self, place, buf, pieces, sems):
        self.p, self.buf, self.pieces = place, buf, pieces
        self.ss, self.rs, self.xs, self.xr = sems
        self.rows = buf.shape[1] // pieces

    def far(self, di, h):
        near = self.p.nz // 2 - 1
        return near + 1 if di == h else near

    def at(self, offset, rel, h):
        return self.buf.at[self.p.source(offset, rel), pl.ds(h * self.rows, self.rows)]

    def hop(self, di, h, k, offset):
        d = 1 - 2 * di
        ref = self.at(offset, 0, h)
        return pltpu.make_async_remote_copy(ref, ref, self.ss.at[di, h, k - 1], self.rs.at[di, h, k - 1],
                                            device_id=self.p.device(d), device_id_type=MESH)

    def send(self, di, h, k):
        d = 1 - 2 * di
        return self.hop(di, h, k, -d * (k - 1))

    def recv(self, di, h, k):
        d = 1 - 2 * di
        return self.hop(di, h, k, -d * k)

    def cross(self, h, offset, rel=0):
        ref = self.at(offset, rel, h)
        roff = lax.rem(offset + self.p.nz, self.p.nz) if not isinstance(offset, int) else offset % self.p.nz
        return pltpu.make_async_remote_copy(ref, ref, self.xs.at[roff, h], self.xr.at[roff, h],
                                            device_id=self.p.device(0, 1), device_id_type=MESH)

    def start(self):
        for h in range(self.pieces):
            for di in range(2):
                self.send(di, h, 1).start()
        for h in range(self.pieces):
            self.cross(h, 0).start()

    def step(self, k):
        for h in range(self.pieces):
            for di in range(2):
                d = 1 - 2 * di
                far = self.far(di, h)

                def arrive(di=di, h=h, d=d, far=far):
                    self.recv(di, h, k).wait_recv()
                    when(k + 1 <= far, lambda: self.send(di, h, k + 1).start())
                    self.cross(h, -d * k).start()

                when(k <= far, arrive)

    def wait_cross(self, offset):
        for h in range(self.pieces):
            self.cross(h, offset, 1).wait_recv()

    def drain(self):
        for h in range(self.pieces):
            for di in range(2):
                for k in range(1, self.far(di, h) + 1):
                    self.send(di, h, k).wait_send()
            for roff in range(self.p.nz):
                self.cross(h, roff).wait_send()


class Scatter:
    def __init__(self, place, acc, out, sib, box, sems):
        self.p, self.acc, self.out, self.sib, self.box = place, acc, out, sib, box
        self.xs, self.xr, self.ss, self.rs = sems
        self.half = acc.shape[1] // 2
        self.steps = place.nz - 1

    def cross(self, roff, slot):
        return pltpu.make_async_remote_copy(self.out.at[slot], self.sib.at[roff], self.xs.at[roff], self.xr.at[roff],
                                            device_id=self.p.device(0, 1), device_id_type=MESH)

    def merge(self, roff):
        self.cross(roff, 0).wait_recv()

        def add(i, carry):
            rows = pl.ds(i * 64, 64)
            self.acc[roff, rows, :] += self.sib[roff, rows, :]
            return carry

        lax.fori_loop(0, self.acc.shape[1] // 64, add, 0)

    def reach(self, i):
        return self.p.nz // 2 - (i + 1) // 2

    def roff(self, di, i):
        r = self.reach(i)
        return r if di == 0 else self.p.nz - r

    def side(self, di, i):
        return (i + di) % 2

    def hop(self, di, i, part):
        size = self.half // PARTS
        rows = pl.ds(self.side(di, i) * self.half + part * size, size)
        return pltpu.make_async_remote_copy(self.acc.at[self.roff(di, i), rows],
                                            self.box.at[di, i, pl.ds(part * size, size)],
                                            self.ss.at[di, i, part], self.rs.at[di, i, part],
                                            device_id=self.p.device(1 - 2 * di), device_id_type=MESH)

    def take(self, di, i, part, roff):
        self.hop(di, i, part).wait_recv()
        size = self.half // PARTS
        into = pl.ds(pl.multiple_of(self.side(di, i) * self.half + part * size, size), size)
        self.acc[roff, into, :] += self.box[di, i, pl.ds(part * size, size), :]

    def begin(self, i):
        for roff in sorted({self.roff(0, i), self.roff(1, i)}):
            self.merge(roff)
        for part in range(PARTS):
            for di in range(2):
                self.hop(di, i, part).start()

    def step(self, i):
        for part in range(PARTS):
            for di in range(2):
                self.take(di, i - 2, part, self.roff(di, i))
                self.hop(di, i, part).start()

    def merge_for(self, i):
        self.merge(self.roff(0, i))
        self.merge(self.roff(1, i))

    def free(self, frees):
        for slot, roff, cond in frees:
            when(cond, functools.partial(lambda slot, roff: self.cross(roff, slot).wait_send(), slot, roff))

    def finish(self):
        for i in (self.steps - 2, self.steps - 1):
            for part in range(PARTS):
                for di in range(2):
                    self.take(di, i, part, 0)

    def drain(self):
        for i in range(self.steps):
            for part in range(PARTS):
                for di in range(2):
                    self.hop(di, i, part).wait_send()


def step_kernel(names, dims, *refs):
    r = dict(zip(names, refs))
    nz, n_local, cap, tokens, top_k = dims
    p = Place(nz)
    n_dev = 2 * nz
    far = nz // 2

    def load_weights(tag):
        return [pltpu.make_async_copy(r[n + tag], r[n], r['wsem'].at[i])
                for i, n in enumerate(('w1', 'w3', 'w2', 'ws1', 'ws3', 'ws2'))]

    def load_own(name, buf, i):
        return pltpu.make_async_copy(r[name], r[buf].at[p.me], r['lsem'].at[i])

    own_x, own_dy = load_own('x_in', 'xg', 1), load_own('dy_in', 'dg', 2)
    parts = [pltpu.make_async_copy(r[n + '_in'], r[n], r['tsem'].at[i])
             for i, n in enumerate(('idx_a', 'idx_b', 'gate_a', 'gate_b'))]
    for copy in parts + [own_x, own_dy]:
        copy.start()
    for i, (copy, name) in enumerate(zip(parts, ('idx_a', 'idx_b', 'gate_a', 'gate_b'))):
        copy.wait()
        rows = r[name][...].astype(F32)
        fill = jnp.full((TAB - rows.shape[0], tokens), -1.0 if i < 2 else 0.0, F32)
        r['tab'][p.me, i * TAB:(i + 1) * TAB, :] = jnp.concatenate([rows, fill], axis=0)

    barrier = pltpu.get_barrier_semaphore()
    for peer in (p.device(1), p.device(-1), p.device(0, 1)):
        pl.semaphore_signal(barrier, inc=1, device_id=peer, device_id_type=MESH)
    pl.semaphore_wait(barrier, 3)

    tabs = Gather(p, r['tab'], 1, (r['ts'], r['tr'], r['txs'], r['txr']))
    xs = Gather(p, r['xg'], 2, (r['gs'], r['gr'], r['gxs'], r['gxr']))
    ds = Gather(p, r['dg'], 2, (r['ds'], r['dr'], r['dxs'], r['dxr']))
    sf = Scatter(p, r['facc'], r['fout'], r['fsib'], r['fbox'], (r['fxs'], r['fxr'], r['fss'], r['frs']))
    sb = Scatter(p, r['bacc'], r['bout'], r['bsib'], r['bbox'], (r['bxs'], r['bxr'], r['bss'], r['brs']))

    own_x.wait()
    tabs.start()
    xs.start()

    tri = (lax.broadcasted_iota(jnp.int32, (tokens, tokens), 0)
           < lax.broadcasted_iota(jnp.int32, (tokens, tokens), 1))
    r['tri'][...] = jnp.where(tri, 1.0, 0.0).astype(BF16)

    def offset_of(k, q):
        return k * (1 - 2 * (q // 2))

    def pos_rows(base, n):
        return pl.ds(pl.multiple_of(base * cap, 16), n * cap)

    def spot(k):
        if isinstance(k, int) and k in (0, far):
            return (0 if k == 0 else n_dev - 2), 2
        return 2 + (k - 1) * 4, 4

    def arrived(st, k):
        for i in range(spot(k)[1] // 2):
            st.wait_cross(offset_of(k, 2 * i))

    def route(k, layer):
        base, n = spot(k)

        def body(q, carry):
            s = p.source(offset_of(k, q), q % 2)
            ids = r['tab'][s, pl.ds(layer * TAB, TAB), :]
            gates = r['tab'][s, pl.ds((2 + layer) * TAB, TAB), :]
            used, gate = [], []
            for e in range(n_local):
                hit = ids == (p.me * n_local + e).astype(F32)
                used.append(jnp.max(jnp.where(hit, 1.0, 0.0), axis=0, keepdims=True))
                gate.append(jnp.sum(jnp.where(hit, gates, 0.0), axis=0, keepdims=True))
            zeros = jnp.zeros((8 - n_local, tokens), F32)
            used = jnp.concatenate(used + [zeros], axis=0)
            rank = dot(used.astype(BF16), r['tri'][...])
            slot = jnp.where(used > 0, rank, -1.0)
            pos = base + q
            r['grow'][pos] = jnp.concatenate(gate + [zeros], axis=0)
            place = lax.broadcasted_iota(jnp.int32, (cap, tokens), 0).astype(F32)
            for e in range(n_local):
                r['pall'][pos, e * cap:(e + 1) * cap, :] = jnp.where(place == slot[e:e + 1, :], 1.0, 0.0).astype(BF16)
            return carry

        lax.fori_loop(0, n, body, 0)

    def dispatch(k):
        base, n = spot(k)

        def body(q, carry):
            s = p.source(offset_of(k, q), q % 2)
            pos = base + q
            rows = dot(r['pall'][pos], r['xg'][s]).astype(BF16)
            for e in range(n_local):
                r['xr'][e, pos_rows(pos, 1), :] = rows[e * cap:(e + 1) * cap]
            return carry

        lax.fori_loop(0, n, body, 0)

    def dispatch_dy(k):
        base, n = spot(k)

        def body(q, carry):
            s = p.source(offset_of(k, q), q % 2)
            pos = base + q
            pick = r['pall'][pos]
            gate = r['grow'][pos]
            rows = dot(pick, r['dg'][s]).astype(BF16)
            for e in range(n_local):
                wide = pick[e * cap:(e + 1) * cap].astype(F32) * gate[e:e + 1, :]
                col = jnp.sum(wide, axis=1, keepdims=True)
                r['gcol'][e, pl.ds(pl.multiple_of(q * cap, 16), cap), :] = jnp.broadcast_to(col, (cap, 128))
                r['dyr'][e, pos_rows(pos, 1), :] = rows[e * cap:(e + 1) * cap]
            return carry

        lax.fori_loop(0, n, body, 0)

    def expert_fwd(k):
        base, n = spot(k)

        def body(e, carry):
            hidden = hidden_of(r['xr'][e, pos_rows(base, n), :], r['w1'][e], r['w3'][e])[2]
            r['rowbuf'][e, 0:n * cap, :] = dot(hidden, r['w2'][e]).astype(BF16)
            return carry

        lax.fori_loop(0, n_local, body, 0)

    def expert_bwd(k):
        base, n = spot(k)

        def body(e, carry):
            span = pos_rows(base, n)
            here = slice(0, n * cap)
            pre_gate, pre_up, hidden = hidden_of(r['xr'][e, span, :], r['w1'][e], r['w3'][e])
            dy = r['dyr'][e, span, :]
            projected = dot_nt(dy, r['w2'][e])
            gcol = r['gcol'][e, here, 0:1]
            dgate = jnp.sum(hidden.astype(F32) * projected, axis=1, keepdims=True)
            r['gcol'][e, here, :] = jnp.broadcast_to(dgate, (n * cap, 128))
            r['dyr'][e, span, :] = (gcol * dy.astype(F32)).astype(BF16)
            da_gate, da_up = swiglu_grads(pre_gate, pre_up, gcol * projected)
            r['h'][e, span, :] = hidden
            r['da1'][e, span, :] = da_gate
            r['da3'][e, span, :] = da_up
            du = dot(da_gate, r['w1'][e]) + dot(da_up, r['w3'][e])
            r['rowbuf'][e, here, :] = du.astype(BF16)
            return carry

        lax.fori_loop(0, n_local, body, 0)

    def combine(k, sc, gated, frees):
        base, n = spot(k)
        sc.free(frees)
        for ridx in range(n // 2):
            offset = offset_of(k, 2 * ridx)
            roff = offset % nz if isinstance(offset, int) else lax.rem(offset + nz, nz)
            for rel in (1, 0):
                q = 2 * ridx + rel
                pos = base + q
                rows = jnp.concatenate([r['rowbuf'][e, q * cap:(q + 1) * cap, :] for e in range(n_local)], axis=0)
                if gated:
                    pick = r['pall'][pos].astype(F32)
                    gate = r['grow'][pos]
                    part = None
                    for _ in range(3):
                        term = gate.astype(BF16).astype(F32)
                        gate = gate - term
                        wide = jnp.concatenate(
                            [pick[e * cap:(e + 1) * cap] * term[e:e + 1, :] for e in range(n_local)], axis=0)
                        one = dot_tn(wide.astype(BF16), rows)
                        part = one if part is None else part + one
                else:
                    part = dot_tn(r['pall'][pos], rows)
                if rel == 1:
                    sc.out[ridx] = part
                else:
                    sc.acc[roff] = part
            sc.cross(roff, ridx).start()

    def gate_rows(k, dgout):
        base, n = spot(k)

        def body(q, carry):
            s = p.source(offset_of(k, q), q % 2)
            pos = base + q
            rows = []
            for e in range(n_local):
                col = r['gcol'][e, pl.ds(pl.multiple_of(q * cap, 16), cap), 0:1]
                pick = r['pall'][pos, e * cap:(e + 1) * cap, :].astype(F32)
                rows.append(jnp.sum(pick * col, axis=0, keepdims=True))
            wide = jnp.concatenate(rows, axis=0)
            half = tokens // 2
            dgout[s] = jnp.concatenate([wide[:, :half], wide[:, half:]], axis=0)
            return carry

        lax.fori_loop(0, n, body, 0)

    def upward(k, first):
        return [(0, k - 1, k > first), (1, lax.rem(nz - (k - 1), nz), k > max(first, 1))]

    def order(j):
        return 3 + 2 * (j // 2) - j % 2

    def turn(sc, j):
        i = order(j)
        when(j % 2 == 0, lambda: sc.merge_for(i))
        sc.step(i)

    turns = nz - 4

    def phase(fwd, bwd, layer, tag, middle_hook, early, emit_y, emit_dx):
        weights = load_weights(tag)
        for copy in weights:
            copy.start()
        streams = [xs, ds] if bwd else [tabs, xs]
        x_streams = [xs] if bwd else [tabs, xs]
        dgout, dgin, a_ss, a_rs = (r[n] for n in ('dgout', 'dgin' + tag, 'as' + tag, 'ar' + tag)) if bwd else (None,) * 4

        if bwd:
            route(0, layer)
            lax.fori_loop(1, far, lambda k, c: (route(k, layer), c)[1], 0)
            route(far, layer)
        for copy in weights[:3]:
            copy.wait()

        def shared():
            for copy in weights[3:]:
                copy.wait()
            x_own = r['xg'][p.me]
            s_gate, s_up, s_hidden = hidden_of(x_own, r['ws1'][...], r['ws3'][...])
            if fwd:
                r['sh'][...] = dot(s_hidden, r['ws2'][...]) + x_own.astype(F32)
            if bwd:
                d_own = r['dg'][p.me]
                d_sg, d_su = swiglu_grads(s_gate, s_up, dot_nt(d_own, r['ws2'][...]))
                r['shd'][...] = dot(d_sg, r['ws1'][...]) + dot(d_su, r['ws3'][...]) + d_own.astype(F32)

        def group_x(k, frees):
            for st in x_streams:
                arrived(st, k)
            if not bwd:
                route(k, layer)
            dispatch(k)
            if fwd:
                expert_fwd(k)
                combine(k, sf, True, frees)

        def group_dy(k, frees):
            arrived(ds, k)
            dispatch_dy(k)
            expert_bwd(k)
            combine(k, sb, False, frees)
            gate_rows(k, dgout)

        def steps(k):
            if bwd and not fwd:
                ds.step(k)
                if isinstance(k, int):
                    xs.step(k)
                else:
                    when(k == 1, lambda: xs.step(2))
                    when(k == far - 1, lambda: xs.step(far - 1))
                return
            for st in x_streams:
                st.step(k)
            if bwd:
                if isinstance(k, int):
                    ds.step(k)
                else:
                    when(k + 1 < far, lambda: ds.step(k + 1))

        first = 0 if bwd else 1
        if bwd:
            group_x(0, [])
            if not fwd:
                group_dy(0, [])

        def middle(k, carry):
            steps(k)
            if middle_hook is not None:
                pl.when(k == far - 1)(middle_hook)
            group_x(k, upward(k, first))
            if not fwd:
                group_dy(k, upward(k, first))
            return carry

        lax.fori_loop(1, far, middle, 0)
        steps(far)
        lead = sf if fwd else sb
        lead.begin(1)
        last = [(0, far - 1, True)]
        group_x(far, last)
        if not fwd:
            group_dy(far, last)
        lead.begin(0)
        shared()
        left = [(lead, 0, far), (lead, 1, nz - far + 1)]

        def grad_copy(o, wait):
            to = lax.rem(p.me + o, n_dev)
            landed = dgin.at[lax.rem(p.me - o + n_dev, n_dev)] if wait else dgin.at[p.me]
            return pltpu.make_async_remote_copy(dgout.at[to], landed, a_ss.at[o], a_rs.at[o],
                                                device_id={'ep': to}, device_id_type=MESH)

        def put(e):
            return [pltpu.make_async_copy(r['g' + n], r[n + tag].at[e], r['osem'].at[i])
                    for i, n in enumerate(('dw1', 'dw3', 'dw2'))]

        def weight_grads(e):
            copies = put(e)

            @pl.when(e > 0)
            def _():
                for copy in copies:
                    copy.wait()

            rows = r['xr'][e]
            r['gdw1'][...] = dot_tn(r['da1'][e], rows)
            r['gdw3'][...] = dot_tn(r['da3'][e], rows)
            r['gdw2'][...] = dot_tn(r['h'][e], r['dyr'][e])
            for copy in copies:
                copy.start()

        def drain_streams():
            for st in streams:
                st.drain()

        if not bwd:
            turn(sf, 0)
            drain_streams()
            group_x(0, [(0, far, True)])
            left[0] = (sf, 0, 0)
            for j in range(1, turns):
                turn(sf, j)
            sf.step(nz - 2)
        else:
            if fwd:
                group_dy(far, [])
                turn(sf, 0)
                group_dy(far - 1, [(0, far, True)])
                turn(sf, 1)
                sb.begin(1)
                sb.begin(0)

                def outward(j, carry):
                    k = far - j
                    group_dy(k, [(0, k + 1, True), (1, nz - (k + 1), True)])
                    turn(sf, j)
                    return carry

                lax.fori_loop(2, far, outward, 0)
                drain_streams()
                group_dy(0, [(0, 1, True)])
                left += [(sb, 0, 0), (sb, 1, nz - 1)]
                sf.step(nz - 2)

            def push(o, carry):
                grad_copy(o, False).start()
                return carry

            lax.fori_loop(1, n_dev, push, 0)

            def ring(j, carry):
                turn(sb, j)
                weight_grads(j)
                return carry

            lax.fori_loop(0, turns, ring, 0)
            sb.step(nz - 2)
        if not fwd:
            drain_streams()
        if fwd:
            sf.merge(0)
        if bwd:
            sb.merge(0)
        early()
        if bwd:
            dgin[p.me] = dgout[p.me]

            def pull(o, carry):
                grad_copy(o, True).wait_recv()
                return carry

            lax.fori_loop(1, n_dev, pull, 0)
            ids = r['tab'][p.me, pl.ds(layer * TAB, TAB), :]

            def collect(dev, total):
                block = dgin[dev]
                wide = jnp.concatenate([block[:n_local], block[n_local:]], axis=1)
                for e in range(n_local):
                    total += jnp.where(ids == (dev * n_local + e).astype(F32), wide[e:e + 1, :], 0.0)
                return total

            r['dgate' + tag][...] = lax.fori_loop(0, n_dev, collect, jnp.zeros((TAB, tokens), F32))[:top_k]
        if fwd:
            sf.finish()
            emit_y(r['sh'][...] + sf.acc[0])
        if bwd:
            sb.finish()
            emit_dx(r['shd'][...] + sb.acc[0])
            for copy in put(n_local - 1):
                copy.wait()

            def done(o, carry):
                grad_copy(o, False).wait_send()
                return carry

            lax.fori_loop(1, n_dev, done, 0)
        for sc, slot, roff in left:
            sc.cross(roff, slot).wait_send()
        if fwd:
            sf.drain()
        if bwd:
            sb.drain()

    def store(name, index=None):
        def put(value):
            if index is None:
                r[name][...] = value.astype(BF16)
            else:
                r[name][index] = value.astype(BF16)
        return put

    def nothing():
        pass

    def send_dy():
        own_dy.wait()
        ds.start()

    phase(True, False, 0, '_a', send_dy, lambda: ds.step(1), store('xg', p.me), None)
    xs.start()

    again = load_own('x_in', 'xg', 1)

    def send_x():
        again.start()
        again.wait()
        xs.start()

    phase(True, True, 1, '_b', None, send_x, store('y_out'), store('dg', p.me))
    ds.start()
    xs.step(1)

    phase(False, True, 0, '_a', None, nothing, None, store('dx_out'))


def run_step(dims, x, dy, routes, weights_a, weights_b):
    nz, n_local, cap, tokens, top_k = dims
    n_dev = 2 * nz
    d = x.shape[1]
    f = weights_a[0].shape[1]
    slots = n_local * cap
    rows = n_dev * cap
    any_spec = pl.BlockSpec(memory_space=pl.ANY)
    vmem_spec = pl.BlockSpec(memory_space=pltpu.VMEM)
    dma = pltpu.SemaphoreType.DMA
    kinds = ('w1', 'w3', 'w2', 'ws1', 'ws3', 'ws2')
    ins = {'x_in': x, 'dy_in': dy}
    ins.update({n + '_in': a for n, a in routes.items()})
    ins.update({n + '_a': w for n, w in zip(kinds, weights_a)})
    ins.update({n + '_b': w for n, w in zip(kinds, weights_b)})
    outs = {'y_out': ((tokens, d), BF16, vmem_spec), 'dx_out': ((tokens, d), BF16, vmem_spec)}
    for tag in ('_a', '_b'):
        for n in ('dw1', 'dw3', 'dw2'):
            outs[n + tag] = ((n_local, f, d), F32, any_spec)
        outs['dgate' + tag] = ((top_k, tokens), F32, vmem_spec)
    scratch = {n: pltpu.VMEM(w.shape, BF16) for n, w in zip(kinds, weights_a)}
    scratch.update({
        **{n: pltpu.VMEM(a.shape, a.dtype) for n, a in routes.items()},
        'tsem': dma((4,)), 'lsem': dma((3,)), 'wsem': dma((6,)), 'osem': dma((3,)),
        'xg': pltpu.VMEM((n_dev, tokens, d), BF16),
        'dg': pltpu.VMEM((n_dev, tokens, d), BF16),
        'tab': pltpu.VMEM((n_dev, 4 * TAB, tokens), F32),
        'tri': pltpu.VMEM((tokens, tokens), BF16),
        'pall': pltpu.VMEM((n_dev, slots, tokens), BF16),
        'grow': pltpu.VMEM((n_dev, 8, tokens), F32),
        'xr': pltpu.VMEM((n_local, rows, d), BF16),
        'dyr': pltpu.VMEM((n_local, rows, d), BF16),
        'rowbuf': pltpu.VMEM((n_local, 4 * cap, d), BF16),
        'gcol': pltpu.VMEM((n_local, 4 * cap, 128), F32),
        'h': pltpu.VMEM((n_local, rows, f), BF16),
        'da1': pltpu.VMEM((n_local, rows, f), BF16),
        'da3': pltpu.VMEM((n_local, rows, f), BF16),
        'gdw1': pltpu.VMEM((f, d), F32), 'gdw3': pltpu.VMEM((f, d), F32), 'gdw2': pltpu.VMEM((f, d), F32),
        'dgout': pltpu.VMEM((n_dev, 2 * n_local, tokens // 2), F32),
        'sh': pltpu.VMEM((tokens, d), F32), 'shd': pltpu.VMEM((tokens, d), F32),
        'gs': dma((2, 2, nz // 2)), 'gr': dma((2, 2, nz // 2)), 'gxs': dma((nz, 2)), 'gxr': dma((nz, 2)),
        'ds': dma((2, 2, nz // 2)), 'dr': dma((2, 2, nz // 2)), 'dxs': dma((nz, 2)), 'dxr': dma((nz, 2)),
        'ts': dma((2, 1, nz // 2)), 'tr': dma((2, 1, nz // 2)), 'txs': dma((nz, 1)), 'txr': dma((nz, 1)),
    })
    for tag in ('_a', '_b'):
        scratch.update({
            'dgin' + tag: pltpu.VMEM((n_dev, 2 * n_local, tokens // 2), F32),
            'as' + tag: dma((n_dev,)), 'ar' + tag: dma((n_dev,)),
        })
    for tag in ('f', 'b'):
        scratch.update({
            tag + 'acc': pltpu.VMEM((nz, tokens, d), F32),
            tag + 'out': pltpu.VMEM((2, tokens, d), F32),
            tag + 'sib': pltpu.VMEM((nz, tokens, d), F32),
            tag + 'box': pltpu.VMEM((2, nz - 1, tokens // 2, d), F32),
            tag + 'xs': dma((nz,)), tag + 'xr': dma((nz,)),
            tag + 'ss': dma((2, nz - 1, PARTS)), tag + 'rs': dma((2, nz - 1, PARTS)),
        })
    result = pl.pallas_call(
        functools.partial(step_kernel, list(ins) + list(outs) + list(scratch), dims),
        out_shape=[jax.ShapeDtypeStruct(s, t) for s, t, _ in outs.values()],
        in_specs=[any_spec] * len(ins),
        out_specs=[spec for _, _, spec in outs.values()],
        scratch_shapes=list(scratch.values()),
        compiler_params=pltpu.CompilerParams(collective_id=0, has_side_effects=True, vmem_limit_bytes=VMEM_BYTES),
        name='two_layers',
    )(*ins.values())
    return dict(zip(outs, result))


def settle_kernel(pieces, *refs):
    n = len(refs[:-2]) // 3
    ins, outs, bufs = refs[:n], refs[n:2 * n], refs[2 * n:3 * n]
    get_sem, put_sem = refs[-2:]
    gets, puts = [], []
    for i in range(n):
        for j in range(pieces[i]):
            rows = pl.ds(j * (ins[i].shape[0] // pieces[i]), ins[i].shape[0] // pieces[i])
            at = len(gets)
            gets.append(pltpu.make_async_copy(ins[i].at[rows], bufs[i].at[rows], get_sem.at[at]))
            puts.append(pltpu.make_async_copy(bufs[i].at[rows], outs[i].at[rows], put_sem.at[at]))
    for get in gets:
        get.start()
    for get, put in zip(gets, puts):
        get.wait()
        put.start()
    for put in puts:
        put.wait()


def settle(arrays):
    pieces = [a.shape[0] if a.ndim == 3 else 1 for a in arrays]
    total = sum(pieces)
    any_spec = pl.BlockSpec(memory_space=pl.ANY)
    return pl.pallas_call(
        functools.partial(settle_kernel, pieces),
        out_shape=[jax.ShapeDtypeStruct(a.shape, a.dtype) for a in arrays],
        in_specs=[any_spec] * len(arrays),
        out_specs=[any_spec] * len(arrays),
        scratch_shapes=[pltpu.VMEM(a.shape, a.dtype) for a in arrays]
        + [pltpu.SemaphoreType.DMA((total,)), pltpu.SemaphoreType.DMA((total,))],
        compiler_params=pltpu.CompilerParams(vmem_limit_bytes=VMEM_BYTES),
        name='settle',
    )(*arrays)


def solution(mesh):
    group_size = mesh.shape['ep']
    token_spec = P(('dp', 'ep'), None)
    expert_spec = P('ep', None, None)
    shared_spec = P(None, None)
    grad_spec = P(('dp', 'ep'), None, None)
    layer_specs = (expert_spec,) * 3 + (shared_spec,) * 3

    def device_step(x_in, d_out, idx_a, gate_a, idx_b, gate_b,
                    w1_a, w3_a, w2_a, ws1_a, ws3_a, ws2_a,
                    w1_b, w3_b, w2_b, ws1_b, ws3_b, ws2_b):
        def turned(w):
            return jnp.swapaxes(w, -1, -2)

        weights_a = (turned(w1_a), turned(w3_a), w2_a, turned(ws1_a), turned(ws3_a), ws2_a)
        weights_b = (turned(w1_b), turned(w3_b), w2_b, turned(ws1_b), turned(ws3_b), ws2_b)
        tokens, top_k = idx_a.shape
        n_local = w1_a.shape[0]
        dims = (group_size // 2, n_local, slot_capacity(tokens, n_local * group_size, top_k), tokens, top_k)
        routes = {'idx_a': idx_a.T, 'idx_b': idx_b.T, 'gate_a': gate_a.T, 'gate_b': gate_b.T}
        got = run_step(dims, x_in, d_out, routes, weights_a, weights_b)
        x_last, d_first, *grads = settle(
            [got['y_out'], got['dx_out']]
            + [got[n + tag] for tag in ('_a', '_b') for n in ('dw1', 'dw3', 'dw2')]
            + [got['dgate_a'], got['dgate_b']])
        for at in (0, 1, 3, 4):
            grads[at] = turned(grads[at])
        return (x_last, d_first, *grads[:6], grads[6].T, grads[7].T)

    in_specs = (token_spec,) * 6 + layer_specs + layer_specs
    out_specs = (token_spec, token_spec) + (grad_spec,) * 6 + (token_spec, token_spec)
    return jax.shard_map(device_step, mesh=mesh, in_specs=in_specs, out_specs=out_specs, check_vma=False)
```

```python
import functools

import jax
import jax.numpy as jnp
from jax import lax
from jax.experimental import pallas as pl
from jax.experimental.pallas import tpu as pltpu
from jax.sharding import PartitionSpec as P

F32 = jnp.float32
BF16 = jnp.bfloat16
MESH = pl.DeviceIdType.MESH
VMEM_BYTES = 67_000_000
TAB = 8
PARTS = 2


def slot_capacity(tokens, n_experts, top_k):
    return top_k * ((2 * tokens + n_experts - 1) // n_experts)


def dot(a, b):
    return jnp.dot(a, b, preferred_element_type=F32)


def dot_nt(a, b):
    return lax.dot_general(a, b, (((1,), (1,)), ((), ())), preferred_element_type=F32)


def dot_tn(a, b):
    return lax.dot_general(a, b, (((0,), (0,)), ((), ())), preferred_element_type=F32)


def swiglu_grads(pre_gate, pre_up, d_hidden):
    sigma = jax.nn.sigmoid(pre_gate)
    d_gate = d_hidden * pre_up * sigma * (1.0 + pre_gate * (1.0 - sigma))
    d_up = d_hidden * pre_gate * sigma
    return d_gate.astype(BF16), d_up.astype(BF16)


def hidden_of(rows, w_gate, w_up):
    pre_gate = dot_nt(rows, w_gate)
    pre_up = dot_nt(rows, w_up)
    return pre_gate, pre_up, (pre_gate * jax.nn.sigmoid(pre_gate) * pre_up).astype(BF16)


def when(cond, body):
    if isinstance(cond, bool):
        if cond:
            body()
    else:
        pl.when(cond)(body)


class Place:
    def __init__(self, nz):
        self.nz = nz
        self.me = lax.axis_index('ep')
        self.z = self.me // 2
        self.c = self.me % 2

    def chip(self, offset):
        return lax.rem(self.z + offset + 2 * self.nz, self.nz)

    def source(self, offset, rel):
        return self.chip(offset) * 2 + lax.rem(self.c + rel, 2)

    def device(self, offset, rel=0):
        return {'ep': self.source(offset, rel)}


class Gather:
    def __init__(self, place, buf, pieces, sems):
        self.p, self.buf, self.pieces = place, buf, pieces
        self.ss, self.rs, self.xs, self.xr = sems
        self.rows = buf.shape[1] // pieces

    def far(self, di, h):
        near = self.p.nz // 2 - 1
        return near + 1 if di == h else near

    def at(self, offset, rel, h):
        return self.buf.at[self.p.source(offset, rel), pl.ds(h * self.rows, self.rows)]

    def hop(self, di, h, k, offset):
        d = 1 - 2 * di
        ref = self.at(offset, 0, h)
        return pltpu.make_async_remote_copy(ref, ref, self.ss.at[di, h, k - 1], self.rs.at[di, h, k - 1],
                                            device_id=self.p.device(d), device_id_type=MESH)

    def send(self, di, h, k):
        d = 1 - 2 * di
        return self.hop(di, h, k, -d * (k - 1))

    def recv(self, di, h, k):
        d = 1 - 2 * di
        return self.hop(di, h, k, -d * k)

    def cross(self, h, offset, rel=0):
        ref = self.at(offset, rel, h)
        roff = lax.rem(offset + self.p.nz, self.p.nz) if not isinstance(offset, int) else offset % self.p.nz
        return pltpu.make_async_remote_copy(ref, ref, self.xs.at[roff, h], self.xr.at[roff, h],
                                            device_id=self.p.device(0, 1), device_id_type=MESH)

    def start(self):
        for h in range(self.pieces):
            for di in range(2):
                self.send(di, h, 1).start()
        for h in range(self.pieces):
            self.cross(h, 0).start()

    def step(self, k):
        for h in range(self.pieces):
            for di in range(2):
                d = 1 - 2 * di
                far = self.far(di, h)

                def arrive(di=di, h=h, d=d, far=far):
                    self.recv(di, h, k).wait_recv()
                    when(k + 1 <= far, lambda: self.send(di, h, k + 1).start())
                    self.cross(h, -d * k).start()

                when(k <= far, arrive)

    def wait_cross(self, offset):
        for h in range(self.pieces):
            self.cross(h, offset, 1).wait_recv()

    def drain(self):
        for h in range(self.pieces):
            for di in range(2):
                for k in range(1, self.far(di, h) + 1):
                    self.send(di, h, k).wait_send()
            for roff in range(self.p.nz):
                self.cross(h, roff).wait_send()


class Scatter:
    def __init__(self, place, acc, out, sib, box, sems):
        self.p, self.acc, self.out, self.sib, self.box = place, acc, out, sib, box
        self.xs, self.xr, self.ss, self.rs = sems
        self.half = acc.shape[1] // 2
        self.steps = place.nz - 1

    def cross(self, roff, slot):
        return pltpu.make_async_remote_copy(self.out.at[slot], self.sib.at[roff], self.xs.at[roff], self.xr.at[roff],
                                            device_id=self.p.device(0, 1), device_id_type=MESH)

    def merge(self, roff):
        self.cross(roff, 0).wait_recv()

        def add(i, carry):
            rows = pl.ds(i * 64, 64)
            self.acc[roff, rows, :] += self.sib[roff, rows, :]
            return carry

        lax.fori_loop(0, self.acc.shape[1] // 64, add, 0)

    def reach(self, i):
        return self.p.nz // 2 - (i + 1) // 2

    def roff(self, di, i):
        r = self.reach(i)
        return r if di == 0 else self.p.nz - r

    def side(self, di, i):
        return (i + di) % 2

    def hop(self, di, i, part):
        size = self.half // PARTS
        rows = pl.ds(self.side(di, i) * self.half + part * size, size)
        return pltpu.make_async_remote_copy(self.acc.at[self.roff(di, i), rows],
                                            self.box.at[di, i, pl.ds(part * size, size)],
                                            self.ss.at[di, i, part], self.rs.at[di, i, part],
                                            device_id=self.p.device(1 - 2 * di), device_id_type=MESH)

    def take(self, di, i, part, roff):
        self.hop(di, i, part).wait_recv()
        size = self.half // PARTS
        into = pl.ds(pl.multiple_of(self.side(di, i) * self.half + part * size, size), size)
        self.acc[roff, into, :] += self.box[di, i, pl.ds(part * size, size), :]

    def begin(self, i):
        for roff in sorted({self.roff(0, i), self.roff(1, i)}):
            self.merge(roff)
        for part in range(PARTS):
            for di in range(2):
                self.hop(di, i, part).start()

    def step(self, i):
        for part in range(PARTS):
            for di in range(2):
                self.take(di, i - 2, part, self.roff(di, i))
                self.hop(di, i, part).start()

    def merge_for(self, i):
        self.merge(self.roff(0, i))
        self.merge(self.roff(1, i))

    def free(self, frees):
        for slot, roff, cond in frees:
            when(cond, functools.partial(lambda slot, roff: self.cross(roff, slot).wait_send(), slot, roff))

    def finish(self):
        for i in (self.steps - 2, self.steps - 1):
            for part in range(PARTS):
                for di in range(2):
                    self.take(di, i, part, 0)

    def drain(self):
        for i in range(self.steps):
            for part in range(PARTS):
                for di in range(2):
                    self.hop(di, i, part).wait_send()


def step_kernel(names, dims, *refs):
    r = dict(zip(names, refs))
    nz, n_local, cap, tokens, top_k = dims
    p = Place(nz)
    n_dev = 2 * nz
    far = nz // 2

    def load_weights(tag):
        return [pltpu.make_async_copy(r[n + tag], r[n], r['wsem'].at[i])
                for i, n in enumerate(('w1', 'w3', 'w2', 'ws1', 'ws3', 'ws2'))]

    def load_own(name, buf, i):
        return pltpu.make_async_copy(r[name], r[buf].at[p.me], r['lsem'].at[i])

    own_x, own_dy = load_own('x_in', 'xg', 1), load_own('dy_in', 'dg', 2)
    parts = [pltpu.make_async_copy(r[n + '_in'], r[n], r['tsem'].at[i])
             for i, n in enumerate(('idx_a', 'idx_b', 'gate_a', 'gate_b'))]
    for copy in parts + [own_x, own_dy]:
        copy.start()
    for i, (copy, name) in enumerate(zip(parts, ('idx_a', 'idx_b', 'gate_a', 'gate_b'))):
        copy.wait()
        rows = r[name][...].astype(F32)
        fill = jnp.full((TAB - rows.shape[0], tokens), -1.0 if i < 2 else 0.0, F32)
        r['tab'][p.me, i * TAB:(i + 1) * TAB, :] = jnp.concatenate([rows, fill], axis=0)

    barrier = pltpu.get_barrier_semaphore()
    for peer in (p.device(1), p.device(-1), p.device(0, 1)):
        pl.semaphore_signal(barrier, inc=1, device_id=peer, device_id_type=MESH)
    pl.semaphore_wait(barrier, 3)

    tabs = Gather(p, r['tab'], 1, (r['ts'], r['tr'], r['txs'], r['txr']))
    xs = Gather(p, r['xg'], 2, (r['gs'], r['gr'], r['gxs'], r['gxr']))
    ds = Gather(p, r['dg'], 2, (r['ds'], r['dr'], r['dxs'], r['dxr']))
    sf = Scatter(p, r['facc'], r['fout'], r['fsib'], r['fbox'], (r['fxs'], r['fxr'], r['fss'], r['frs']))
    sb = Scatter(p, r['bacc'], r['bout'], r['bsib'], r['bbox'], (r['bxs'], r['bxr'], r['bss'], r['brs']))

    own_x.wait()
    tabs.start()
    xs.start()

    tri = (lax.broadcasted_iota(jnp.int32, (tokens, tokens), 0)
           < lax.broadcasted_iota(jnp.int32, (tokens, tokens), 1))
    r['tri'][...] = jnp.where(tri, 1.0, 0.0).astype(BF16)

    def offset_of(k, q):
        return k * (1 - 2 * (q // 2))

    def pos_rows(base, n):
        return pl.ds(pl.multiple_of(base * cap, 16), n * cap)

    def spot(k):
        if isinstance(k, int) and k in (0, far):
            return (0 if k == 0 else n_dev - 2), 2
        return 2 + (k - 1) * 4, 4

    def arrived(st, k):
        for i in range(spot(k)[1] // 2):
            st.wait_cross(offset_of(k, 2 * i))

    def route(k, layer):
        base, n = spot(k)

        def body(q, carry):
            s = p.source(offset_of(k, q), q % 2)
            ids = r['tab'][s, pl.ds(layer * TAB, TAB), :]
            gates = r['tab'][s, pl.ds((2 + layer) * TAB, TAB), :]
            used, gate = [], []
            for e in range(n_local):
                hit = ids == (p.me * n_local + e).astype(F32)
                used.append(jnp.max(jnp.where(hit, 1.0, 0.0), axis=0, keepdims=True))
                gate.append(jnp.sum(jnp.where(hit, gates, 0.0), axis=0, keepdims=True))
            zeros = jnp.zeros((8 - n_local, tokens), F32)
            used = jnp.concatenate(used + [zeros], axis=0)
            rank = dot(used.astype(BF16), r['tri'][...])
            slot = jnp.where(used > 0, rank, -1.0)
            pos = base + q
            r['grow'][pos] = jnp.concatenate(gate + [zeros], axis=0)
            place = lax.broadcasted_iota(jnp.int32, (cap, tokens), 0).astype(F32)
            for e in range(n_local):
                r['pall'][pos, e * cap:(e + 1) * cap, :] = jnp.where(place == slot[e:e + 1, :], 1.0, 0.0).astype(BF16)
            return carry

        lax.fori_loop(0, n, body, 0)

    def dispatch(k):
        base, n = spot(k)

        def body(q, carry):
            s = p.source(offset_of(k, q), q % 2)
            pos = base + q
            rows = dot(r['pall'][pos], r['xg'][s]).astype(BF16)
            for e in range(n_local):
                r['xr'][e, pos_rows(pos, 1), :] = rows[e * cap:(e + 1) * cap]
            return carry

        lax.fori_loop(0, n, body, 0)

    def dispatch_dy(k):
        base, n = spot(k)

        def body(q, carry):
            s = p.source(offset_of(k, q), q % 2)
            pos = base + q
            pick = r['pall'][pos]
            gate = r['grow'][pos]
            rows = dot(pick, r['dg'][s]).astype(BF16)
            for e in range(n_local):
                wide = pick[e * cap:(e + 1) * cap].astype(F32) * gate[e:e + 1, :]
                col = jnp.sum(wide, axis=1, keepdims=True)
                r['gcol'][e, pl.ds(pl.multiple_of(q * cap, 16), cap), :] = jnp.broadcast_to(col, (cap, 128))
                r['dyr'][e, pos_rows(pos, 1), :] = rows[e * cap:(e + 1) * cap]
            return carry

        lax.fori_loop(0, n, body, 0)

    def expert_fwd(k):
        base, n = spot(k)

        def body(e, carry):
            hidden = hidden_of(r['xr'][e, pos_rows(base, n), :], r['w1'][e], r['w3'][e])[2]
            r['rowbuf'][e, 0:n * cap, :] = dot(hidden, r['w2'][e]).astype(BF16)
            return carry

        lax.fori_loop(0, n_local, body, 0)

    def expert_bwd(k):
        base, n = spot(k)

        def body(e, carry):
            span = pos_rows(base, n)
            here = slice(0, n * cap)
            pre_gate, pre_up, hidden = hidden_of(r['xr'][e, span, :], r['w1'][e], r['w3'][e])
            dy = r['dyr'][e, span, :]
            projected = dot_nt(dy, r['w2'][e])
            gcol = r['gcol'][e, here, 0:1]
            dgate = jnp.sum(hidden.astype(F32) * projected, axis=1, keepdims=True)
            r['gcol'][e, here, :] = jnp.broadcast_to(dgate, (n * cap, 128))
            r['dyr'][e, span, :] = (gcol * dy.astype(F32)).astype(BF16)
            da_gate, da_up = swiglu_grads(pre_gate, pre_up, gcol * projected)
            r['h'][e, span, :] = hidden
            r['da1'][e, span, :] = da_gate
            r['da3'][e, span, :] = da_up
            du = dot(da_gate, r['w1'][e]) + dot(da_up, r['w3'][e])
            r['rowbuf'][e, here, :] = du.astype(BF16)
            return carry

        lax.fori_loop(0, n_local, body, 0)

    def combine(k, sc, gated, frees):
        base, n = spot(k)
        sc.free(frees)
        for ridx in range(n // 2):
            offset = offset_of(k, 2 * ridx)
            roff = offset % nz if isinstance(offset, int) else lax.rem(offset + nz, nz)
            for rel in (1, 0):
                q = 2 * ridx + rel
                pos = base + q
                rows = jnp.concatenate([r['rowbuf'][e, q * cap:(q + 1) * cap, :] for e in range(n_local)], axis=0)
                if gated:
                    pick = r['pall'][pos].astype(F32)
                    gate = r['grow'][pos]
                    part = None
                    for _ in range(3):
                        term = gate.astype(BF16).astype(F32)
                        gate = gate - term
                        wide = jnp.concatenate(
                            [pick[e * cap:(e + 1) * cap] * term[e:e + 1, :] for e in range(n_local)], axis=0)
                        one = dot_tn(wide.astype(BF16), rows)
                        part = one if part is None else part + one
                else:
                    part = dot_tn(r['pall'][pos], rows)
                if rel == 1:
                    sc.out[ridx] = part
                else:
                    sc.acc[roff] = part
            sc.cross(roff, ridx).start()

    def gate_rows(k, dgout):
        base, n = spot(k)

        def body(q, carry):
            s = p.source(offset_of(k, q), q % 2)
            pos = base + q
            rows = []
            for e in range(n_local):
                col = r['gcol'][e, pl.ds(pl.multiple_of(q * cap, 16), cap), 0:1]
                pick = r['pall'][pos, e * cap:(e + 1) * cap, :].astype(F32)
                rows.append(jnp.sum(pick * col, axis=0, keepdims=True))
            wide = jnp.concatenate(rows, axis=0)
            half = tokens // 2
            dgout[s] = jnp.concatenate([wide[:, :half], wide[:, half:]], axis=0)
            return carry

        lax.fori_loop(0, n, body, 0)

    def upward(k, first):
        return [(0, k - 1, k > first), (1, lax.rem(nz - (k - 1), nz), k > max(first, 1))]

    def order(j):
        return 3 + 2 * (j // 2) - j % 2

    def turn(sc, j):
        i = order(j)
        when(j % 2 == 0, lambda: sc.merge_for(i))
        sc.step(i)

    turns = nz - 4

    def phase(fwd, bwd, layer, tag, middle_hook, early, emit_y, emit_dx):
        weights = load_weights(tag)
        for copy in weights:
            copy.start()
        streams = [xs, ds] if bwd else [tabs, xs]
        x_streams = [xs] if bwd else [tabs, xs]
        dgout, dgin, a_ss, a_rs = (r[n] for n in ('dgout', 'dgin' + tag, 'as' + tag, 'ar' + tag)) if bwd else (None,) * 4

        if bwd:
            route(0, layer)
            lax.fori_loop(1, far, lambda k, c: (route(k, layer), c)[1], 0)
            route(far, layer)
        for copy in weights[:3]:
            copy.wait()

        def shared():
            for copy in weights[3:]:
                copy.wait()
            x_own = r['xg'][p.me]
            s_gate, s_up, s_hidden = hidden_of(x_own, r['ws1'][...], r['ws3'][...])
            if fwd:
                r['sh'][...] = dot(s_hidden, r['ws2'][...]) + x_own.astype(F32)
            if bwd:
                d_own = r['dg'][p.me]
                d_sg, d_su = swiglu_grads(s_gate, s_up, dot_nt(d_own, r['ws2'][...]))
                r['shd'][...] = dot(d_sg, r['ws1'][...]) + dot(d_su, r['ws3'][...]) + d_own.astype(F32)

        def group_x(k, frees):
            for st in x_streams:
                arrived(st, k)
            if not bwd:
                route(k, layer)
            dispatch(k)
            if fwd:
                expert_fwd(k)
                combine(k, sf, True, frees)

        def group_dy(k, frees):
            arrived(ds, k)
            dispatch_dy(k)
            expert_bwd(k)
            combine(k, sb, False, frees)
            gate_rows(k, dgout)

        def steps(k):
            if bwd and not fwd:
                ds.step(k)
                if isinstance(k, int):
                    xs.step(k)
                else:
                    when(k == 1, lambda: xs.step(2))
                    when(k == far - 1, lambda: xs.step(far - 1))
                return
            for st in x_streams:
                st.step(k)
            if bwd:
                if isinstance(k, int):
                    ds.step(k)
                else:
                    when(k + 1 < far, lambda: ds.step(k + 1))

        first = 0 if bwd else 1
        if bwd:
            group_x(0, [])
            if not fwd:
                group_dy(0, [])

        def middle(k, carry):
            steps(k)
            if middle_hook is not None:
                pl.when(k == far - 1)(middle_hook)
            group_x(k, upward(k, first))
            if not fwd:
                group_dy(k, upward(k, first))
            return carry

        lax.fori_loop(1, far, middle, 0)
        steps(far)
        lead = sf if fwd else sb
        lead.begin(1)
        last = [(0, far - 1, True)]
        group_x(far, last)
        if not fwd:
            group_dy(far, last)
        lead.begin(0)
        shared()
        left = [(lead, 0, far), (lead, 1, nz - far + 1)]

        def grad_copy(o, wait):
            to = lax.rem(p.me + o, n_dev)
            landed = dgin.at[lax.rem(p.me - o + n_dev, n_dev)] if wait else dgin.at[p.me]
            return pltpu.make_async_remote_copy(dgout.at[to], landed, a_ss.at[o], a_rs.at[o],
                                                device_id={'ep': to}, device_id_type=MESH)

        def put(e):
            return [pltpu.make_async_copy(r['g' + n], r[n + tag].at[e], r['osem'].at[i])
                    for i, n in enumerate(('dw1', 'dw3', 'dw2'))]

        def weight_grads(e):
            copies = put(e)

            @pl.when(e > 0)
            def _():
                for copy in copies:
                    copy.wait()

            rows = r['xr'][e]
            r['gdw1'][...] = dot_tn(r['da1'][e], rows)
            r['gdw3'][...] = dot_tn(r['da3'][e], rows)
            r['gdw2'][...] = dot_tn(r['h'][e], r['dyr'][e])
            for copy in copies:
                copy.start()

        def drain_streams():
            for st in streams:
                st.drain()

        if not bwd:
            turn(sf, 0)
            drain_streams()
            group_x(0, [(0, far, True)])
            left[0] = (sf, 0, 0)
            for j in range(1, turns):
                turn(sf, j)
            sf.step(nz - 2)
        else:
            if fwd:
                group_dy(far, [])
                turn(sf, 0)
                group_dy(far - 1, [(0, far, True)])
                turn(sf, 1)
                sb.begin(1)
                sb.begin(0)

                def outward(j, carry):
                    k = far - j
                    group_dy(k, [(0, k + 1, True), (1, nz - (k + 1), True)])
                    turn(sf, j)
                    return carry

                lax.fori_loop(2, far, outward, 0)
                drain_streams()
                group_dy(0, [(0, 1, True)])
                left += [(sb, 0, 0), (sb, 1, nz - 1)]
                sf.step(nz - 2)

            def push(o, carry):
                grad_copy(o, False).start()
                return carry

            lax.fori_loop(1, n_dev, push, 0)

            def ring(j, carry):
                turn(sb, j)
                weight_grads(j)
                return carry

            lax.fori_loop(0, turns, ring, 0)
            sb.step(nz - 2)
        if not fwd:
            drain_streams()
        if fwd:
            sf.merge(0)
        if bwd:
            sb.merge(0)
        early()
        if bwd:
            dgin[p.me] = dgout[p.me]

            def pull(o, carry):
                grad_copy(o, True).wait_recv()
                return carry

            lax.fori_loop(1, n_dev, pull, 0)
            ids = r['tab'][p.me, pl.ds(layer * TAB, TAB), :]

            def collect(dev, total):
                block = dgin[dev]
                wide = jnp.concatenate([block[:n_local], block[n_local:]], axis=1)
                for e in range(n_local):
                    total += jnp.where(ids == (dev * n_local + e).astype(F32), wide[e:e + 1, :], 0.0)
                return total

            r['dgate' + tag][...] = lax.fori_loop(0, n_dev, collect, jnp.zeros((TAB, tokens), F32))[:top_k]
        if fwd:
            sf.finish()
            emit_y(r['sh'][...] + sf.acc[0])
        if bwd:
            sb.finish()
            emit_dx(r['shd'][...] + sb.acc[0])
            for copy in put(n_local - 1):
                copy.wait()

            def done(o, carry):
                grad_copy(o, False).wait_send()
                return carry

            lax.fori_loop(1, n_dev, done, 0)
        for sc, slot, roff in left:
            sc.cross(roff, slot).wait_send()
        if fwd:
            sf.drain()
        if bwd:
            sb.drain()

    def store(name, index=None, then=None):
        def put(value):
            if index is None:
                r[name][...] = value.astype(BF16)
            else:
                r[name][index] = value.astype(BF16)
            if then is not None:
                then()
        return put

    def nothing():
        pass

    def send_dy():
        own_dy.wait()
        ds.start()

    phase(True, False, 0, '_a', send_dy, lambda: ds.step(1), store('xg', p.me, xs.start), None)

    again = load_own('x_in', 'xg', 1)

    def send_x():
        again.start()
        again.wait()
        xs.start()

    phase(True, True, 1, '_b', None, send_x, store('y_out'), store('dg', p.me, ds.start))
    xs.step(1)

    phase(False, True, 0, '_a', None, nothing, None, store('dx_out'))


def run_step(dims, x, dy, routes, weights_a, weights_b):
    nz, n_local, cap, tokens, top_k = dims
    n_dev = 2 * nz
    d = x.shape[1]
    f = weights_a[0].shape[1]
    slots = n_local * cap
    rows = n_dev * cap
    any_spec = pl.BlockSpec(memory_space=pl.ANY)
    vmem_spec = pl.BlockSpec(memory_space=pltpu.VMEM)
    dma = pltpu.SemaphoreType.DMA
    kinds = ('w1', 'w3', 'w2', 'ws1', 'ws3', 'ws2')
    ins = {'x_in': x, 'dy_in': dy}
    ins.update({n + '_in': a for n, a in routes.items()})
    ins.update({n + '_a': w for n, w in zip(kinds, weights_a)})
    ins.update({n + '_b': w for n, w in zip(kinds, weights_b)})
    outs = {'y_out': ((tokens, d), BF16, vmem_spec), 'dx_out': ((tokens, d), BF16, vmem_spec)}
    for tag in ('_a', '_b'):
        for n in ('dw1', 'dw3', 'dw2'):
            outs[n + tag] = ((n_local, f, d), F32, any_spec)
        outs['dgate' + tag] = ((top_k, tokens), F32, vmem_spec)
    scratch = {n: pltpu.VMEM(w.shape, BF16) for n, w in zip(kinds, weights_a)}
    scratch.update({
        **{n: pltpu.VMEM(a.shape, a.dtype) for n, a in routes.items()},
        'tsem': dma((4,)), 'lsem': dma((3,)), 'wsem': dma((6,)), 'osem': dma((3,)),
        'xg': pltpu.VMEM((n_dev, tokens, d), BF16),
        'dg': pltpu.VMEM((n_dev, tokens, d), BF16),
        'tab': pltpu.VMEM((n_dev, 4 * TAB, tokens), F32),
        'tri': pltpu.VMEM((tokens, tokens), BF16),
        'pall': pltpu.VMEM((n_dev, slots, tokens), BF16),
        'grow': pltpu.VMEM((n_dev, 8, tokens), F32),
        'xr': pltpu.VMEM((n_local, rows, d), BF16),
        'dyr': pltpu.VMEM((n_local, rows, d), BF16),
        'rowbuf': pltpu.VMEM((n_local, 4 * cap, d), BF16),
        'gcol': pltpu.VMEM((n_local, 4 * cap, 128), F32),
        'h': pltpu.VMEM((n_local, rows, f), BF16),
        'da1': pltpu.VMEM((n_local, rows, f), BF16),
        'da3': pltpu.VMEM((n_local, rows, f), BF16),
        'gdw1': pltpu.VMEM((f, d), F32), 'gdw3': pltpu.VMEM((f, d), F32), 'gdw2': pltpu.VMEM((f, d), F32),
        'dgout': pltpu.VMEM((n_dev, 2 * n_local, tokens // 2), F32),
        'sh': pltpu.VMEM((tokens, d), F32), 'shd': pltpu.VMEM((tokens, d), F32),
        'gs': dma((2, 2, nz // 2)), 'gr': dma((2, 2, nz // 2)), 'gxs': dma((nz, 2)), 'gxr': dma((nz, 2)),
        'ds': dma((2, 2, nz // 2)), 'dr': dma((2, 2, nz // 2)), 'dxs': dma((nz, 2)), 'dxr': dma((nz, 2)),
        'ts': dma((2, 1, nz // 2)), 'tr': dma((2, 1, nz // 2)), 'txs': dma((nz, 1)), 'txr': dma((nz, 1)),
    })
    for tag in ('_a', '_b'):
        scratch.update({
            'dgin' + tag: pltpu.VMEM((n_dev, 2 * n_local, tokens // 2), F32),
            'as' + tag: dma((n_dev,)), 'ar' + tag: dma((n_dev,)),
        })
    for tag in ('f', 'b'):
        scratch.update({
            tag + 'acc': pltpu.VMEM((nz, tokens, d), F32),
            tag + 'out': pltpu.VMEM((2, tokens, d), F32),
            tag + 'sib': pltpu.VMEM((nz, tokens, d), F32),
            tag + 'box': pltpu.VMEM((2, nz - 1, tokens // 2, d), F32),
            tag + 'xs': dma((nz,)), tag + 'xr': dma((nz,)),
            tag + 'ss': dma((2, nz - 1, PARTS)), tag + 'rs': dma((2, nz - 1, PARTS)),
        })
    result = pl.pallas_call(
        functools.partial(step_kernel, list(ins) + list(outs) + list(scratch), dims),
        out_shape=[jax.ShapeDtypeStruct(s, t) for s, t, _ in outs.values()],
        in_specs=[any_spec] * len(ins),
        out_specs=[spec for _, _, spec in outs.values()],
        scratch_shapes=list(scratch.values()),
        compiler_params=pltpu.CompilerParams(collective_id=0, has_side_effects=True, vmem_limit_bytes=VMEM_BYTES),
        name='two_layers',
    )(*ins.values())
    return dict(zip(outs, result))


def settle_kernel(pieces, *refs):
    n = len(refs[:-2]) // 3
    ins, outs, bufs = refs[:n], refs[n:2 * n], refs[2 * n:3 * n]
    get_sem, put_sem = refs[-2:]
    gets, puts = [], []
    for i in range(n):
        for j in range(pieces[i]):
            rows = pl.ds(j * (ins[i].shape[0] // pieces[i]), ins[i].shape[0] // pieces[i])
            at = len(gets)
            gets.append(pltpu.make_async_copy(ins[i].at[rows], bufs[i].at[rows], get_sem.at[at]))
            puts.append(pltpu.make_async_copy(bufs[i].at[rows], outs[i].at[rows], put_sem.at[at]))
    for get in gets:
        get.start()
    for get, put in zip(gets, puts):
        get.wait()
        put.start()
    for put in puts:
        put.wait()


def settle(arrays):
    pieces = [a.shape[0] if a.ndim == 3 else 1 for a in arrays]
    total = sum(pieces)
    any_spec = pl.BlockSpec(memory_space=pl.ANY)
    return pl.pallas_call(
        functools.partial(settle_kernel, pieces),
        out_shape=[jax.ShapeDtypeStruct(a.shape, a.dtype) for a in arrays],
        in_specs=[any_spec] * len(arrays),
        out_specs=[any_spec] * len(arrays),
        scratch_shapes=[pltpu.VMEM(a.shape, a.dtype) for a in arrays]
        + [pltpu.SemaphoreType.DMA((total,)), pltpu.SemaphoreType.DMA((total,))],
        compiler_params=pltpu.CompilerParams(vmem_limit_bytes=VMEM_BYTES),
        name='settle',
    )(*arrays)


def solution(mesh):
    group_size = mesh.shape['ep']
    token_spec = P(('dp', 'ep'), None)
    expert_spec = P('ep', None, None)
    shared_spec = P(None, None)
    grad_spec = P(('dp', 'ep'), None, None)
    layer_specs = (expert_spec,) * 3 + (shared_spec,) * 3

    def device_step(x_in, d_out, idx_a, gate_a, idx_b, gate_b,
                    w1_a, w3_a, w2_a, ws1_a, ws3_a, ws2_a,
                    w1_b, w3_b, w2_b, ws1_b, ws3_b, ws2_b):
        def turned(w):
            return jnp.swapaxes(w, -1, -2)

        weights_a = (turned(w1_a), turned(w3_a), w2_a, turned(ws1_a), turned(ws3_a), ws2_a)
        weights_b = (turned(w1_b), turned(w3_b), w2_b, turned(ws1_b), turned(ws3_b), ws2_b)
        tokens, top_k = idx_a.shape
        n_local = w1_a.shape[0]
        dims = (group_size // 2, n_local, slot_capacity(tokens, n_local * group_size, top_k), tokens, top_k)
        routes = {'idx_a': idx_a.T, 'idx_b': idx_b.T, 'gate_a': gate_a.T, 'gate_b': gate_b.T}
        got = run_step(dims, x_in, d_out, routes, weights_a, weights_b)
        x_last, d_first, *grads = settle(
            [got['y_out'], got['dx_out']]
            + [got[n + tag] for tag in ('_a', '_b') for n in ('dw1', 'dw3', 'dw2')]
            + [got['dgate_a'], got['dgate_b']])
        for at in (0, 1, 3, 4):
            grads[at] = turned(grads[at])
        return (x_last, d_first, *grads[:6], grads[6].T, grads[7].T)

    in_specs = (token_spec,) * 6 + layer_specs + layer_specs
    out_specs = (token_spec, token_spec) + (grad_spec,) * 6 + (token_spec, token_spec)
    return jax.shard_map(device_step, mesh=mesh, in_specs=in_specs, out_specs=out_specs, check_vma=False)
```
